512 devices in a mesh: dp: 64 (over z, x_lo, core), mp: 8 (over y, x_hi).
Axes of the slice: x: 4 (x_hi: 2, x_lo: 2; x = x_hi * 2 + x_lo), y: 4, z: 16, core: 2. Of those that a mesh axis runs over, the one named last changes fastest.
Arguments:
- inputs_store: bfloat16 [512, 128], replicated, may hold values from -6 to 6
- window: int32 [64], replicated, may hold values from 0 to 511
- targets_store: bfloat16 [512, 4096], P(None, ('dp', 'mp')), may hold values from -6 to 6
- jac_store: bfloat16 [512, 4096, 128], P(None, ('dp', 'mp')), may hold values from -4 to 4
- first_weight: bfloat16 [128, 1024], replicated, may hold values from -0.5 to 0.5
- first_bias: bfloat16 [1024], replicated, may hold values from -3 to 3
- hidden_weight: bfloat16 [1024, 1024], P(None, 'mp'), may hold values from -0.1875 to 0.1875
- hidden_bias: bfloat16 [1024], P('mp'), may hold values from -3 to 3
- decoder_weight: bfloat16 [4096, 1024], P(('dp', 'mp')), may hold values from -0.1875 to 0.1875
Outputs:
- first_weights: float32 [128, 1024], replicated
- first_biases: float32 [1024], replicated
- hidden_weights: float32 [1024, 1024], P(None, 'mp')
- hidden_biases: float32 [1024], P('mp')
- decoder_grad: float32 [4096, 1024], P(('dp', 'mp'))
The draws below stay inside these ranges and needn't reach their ends.
Inputs may be any that keep to these rules, and one draw needn't show every extreme that they name: `window`: indices of stored samples; an index may repeat.
All inputs are finite; a program needn't handle non-finite values.
Results may differ from the reference program's by a relative error of at most 0.011.
Values may be sent and summed in bfloat16 or wider, within the bound.
A program may use at most 64 MiB of HBM per device.

```python
import math
import jax
import jax.numpy as jnp
from jax import lax

RANK = 128
H = 1024
OUT = 4096
NSTORE = 512
SAMPLES = 64
N_DP = 64
N_MP = 8


def place_ends(values, stream_key, low, high):
    dims = values.shape
    place = [jax.random.randint(jax.random.fold_in(stream_key, axis), (), 0, dims[axis]) for axis in range(len(dims))]
    values = values.at[tuple(place)].set(low)
    longest = dims.index(max(dims))
    place[longest] = (place[longest] + 1) % dims[longest]
    return values.at[tuple(place)].set(high)


def steps_of(key, shape, pieces, low, top_value):
    loudness = 1.0
    for axis_at, blocks in pieces:
        steps = jax.random.uniform(jax.random.fold_in(jax.random.fold_in(key, 6), axis_at), (blocks,), jnp.float32, low / len(pieces), top_value / len(pieces))
        loudness = loudness * jnp.repeat(jnp.exp(steps), shape[axis_at] // blocks).reshape((-1,) + (1,) * (len(shape) - 1 - axis_at))
    return loudness


def centred(key, extent, scale, most, pieces=(), kind=jnp.bfloat16):
    factor_of = steps_of(key, extent, pieces, -0.22, 0.18) if pieces else 1.0
    values = jax.random.normal(key, extent, jnp.float32) * scale * factor_of
    return jnp.minimum(jnp.maximum(values, -most), most).astype(kind)


def setup_inputs(seed: int = 0) -> dict:
    keys = jax.random.split(jax.random.key(seed), 10)
    return {
        "inputs_store": centred(keys[0], (NSTORE, RANK), 1.0, 6.0),
        "window": place_ends(jax.random.randint(keys[1], (SAMPLES,), 0, NSTORE), jax.random.fold_in(keys[1], 1), 0, NSTORE - 1).astype(jnp.int32),
        "targets_store": centred(keys[2], (NSTORE, OUT), 1.0, 6.0, ((1, 512),)),
        "jac_store": centred(keys[3], (NSTORE, OUT, RANK), 0.3, 4.0, ((1, 512),)),
        "first_weight": centred(keys[4], (RANK, H), RANK ** -0.5, 0.5),
        "first_bias": centred(keys[5], (H,), 0.5, 3.0),
        "hidden_weight": centred(keys[6], (H, H), H ** -0.5, 0.1875, ((1, 8),)),
        "hidden_bias": centred(keys[7], (H,), 0.5, 3.0, ((0, 8),)),
        "decoder_weight": centred(keys[8], (OUT, H), H ** -0.5, 0.1875, ((0, 512),)),
    }


def rounded(values):
    return lax.optimization_barrier(values.astype(jnp.bfloat16)).astype(jnp.float32)


def reference(inputs_store, window, targets_store, jac_store, first_weight, first_bias, hidden_weight, hidden_bias, decoder_weight):
    block = math.gcd(SAMPLES, 8)
    out_rows = OUT // (N_DP * N_MP)
    weight_one = first_weight.astype(jnp.float32)
    weight_two = hidden_weight.astype(jnp.float32)
    readout_weight = decoder_weight.astype(jnp.float32)
    dec_groups = readout_weight.reshape(N_DP, N_MP, out_rows, H)

    def block_step(totals, indices):
        grad_one, bias_one, grad_two, bias_two, decoder_gradient = totals
        inputs = inputs_store[indices]
        targets = targets_store[indices].astype(jnp.float32)
        jacobians = jac_store[indices].astype(jnp.float32)
        first_pre = jnp.dot(inputs, first_weight, preferred_element_type=jnp.float32) + first_bias.astype(jnp.float32)
        first_act = jnp.tanh(first_pre)
        first_slope = 1.0 - first_act * first_act
        first_tan = rounded(first_slope[:, None, :] * weight_one[None])
        first_round = rounded(first_act)
        hidden_lin = jnp.einsum("srh,hk->srk", first_tan, weight_two)
        hidden_pre = jnp.einsum("sh,hk->sk", first_round, weight_two) + hidden_bias.astype(jnp.float32)
        hidden_act = jnp.tanh(hidden_pre)
        hidden_slope = 1.0 - hidden_act * hidden_act
        hidden_tangent = rounded(hidden_slope[:, None, :] * hidden_lin)
        hidden_rounded_state = rounded(hidden_act)
        outputs_net = jnp.einsum("sk,ok->so", hidden_rounded_state, readout_weight)
        jacobian_predicted = jnp.einsum("mvn,an->mav", hidden_tangent, readout_weight)
        output_residual = rounded(outputs_net - targets)
        jacobian_residual = rounded(jacobian_predicted - jacobians)
        decoder_gradient = decoder_gradient + jnp.einsum("qi,qm->im", output_residual, hidden_rounded_state) + jnp.einsum("hzy,hym->zm", jacobian_residual, hidden_tangent)
        miss_groups = output_residual.reshape(block, N_DP, N_MP, out_rows)
        jac_groups = jacobian_residual.reshape(block, N_DP, N_MP, out_rows, RANK)
        act_back = jnp.sum(rounded(jnp.einsum("sdmk,dmkh->smh", miss_groups, dec_groups)), axis=1)
        tan_back = jnp.sum(rounded(jnp.einsum("sdmkr,dmkh->smrh", jac_groups, dec_groups)), axis=1)
        lin_back = tan_back * hidden_slope[:, None, :]
        pre_back = act_back * hidden_slope - 2.0 * hidden_act * hidden_slope * jnp.sum(tan_back * hidden_lin, axis=1)
        lin_round = rounded(lin_back)
        pre_round = rounded(pre_back)
        grad_two = grad_two + jnp.einsum("sh,sk->hk", first_round, pre_round) + jnp.einsum("srh,srk->hk", first_tan, lin_round)
        bias_two = bias_two + jnp.sum(pre_back, axis=0)
        tan_lower = jnp.einsum("srk,hk->srh", lin_round, weight_two)
        act_lower = jnp.einsum("sk,hk->sh", pre_round, weight_two)
        pre_lower = act_lower * first_slope - 2.0 * first_act * first_slope * jnp.sum(tan_lower * weight_one[None], axis=1)
        grad_one = grad_one + jnp.einsum("sr,sh->rh", inputs.astype(jnp.float32), pre_lower, precision=lax.Precision.HIGHEST) + jnp.sum(tan_lower * first_slope[:, None, :], axis=0)
        bias_one = bias_one + jnp.sum(pre_lower, axis=0)
        return (grad_one, bias_one, grad_two, bias_two, decoder_gradient), None

    start_totals = (jnp.zeros((RANK, H), jnp.float32), jnp.zeros((H,), jnp.float32), jnp.zeros((H, H), jnp.float32), jnp.zeros((H,), jnp.float32), jnp.zeros((OUT, H), jnp.float32))
    totals, unused = lax.scan(block_step, start_totals, window.reshape(-1, block))
    return totals[0], totals[1], totals[2], totals[3], totals[4]
```

```python
import jax
import jax.numpy as jnp
from jax import lax
from jax.experimental import pallas as pl
from jax.experimental.pallas import tpu as pltpu
from jax.sharding import Mesh
from jax.sharding import PartitionSpec as P

MESH = pl.DeviceIdType.MESH
DP = ("z", "xl", "c")
MP = ("y", "xh")
ALL = DP + MP
BF = jnp.bfloat16
F32 = jnp.float32

R = 128
H = 1024
NZ = 16
NT = (((1,), (1,)), ((), ()))
TN = (((0,), (0,)), ((), ()))


def dot(a, b, dims=(((1,), (0,)), ((), ()))):
    return lax.dot_general(a, b, dims, preferred_element_type=F32)


def remote(src, dst, send, recv, to):
    return pltpu.make_async_remote_copy(
        src_ref=src, dst_ref=dst, send_sem=send, recv_sem=recv, device_id=to, device_id_type=MESH
    )


def each(n, body):
    def step(t, carry):
        body(t)
        return carry

    lax.fori_loop(0, n, step, 0)


def far_first(t):
    odd = t % 2
    return NZ // 2 + odd * ((t + 1) // 2) - (1 - odd) * (t // 2)


def kernel(
    x_ref,
    jac_ref,
    tgt_ref,
    w1_ref,
    b1_ref,
    hw_ref,
    hb_ref,
    dec_ref,
    fw_ref,
    fb_ref,
    hg_ref,
    hbg_ref,
    dg_ref,
    ft,
    tsend,
    tfull,
    dblk,
    dmat,
    jbuf,
    tbuf,
    pbuf,
    rbuf,
    gsend,
    grecv,
    gown,
    hsend,
    hrecv,
    qsend,
    qrecv,
    fsend,
    frecv,
    zsend,
    zrecv,
    zall,
    hall,
    fall,
    s_tan,
    r_tan,
    s_dec,
    r_dec,
    s_half,
    r_half,
    s_jac,
    r_jac,
    s_tgt,
    r_tgt,
    s_back,
    r_back,
    s_gc,
    r_gc,
    s_gz,
    r_gz,
    s_q,
    r_q,
    s_f,
    r_f,
    s_zr,
    r_zr,
    s_zg,
    r_zg,
    s_h,
    r_h,
    s_fa,
    r_fa,
):
    z, xl, c = lax.axis_index("z"), lax.axis_index("xl"), lax.axis_index("c")
    y, xh = lax.axis_index("y"), lax.axis_index("xh")
    m = y * 2 + xh
    q = m * 2 + xl
    e = c * 2 + xl
    w = m * 4 + e
    b = c * NZ + z

    def at_z(zz):
        return {"z": zz}

    def at_zc(bb):
        return {"z": bb % NZ, "c": bb // NZ}

    def at_q(qq):
        return {"y": qq // 4, "xh": (qq // 2) % 2, "xl": qq % 2}

    def at_e(ee):
        return {"c": ee // 2, "xl": ee % 2}

    def at_w(ww):
        return {"y": ww // 8, "xh": (ww // 4) % 2, "c": (ww // 2) % 2, "xl": ww % 2}

    partner = {"c": 1 - c}
    barrier = pltpu.get_barrier_semaphore()

    def greet_zc(t):
        pl.semaphore_signal(barrier, inc=1, device_id=at_zc((b + t + 1) % 32), device_id_type=MESH)

    def greet_w(t):
        pl.semaphore_signal(barrier, inc=1, device_id=at_w((w + t + 1) % 32), device_id_type=MESH)

    each(31, greet_zc)
    each(31, greet_w)

    w1 = w1_ref[...].astype(F32)
    x_row = jnp.broadcast_to(x_ref[...], (16, R))
    first_pre = dot(x_row.astype(BF), w1_ref[...]) + b1_ref[...].astype(F32)
    first_act = jnp.tanh(first_pre)[0:1]
    first_slope = 1.0 - first_act * first_act
    top16 = lax.broadcasted_iota(jnp.int32, (16, H), 0) == 0
    ft[0:R, :] = (first_slope * w1).astype(BF)
    ft[R : R + 16, :] = jnp.where(top16, jnp.broadcast_to(first_act, (16, H)), 0.0).astype(BF)
    lin = dot(ft[...], hw_ref[...])
    hidden_lin = lin[0:R]
    hidden_act = jnp.tanh(lin[R : R + 1] + hb_ref[...].astype(F32))
    hidden_slope = 1.0 - hidden_act * hidden_act
    top = lax.broadcasted_iota(jnp.int32, (16, R), 0) == 0
    tsend[0:R, :] = (hidden_slope * hidden_lin).astype(BF)
    tsend[R : R + 16, :] = jnp.where(top, jnp.broadcast_to(hidden_act, (16, R)), 0.0).astype(BF)
    tfull[:, R + 16 :, :] = jnp.zeros((2, 2 * R - R - 16, H), BF)
    mine = pl.ds(pl.multiple_of(m * R, R), R)
    tfull[xl, 0 : R + 16, mine] = tsend[...]
    dblk[c, z] = dec_ref[...]
    jbuf[b] = jac_ref[b]
    tbuf[b] = tgt_ref[b]

    pl.semaphore_wait(barrier, 62)

    def tan_copy(peer, src):
        lanes = pl.ds(pl.multiple_of((src // 2) * R, R), R)
        return remote(
            tsend, tfull.at[src % 2, pl.ds(0, R + 16), lanes], s_tan.at[peer], r_tan.at[src], at_q(peer)
        )

    def dec_copy(peer, src):
        return remote(dec_ref, dblk.at[c, src], s_dec.at[peer], r_dec.at[src], at_z(peer))

    def jac_copy(peer, src):
        return remote(jac_ref.at[peer], jbuf.at[src], s_jac.at[peer], r_jac.at[src], at_zc(peer))

    def tgt_copy(peer, src):
        return remote(tgt_ref.at[peer], tbuf.at[src], s_tgt.at[peer], r_tgt.at[src], at_zc(peer))

    def half_copy(side):
        return remote(dblk.at[side], dblk.at[side], s_half, r_half, partner)

    def others(n, me, copy, what):
        def go(t):
            peer = (me + t + 1) % n
            if what == "start":
                copy(peer, me).start()
            elif what == "recv":
                copy(me, peer).wait_recv()
            else:
                copy(peer, me).wait_send()

        each(n - 1, go)

    def start_z(copy):
        def go(t):
            copy((z + far_first(t)) % NZ, z).start()

        each(NZ - 1, go)

    others(16, q, tan_copy, "start")
    start_z(dec_copy)

    def start_jac(t):
        zz = (z + far_first(t)) % NZ
        for cc in range(2):
            peer = cc * NZ + zz
            jac_copy(peer, b).start()
            tgt_copy(peer, b).start()

    each(NZ - 1, start_jac)
    pb = (1 - c) * NZ + z
    jac_copy(pb, b).start()
    tgt_copy(pb, b).start()

    others(NZ, z, dec_copy, "recv")
    half_copy(c).start()
    own_half = dblk[c].astype(F32).reshape(R, H).astype(BF)
    dmat[pl.ds(pl.multiple_of(c * R, R), R), :] = own_half
    others(16, q, tan_copy, "recv")
    others(32, b, jac_copy, "recv")
    others(32, b, tgt_copy, "recv")
    half_copy(1 - c).wait_recv()
    other_half = dblk[1 - c].astype(F32).reshape(R, H).astype(BF)
    dmat[pl.ds(pl.multiple_of((1 - c) * R, R), R), :] = other_half

    lane = lax.broadcasted_iota(jnp.int32, (32, 8, R), 2)
    row = lax.broadcasted_iota(jnp.int32, (32, 8, R), 1)
    tgt = jnp.broadcast_to(tbuf[...], (32, 8, R))
    miss = []
    for i in range(2):
        want = jnp.sum(jnp.where(lane == row + 8 * i, tgt, 0.0), axis=2, keepdims=True)
        want = jnp.where(lane == 0, jnp.broadcast_to(want, (32, 8, R)), 0.0).reshape(2 * R, R)
        stored = jbuf[:, i].astype(F32).reshape(2 * R, R)
        net = dot(dmat[...], tfull[i], NT)
        miss_i = (net - jnp.concatenate([stored, want], axis=1)).astype(BF)
        miss.append(miss_i)
        pbuf[i] = dot(miss_i, dmat[...], TN)[0 : R + 16].astype(BF)

    def back_copy(peer, src):
        lanes = pl.ds(pl.multiple_of((peer // 2) * R, R), R)
        return remote(
            pbuf.at[peer % 2, :, lanes], rbuf.at[src], s_back.at[peer], r_back.at[src], at_q(peer)
        )

    others(16, q, back_copy, "start")

    gown[...] = dot(miss[0], tfull[0]) + dot(miss[1], tfull[1])
    theirs = gown[pl.ds(pl.multiple_of((1 - c) * R, R), R), :]
    gsend[...] = theirs.reshape(NZ, 8, H).astype(BF)

    def gc_copy():
        return remote(gsend, grecv, s_gc, r_gc, partner)

    gc_copy().start()
    ours = gown[pl.ds(pl.multiple_of(c * R, R), R), :].reshape(NZ, 8, H)
    gc_copy().wait_recv()
    hsend[...] = (ours + grecv[...].astype(F32)).astype(BF)

    def gz_copy(peer, src):
        return remote(hsend.at[peer], hrecv.at[src], s_gz.at[peer], r_gz.at[src], at_z(peer))

    start_z(gz_copy)
    hrecv[z] = hsend[z]

    others(16, q, back_copy, "recv")
    rbuf[q] = pbuf[xl, :, mine]
    back = jnp.sum(rbuf[...].astype(F32), axis=0)
    tan_back = back[0:R]
    act_back = back[R : R + 1]
    lin_round = (tan_back * hidden_slope).astype(BF)
    pre_back = act_back * hidden_slope - 2.0 * hidden_act * hidden_slope * jnp.sum(
        tan_back * hidden_lin, axis=0, keepdims=True
    )
    pre_round = jnp.where(top, jnp.broadcast_to(pre_back, (16, R)), 0.0).astype(BF)
    both = jnp.concatenate([lin_round, pre_round], axis=0)
    qsend[...] = dot(ft[...], both, TN).astype(BF).reshape(4, 2 * R, R)

    def q_copy(peer, src):
        return remote(qsend.at[peer], qrecv.at[src], s_q.at[peer], r_q.at[src], at_e(peer))

    others(4, e, q_copy, "start")
    qrecv[e] = qsend[e]

    low = dot(both, hw_ref[...], NT)
    tan_lower = low[0:R]
    pre_lower = low[R : R + 1] * first_slope - 2.0 * first_act * first_slope * jnp.sum(
        tan_lower * w1, axis=0, keepdims=True
    )
    x_col = jnp.transpose(jnp.broadcast_to(x_ref[...], (R, R)))[:, 0:1]
    fw = x_col * pre_lower + tan_lower * first_slope
    place = lax.broadcasted_iota(jnp.int32, (16, H), 1) // R == m
    second = lax.broadcasted_iota(jnp.int32, (16, H), 0) == 1
    pre_wide = jnp.concatenate([pre_back] * 8, axis=1)
    tail = jnp.where(top16, jnp.broadcast_to(pre_lower, (16, H)), 0.0)
    tail = tail + jnp.where(second & place, jnp.broadcast_to(pre_wide, (16, H)), 0.0)
    for k in range(4):
        fsend[k, 0:32, :] = fw[32 * k : 32 * k + 32].astype(BF)
        fsend[k, 32:48, :] = tail.astype(BF)

    def f_copy(peer, src):
        lanes = pl.ds(pl.multiple_of((peer // 4) * R, R), R)
        return remote(
            fsend.at[peer % 4, :, lanes], frecv.at[src], s_f.at[peer], r_f.at[src], at_w(peer)
        )

    others(32, w, f_copy, "start")
    frecv[w] = fsend[e, :, mine]

    others(4, e, q_copy, "recv")
    quarter = jnp.sum(qrecv[...].astype(F32), axis=0)
    zsend[:, 0:2] = quarter.reshape(NZ, 2, 8, R).astype(BF)
    zsend[:, 2:3] = jnp.zeros((NZ, 1, 8, R), BF)
    others(32, w, f_copy, "recv")
    piece = jnp.sum(frecv[...].astype(F32), axis=0)
    zsend[0:6, 2] = piece.reshape(6, 8, R).astype(BF)

    def zr_copy(peer, src):
        return remote(zsend.at[peer], zrecv.at[src], s_zr.at[peer], r_zr.at[src], at_z(peer))

    start_z(zr_copy)
    zrecv[z] = zsend[z]
    others(NZ, z, zr_copy, "recv")
    zall[z] = jnp.sum(zrecv[...].astype(F32), axis=0).astype(BF)

    def zg_copy(peer, src):
        return remote(zall.at[src], zall.at[src], s_zg.at[peer], r_zg.at[src], at_z(peer))

    start_z(zg_copy)

    others(NZ, z, gz_copy, "recv")
    dg_ref[...] = jnp.sum(hrecv[...].astype(F32), axis=0)

    others(NZ, z, zg_copy, "recv")

    def h_copy(peer, src):
        return remote(zall.at[:, pl.ds(0, 2)], hall.at[src], s_h.at[peer], r_h.at[src], at_e(peer))

    def fa_copy(peer, src):
        return remote(
            zall.at[pl.ds(0, 6), 2], fall.at[src], s_fa.at[peer], r_fa.at[src], at_w(peer)
        )

    others(32, w, fa_copy, "start")
    others(4, e, h_copy, "start")
    hall[e] = zall[:, 0:2]
    fall[w] = zall[0:6, 2]
    hbg_ref[...] = zall[4, 2].astype(F32)[1:2]
    others(4, e, h_copy, "recv")
    hg_ref[...] = hall[...].astype(F32).reshape(H, R)
    others(32, w, fa_copy, "recv")
    for mm in range(8):
        for ee in range(4):
            got = fall[4 * mm + ee].astype(F32)
            fw_ref[32 * ee : 32 * ee + 32, R * mm : R * mm + R] = got[0:4].reshape(32, R)
            if ee == 0:
                fb_ref[:, R * mm : R * mm + R] = got[4, 0:1]

    half_copy(c).wait_send()
    gc_copy().wait_send()
    others(16, q, tan_copy, "send")
    others(NZ, z, dec_copy, "send")
    others(32, b, jac_copy, "send")
    others(32, b, tgt_copy, "send")
    others(16, q, back_copy, "send")
    others(NZ, z, gz_copy, "send")
    others(4, e, q_copy, "send")
    others(32, w, f_copy, "send")
    others(NZ, z, zr_copy, "send")
    others(NZ, z, zg_copy, "send")
    others(4, e, h_copy, "send")
    others(32, w, fa_copy, "send")


def on_device(inputs_store, window, targets_store, jac_store, first_weight, first_bias, hidden_weight, hidden_bias, decoder_weight):
    sample = lax.axis_index("z") * 4 + lax.axis_index("c") * 2 + lax.axis_index("xl")
    x = inputs_store[lax.dynamic_slice_in_dim(window, sample, 1)].astype(F32)
    order = window.reshape(NZ, 2, 2).transpose(1, 0, 2).reshape(64)
    jac = jac_store[order].reshape(32, 2, 8, R)
    tgt = targets_store[order].astype(F32).reshape(32, 1, 16)
    tgt = jnp.pad(tgt, ((0, 0), (0, 0), (0, R - 16)))
    vmem = pl.BlockSpec(memory_space=pltpu.VMEM)
    dma = pltpu.SemaphoreType.DMA
    fw, fb, hg, hbg, dg = pl.pallas_call(
        kernel,
        out_shape=(
            jax.ShapeDtypeStruct((R, H), F32),
            jax.ShapeDtypeStruct((1, H), F32),
            jax.ShapeDtypeStruct((H, R), F32),
            jax.ShapeDtypeStruct((1, R), F32),
            jax.ShapeDtypeStruct((8, H), F32),
        ),
        in_specs=[vmem] * 8,
        out_specs=(vmem,) * 5,
        scratch_shapes=[
            pltpu.VMEM((R + 16, H), BF),
            pltpu.VMEM((R + 16, R), BF),
            pltpu.VMEM((2, 2 * R, H), BF),
            pltpu.VMEM((2, NZ, 8, H), BF),
            pltpu.VMEM((2 * R, H), BF),
            pltpu.VMEM((32, 2, 8, R), BF),
            pltpu.VMEM((32, 1, R), F32),
            pltpu.VMEM((2, R + 16, H), BF),
            pltpu.VMEM((16, R + 16, R), BF),
            pltpu.VMEM((NZ, 8, H), BF),
            pltpu.VMEM((NZ, 8, H), BF),
            pltpu.VMEM((2 * R, H), F32),
            pltpu.VMEM((NZ, 8, H), BF),
            pltpu.VMEM((NZ, 8, H), BF),
            pltpu.VMEM((4, 2 * R, R), BF),
            pltpu.VMEM((4, 2 * R, R), BF),
            pltpu.VMEM((4, 48, H), BF),
            pltpu.VMEM((32, 48, R), BF),
            pltpu.VMEM((NZ, 3, 8, R), BF),
            pltpu.VMEM((NZ, 3, 8, R), BF),
            pltpu.VMEM((NZ, 3, 8, R), BF),
            pltpu.VMEM((4, NZ, 2, 8, R), BF),
            pltpu.VMEM((32, 6, 8, R), BF),
            dma((16,)), dma((16,)),
            dma((NZ,)), dma((NZ,)),
            dma, dma,
            dma((32,)), dma((32,)),
            dma((32,)), dma((32,)),
            dma((16,)), dma((16,)),
            dma, dma,
            dma((NZ,)), dma((NZ,)),
            dma((4,)), dma((4,)),
            dma((32,)), dma((32,)),
            dma((NZ,)), dma((NZ,)),
            dma((NZ,)), dma((NZ,)),
            dma((4,)), dma((4,)),
            dma((32,)), dma((32,)),
        ],
        compiler_params=pltpu.CompilerParams(
            collective_id=0, has_side_effects=True, vmem_limit_bytes=40 * 1024 * 1024
        ),
    )(x, jac, tgt, first_weight, first_bias.reshape(1, H), hidden_weight, hidden_bias.reshape(1, R), decoder_weight)
    return fw, fb.reshape(H), hg, hbg.reshape(R), dg


def solution(mesh):
    torus = Mesh(mesh.devices.reshape(NZ, 2, 2, 4, 2), ALL)
    return jax.shard_map(
        on_device,
        mesh=torus,
        in_specs=(P(), P(), P(None, ALL), P(None, ALL, None), P(), P(), P(None, MP), P(MP), P(ALL, None)),
        out_specs=(P(), P(), P(None, MP), P(MP), P(ALL, None)),
        check_vma=False,
    )
```

```python
import jax
import jax.numpy as jnp
from jax import lax
from jax.experimental import pallas as pl
from jax.experimental.pallas import tpu as pltpu
from jax.sharding import Mesh
from jax.sharding import PartitionSpec as P

MESH = pl.DeviceIdType.MESH
DP = ("z", "xl", "c")
MP = ("y", "xh")
ALL = DP + MP
BF = jnp.bfloat16
F32 = jnp.float32

R = 128
H = 1024
NZ = 16
WIDE = H + R
NT = (((1,), (1,)), ((), ()))
TN = (((0,), (0,)), ((), ()))


def dot(a, b, dims=(((1,), (0,)), ((), ()))):
    return lax.dot_general(a, b, dims, preferred_element_type=F32)


def remote(src, dst, send, recv, to):
    return pltpu.make_async_remote_copy(
        src_ref=src, dst_ref=dst, send_sem=send, recv_sem=recv, device_id=to, device_id_type=MESH
    )


def each(n, body):
    def step(t, carry):
        body(t)
        return carry

    lax.fori_loop(0, n, step, 0)


def far_first(t):
    odd = t % 2
    return NZ // 2 + odd * ((t + 1) // 2) - (1 - odd) * (t // 2)


def slot_of(zz):
    return (zz % 4) * 4 + zz // 4


def kernel(
    ids_ref,
    idv_ref,
    xs_ref,
    jac_ref,
    tgt_ref,
    w1_ref,
    b1_ref,
    hw_ref,
    hb_ref,
    dec_ref,
    fw_ref,
    fb_ref,
    hg_ref,
    hbg_ref,
    dg_ref,
    ft,
    tsend,
    tfull,
    dsend,
    dblk,
    dmat,
    jsend,
    jbuf,
    pbuf,
    rbuf,
    gsend,
    grecv,
    gown,
    hsend,
    hrecv,
    qsend,
    qrecv,
    fsend,
    frecv,
    zsend,
    zrecv,
    zall,
    ysend,
    yrecv,
    yall,
    hall,
    fall,
    sent,
    came,
):
    z, xl, c = lax.axis_index("z"), lax.axis_index("xl"), lax.axis_index("c")
    y, xh = lax.axis_index("y"), lax.axis_index("xh")
    m = y * 2 + xh
    q = m * 2 + xl
    e = c * 2 + xl
    w = m * 4 + e
    zs = slot_of(z)
    b = c * NZ + zs

    def at_z(zz):
        return {"z": zz}

    def at_zc(bb):
        return {"z": bb % NZ, "c": bb // NZ}

    def at_q(qq):
        return {"y": qq // 4, "xh": (qq // 2) % 2, "xl": qq % 2}

    def at_e(ee):
        return {"c": ee // 2, "xl": ee % 2}

    def at_w(ww):
        return {"y": ww // 8, "xh": (ww // 4) % 2, "c": (ww // 2) % 2, "xl": ww % 2}

    partner = {"c": 1 - c}
    barrier = pltpu.get_barrier_semaphore()

    def greet_z(t):
        zz = (z + far_first(t)) % NZ
        for cc in range(2):
            pl.semaphore_signal(barrier, inc=1, device_id={"z": zz, "c": cc}, device_id_type=MESH)

    def greet_w(t):
        pl.semaphore_signal(barrier, inc=1, device_id=at_w((w + t + 1) % 32), device_id_type=MESH)

    each(NZ - 1, greet_z)
    each(31, greet_w)

    def pick(zz):
        for cc in range(2):
            for i in range(2):
                jsend[cc * NZ + slot_of(zz), i] = jac_ref[ids_ref[zz * 4 + cc * 2 + i]]

    each(NZ, pick)
    hot = (lax.broadcasted_iota(jnp.int32, (512, 64), 0) == idv_ref[...]).astype(F32).astype(BF)
    dsend[:, 0:H] = dec_ref[...]
    dsend[:, H : H + 64] = dot(tgt_ref[...], hot).astype(BF)
    dsend[:, H + 64 :] = jnp.zeros((8, R - 64), BF)
    own = ids_ref[z * 4 + c * 2 + xl]
    x_hot = (lax.broadcasted_iota(jnp.int32, (16, 512), 1) == own).astype(F32).astype(BF)
    x_rows = dot(x_hot, xs_ref[...])

    w1 = w1_ref[...].astype(F32)
    first_pre = dot(x_rows.astype(BF), w1_ref[...]) + b1_ref[...].astype(F32)
    first_act = jnp.tanh(first_pre)[0:1]
    first_slope = 1.0 - first_act * first_act
    top16 = lax.broadcasted_iota(jnp.int32, (16, H), 0) == 0
    ft[0:R, :] = (first_slope * w1).astype(BF)
    ft[R : R + 16, :] = jnp.where(top16, jnp.broadcast_to(first_act, (16, H)), 0.0).astype(BF)
    lin = dot(ft[...], hw_ref[...])
    hidden_lin = lin[0:R]
    hidden_act = jnp.tanh(lin[R : R + 1] + hb_ref[...].astype(F32))
    hidden_slope = 1.0 - hidden_act * hidden_act
    top = lax.broadcasted_iota(jnp.int32, (16, R), 0) == 0
    tsend[0:R, :] = (hidden_slope * hidden_lin).astype(BF)
    tsend[R : R + 16, :] = jnp.where(top, jnp.broadcast_to(hidden_act, (16, R)), 0.0).astype(BF)
    tfull[:, R + 16 :, :] = jnp.zeros((2, 2 * R - R - 16, H), BF)
    mine = pl.ds(pl.multiple_of(m * R, R), R)
    tfull[xl, 0 : R + 16, mine] = tsend[...]
    dblk[c, zs] = dsend[...]
    jbuf[b] = jsend[b]

    with jax.named_scope("barrier"):
        pl.semaphore_wait(barrier, 61)

    def tan_copy(peer, src):
        lanes = pl.ds(pl.multiple_of((src // 2) * R, R), R)
        dst = tfull.at[src % 2, pl.ds(0, R + 16), lanes]
        return remote(tsend, dst, sent.at[0], came.at[0], at_q(peer))

    def far_copy(peer, src):
        return remote(dsend, dblk.at[c, slot_of(src)], sent.at[1], came.at[1], at_z(peer))

    def near_copy(peer, first, count):
        part = dblk.at[c, pl.ds(first, count)]
        return remote(part, part, sent.at[2], came.at[2], at_z(peer))

    def half_copy(side):
        return remote(dblk.at[side], dblk.at[side], sent.at[3], came.at[3], partner)

    def jac_copy(zz, cc):
        return remote(
            jsend.at[cc * NZ + slot_of(zz)], jbuf.at[b], sent.at[4], came.at[4], {"z": zz, "c": cc}
        )

    def start(n, me, copy):
        with jax.named_scope(copy.__name__ + "_start"):
            each(n - 1, lambda t: copy((me + t + 1) % n, me).start())

    def start_z(copy):
        with jax.named_scope(copy.__name__ + "_start"):
            each(NZ - 1, lambda t: copy((z + far_first(t)) % NZ, z).start())

    def recv(k, ref):
        with jax.named_scope(f"recv{k}"):
            remote(ref, ref, sent.at[k], came.at[k], partner).wait_recv()

    def left(k, ref):
        remote(ref, ref, sent.at[k], came.at[k], partner).wait_send()

    for d in (8, 4, 12):
        far_copy((z + d) % NZ, z).start()
    start(16, q, tan_copy)

    def start_jac(t):
        zz = (z + far_first(t)) % NZ
        for cc in range(2):
            jac_copy(zz, cc).start()

    each(NZ - 1, start_jac)
    jac_copy(z, 1 - c).start()

    recv(1, dblk.at[0, pl.ds(0, 3)])
    group = (z % 4) * 4
    part = group + 2 * ((z // 4) % 2)
    near_copy((z + 2) % NZ, part, 2).start()
    near_copy((z + 14) % NZ, part, 2).start()
    near_copy((z + 1) % NZ, group, 4).start()
    near_copy((z + 15) % NZ, group, 4).start()
    recv(2, dblk.at[0, pl.ds(0, 12)])
    half_copy(c).start()

    def unpack(side):
        rows = pl.ds(pl.multiple_of(side * R, R), R)
        dmat[rows, :] = dblk[side].astype(F32).reshape(R, WIDE).astype(BF)

    unpack(c)
    recv(0, rbuf.at[pl.ds(0, 15)])
    recv(4, jbuf.at[pl.ds(0, 31)])
    recv(3, dblk.at[0])
    unpack(1 - c)

    lane = lax.broadcasted_iota(jnp.int32, (2 * R, R), 1)
    tgt = dmat[:, H:].astype(F32)
    dec = dmat[:, 0:H]
    miss = []
    for i in range(2):
        want = jnp.sum(jnp.where(lane == z * 4 + c * 2 + i, tgt, 0.0), axis=1, keepdims=True)
        want = jnp.where(lane == 0, jnp.broadcast_to(want, (2 * R, R)), 0.0)
        stored = jbuf[:, i].astype(F32).reshape(2 * R, R)
        net = dot(dec, tfull[i], NT)
        miss_i = (net - jnp.concatenate([stored, want], axis=1)).astype(BF)
        miss.append(miss_i)
        pbuf[i] = dot(miss_i, dec, TN)[0 : R + 16].astype(BF)

    def back_copy(peer, src):
        lanes = pl.ds(pl.multiple_of((peer // 2) * R, R), R)
        return remote(
            pbuf.at[peer % 2, :, lanes], rbuf.at[src], sent.at[5], came.at[5], at_q(peer)
        )

    start(16, q, back_copy)

    gown[...] = dot(miss[0], tfull[0]) + dot(miss[1], tfull[1])
    theirs = gown[pl.ds(pl.multiple_of((1 - c) * R, R), R), :]
    gsend[...] = theirs.reshape(NZ, 8, H).astype(BF)
    remote(gsend, grecv, sent.at[6], came.at[6], partner).start()
    ours = gown[pl.ds(pl.multiple_of(c * R, R), R), :].reshape(NZ, 8, H)
    recv(6, grecv)
    hsend[...] = (ours + grecv[...].astype(F32)).astype(BF)

    def gz_copy(peer, src):
        return remote(
            hsend.at[slot_of(peer)], hrecv.at[slot_of(src)], sent.at[7], came.at[7], at_z(peer)
        )

    start_z(gz_copy)
    hrecv[zs] = hsend[zs]

    recv(5, rbuf.at[pl.ds(0, 15)])
    rbuf[q] = pbuf[xl, :, mine]
    back = jnp.sum(rbuf[...].astype(F32), axis=0)
    tan_back = back[0:R]
    act_back = back[R : R + 1]
    lin_round = (tan_back * hidden_slope).astype(BF)
    pre_back = act_back * hidden_slope - 2.0 * hidden_act * hidden_slope * jnp.sum(
        tan_back * hidden_lin, axis=0, keepdims=True
    )
    pre_round = jnp.where(top, jnp.broadcast_to(pre_back, (16, R)), 0.0).astype(BF)
    both = jnp.concatenate([lin_round, pre_round], axis=0)
    qsend[...] = dot(ft[...], both, TN).astype(BF).reshape(4, 2 * R, R)

    def q_copy(peer, src):
        return remote(qsend.at[peer], qrecv.at[src], sent.at[8], came.at[8], at_e(peer))

    start(4, e, q_copy)
    qrecv[e] = qsend[e]

    low = dot(both, hw_ref[...], NT)
    tan_lower = low[0:R]
    pre_lower = low[R : R + 1] * first_slope - 2.0 * first_act * first_slope * jnp.sum(
        tan_lower * w1, axis=0, keepdims=True
    )
    x_col = jnp.transpose(jnp.broadcast_to(x_rows[0:1], (R, R)))[:, 0:1]
    fw = x_col * pre_lower + tan_lower * first_slope
    place = lax.broadcasted_iota(jnp.int32, (8, H), 1) // R == m
    line = lax.broadcasted_iota(jnp.int32, (8, H), 0)
    pre_wide = jnp.concatenate([pre_back] * 8, axis=1)
    tail = jnp.where(line == 0, jnp.broadcast_to(pre_lower, (8, H)), 0.0)
    tail = tail + jnp.where((line == 1) & place, jnp.broadcast_to(pre_wide, (8, H)), 0.0)
    for k in range(4):
        fsend[k, 0:4] = fw[32 * k : 32 * k + 32].reshape(4, 8, H).astype(BF)
        fsend[k, 4] = tail.astype(BF)

    def f_copy(peer, src):
        lanes = pl.ds(pl.multiple_of((peer // 4) * R, R), R)
        return remote(
            fsend.at[peer % 4, :, :, lanes], frecv.at[src], sent.at[9], came.at[9], at_w(peer)
        )

    start(32, w, f_copy)
    frecv[w] = fsend[e, :, :, mine]

    recv(8, qrecv.at[pl.ds(0, 3)])
    quarter = jnp.sum(qrecv[...].astype(F32), axis=0)
    zsend[...] = quarter.reshape(NZ, 2, 8, R).astype(BF)

    def zr_copy(peer, src):
        return remote(zsend.at[peer], zrecv.at[src], sent.at[10], came.at[10], at_z(peer))

    start_z(zr_copy)
    zrecv[z] = zsend[z]

    recv(9, frecv.at[pl.ds(0, 31)])
    ysend[...] = jnp.sum(frecv[...].astype(F32), axis=0).astype(BF)
    for t in range(5):

        @pl.when(z != t)
        def _():
            remote(ysend.at[t], yrecv.at[z], sent.at[11], came.at[11], at_z(t)).start()

        @pl.when(z == t)
        def _():
            yrecv[z] = ysend[t]

    recv(10, zrecv.at[pl.ds(0, 15)])
    zall[z] = jnp.sum(zrecv[...].astype(F32), axis=0).astype(BF)

    def zg_copy(peer, src):
        return remote(zall.at[src], zall.at[src], sent.at[12], came.at[12], at_z(peer))

    start_z(zg_copy)

    def y_copy(peer, src):
        return remote(yall.at[src], yall.at[src], sent.at[13], came.at[13], at_z(peer))

    @pl.when(z < 5)
    def _():
        recv(11, yrecv.at[pl.ds(0, 15)])
        yall[z] = jnp.sum(yrecv[...].astype(F32), axis=0).astype(BF)
        start_z(y_copy)

    recv(7, hrecv.at[pl.ds(0, 15)])
    dg_ref[...] = jnp.sum(hrecv[...].astype(F32), axis=0)

    recv(12, zall.at[pl.ds(0, 15)])

    def h_copy(peer, src):
        return remote(zall, hall.at[src], sent.at[14], came.at[14], at_e(peer))

    start(4, e, h_copy)

    @pl.when(z < 5)
    def _():
        recv(13, yall.at[pl.ds(0, 4)])

    @pl.when(z >= 5)
    def _():
        recv(13, yall.at[pl.ds(0, 5)])

    def fa_copy(peer, src):
        return remote(yall.at[pl.ds(0, 5)], fall.at[src], sent.at[15], came.at[15], at_w(peer))

    start(32, w, fa_copy)
    hall[e] = zall[...]
    fall[w] = yall[0:5]
    hbg_ref[...] = yall[4].astype(F32)[1:2]
    recv(14, hall.at[pl.ds(0, 3)])
    hg_ref[...] = hall[...].astype(F32).reshape(H, R)
    recv(15, fall.at[pl.ds(0, 31)])
    for mm in range(8):
        for ee in range(4):
            got = fall[4 * mm + ee].astype(F32)
            fw_ref[32 * ee : 32 * ee + 32, R * mm : R * mm + R] = got[0:4].reshape(32, R)
            if ee == 0:
                fb_ref[:, R * mm : R * mm + R] = got[4, 0:1]

    left(0, rbuf.at[pl.ds(0, 15)])
    left(1, dblk.at[0, pl.ds(0, 3)])
    left(2, dblk.at[0, pl.ds(0, 12)])
    left(3, dblk.at[0])
    left(4, jbuf.at[pl.ds(0, 31)])
    left(5, rbuf.at[pl.ds(0, 15)])
    left(6, grecv)
    left(7, hrecv.at[pl.ds(0, 15)])
    left(8, qrecv.at[pl.ds(0, 3)])
    left(9, frecv.at[pl.ds(0, 31)])
    left(10, zrecv.at[pl.ds(0, 15)])

    @pl.when(z < 5)
    def _():
        left(11, yall.at[pl.ds(0, 4)])
        left(13, yrecv.at[pl.ds(0, 15)])

    @pl.when(z >= 5)
    def _():
        left(11, yall.at[pl.ds(0, 5)])

    left(12, zrecv.at[pl.ds(0, 15)])
    left(14, hall.at[pl.ds(0, 3)])
    left(15, fall.at[pl.ds(0, 31)])


def on_device(
    inputs_store,
    window,
    targets_store,
    jac_store,
    first_weight,
    first_bias,
    hidden_weight,
    hidden_bias,
    decoder_weight,
):
    vmem = pl.BlockSpec(memory_space=pltpu.VMEM)
    smem = pl.BlockSpec(memory_space=pltpu.SMEM)
    dma = pltpu.SemaphoreType.DMA
    fw, fb, hg, hbg, dg = pl.pallas_call(
        kernel,
        out_shape=(
            jax.ShapeDtypeStruct((R, H), F32),
            jax.ShapeDtypeStruct((1, H), F32),
            jax.ShapeDtypeStruct((H, R), F32),
            jax.ShapeDtypeStruct((1, R), F32),
            jax.ShapeDtypeStruct((8, H), F32),
        ),
        in_specs=[smem] + [vmem] * 9,
        out_specs=(vmem,) * 5,
        scratch_shapes=[
            pltpu.VMEM((R + 16, H), BF),
            pltpu.VMEM((R + 16, R), BF),
            pltpu.VMEM((2, 2 * R, H), BF),
            pltpu.VMEM((8, WIDE), BF),
            pltpu.VMEM((2, NZ, 8, WIDE), BF),
            pltpu.VMEM((2 * R, WIDE), BF),
            pltpu.VMEM((32, 2, 8, R), BF),
            pltpu.VMEM((32, 2, 8, R), BF),
            pltpu.VMEM((2, R + 16, H), BF),
            pltpu.VMEM((16, R + 16, R), BF),
            pltpu.VMEM((NZ, 8, H), BF),
            pltpu.VMEM((NZ, 8, H), BF),
            pltpu.VMEM((2 * R, H), F32),
            pltpu.VMEM((NZ, 8, H), BF),
            pltpu.VMEM((NZ, 8, H), BF),
            pltpu.VMEM((4, 2 * R, R), BF),
            pltpu.VMEM((4, 2 * R, R), BF),
            pltpu.VMEM((4, 5, 8, H), BF),
            pltpu.VMEM((32, 5, 8, R), BF),
            pltpu.VMEM((NZ, 2, 8, R), BF),
            pltpu.VMEM((NZ, 2, 8, R), BF),
            pltpu.VMEM((NZ, 2, 8, R), BF),
            pltpu.VMEM((5, 8, R), BF),
            pltpu.VMEM((NZ, 8, R), BF),
            pltpu.VMEM((NZ, 8, R), BF),
            pltpu.VMEM((4, NZ, 2, 8, R), BF),
            pltpu.VMEM((32, 5, 8, R), BF),
            dma((16,)),
            dma((16,)),
        ],
        compiler_params=pltpu.CompilerParams(
            collective_id=0, has_side_effects=True, vmem_limit_bytes=40 * 1024 * 1024
        ),
    )(
        window,
        window.reshape(1, 64),
        inputs_store,
        jac_store,
        targets_store.T,
        first_weight,
        first_bias.reshape(1, H),
        hidden_weight,
        hidden_bias.reshape(1, R),
        decoder_weight,
    )
    return fw, fb.reshape(H), hg, hbg.reshape(R), dg


def solution(mesh):
    torus = Mesh(mesh.devices.reshape(NZ, 2, 2, 4, 2), ALL)
    return jax.shard_map(
        on_device,
        mesh=torus,
        in_specs=(
            P(),
            P(),
            P(None, ALL),
            P(None, ALL, None),
            P(),
            P(),
            P(None, MP),
            P(MP),
            P(ALL, None),
        ),
        out_specs=(P(), P(), P(None, MP), P(MP), P(ALL, None)),
        check_vma=False,
    )
```

```python
import jax
import jax.numpy as jnp
from jax import lax
from jax.experimental import pallas as pl
from jax.experimental.pallas import tpu as pltpu
from jax.sharding import Mesh
from jax.sharding import PartitionSpec as P

MESH = pl.DeviceIdType.MESH
DP = ("z", "xl", "c")
MP = ("y", "xh")
ALL = DP + MP
BF = jnp.bfloat16
F32 = jnp.float32

R = 128
H = 1024
NZ = 16
WIDE = H + R
VMEM_MOST = 67043328
NT = (((1,), (1,)), ((), ()))
TN = (((0,), (0,)), ((), ()))


def dot(a, b, dims=(((1,), (0,)), ((), ()))):
    return lax.dot_general(a, b, dims, preferred_element_type=F32)


def remote(src, dst, send, recv, to):
    return pltpu.make_async_remote_copy(
        src_ref=src, dst_ref=dst, send_sem=send, recv_sem=recv, device_id=to, device_id_type=MESH
    )


def each(n, body):
    def step(t, carry):
        body(t)
        return carry

    lax.fori_loop(0, n, step, 0)


def far_first(t):
    odd = t % 2
    return NZ // 2 + odd * ((t + 1) // 2) - (1 - odd) * (t // 2)


def kernel(
    ids_ref,
    idv_ref,
    xs_hbm,
    jac_hbm,
    tgt_hbm,
    w1_hbm,
    b1_hbm,
    hw_hbm,
    hb_hbm,
    dec_hbm,
    hall_hbm,
    fall_hbm,
    tile_hbm,
    dg_hbm,
    xs_ref,
    jac_ref,
    tgt_ref,
    w1_ref,
    b1_ref,
    hw_ref,
    hb_ref,
    dec_ref,
    ft,
    tsend,
    tfull,
    dsend,
    dblk,
    dmat,
    jsend,
    jbuf,
    pbuf,
    rbuf,
    gsend,
    grecv,
    gown,
    hsend,
    hrecv,
    qsend,
    qrecv,
    fsend,
    frecv,
    zsend,
    zrecv,
    zall,
    ysend,
    yrecv,
    yall,
    hall,
    fall,
    tile,
    dg_ref,
    sent,
    came,
    taken,
    put,
):
    z, xl, c = lax.axis_index("z"), lax.axis_index("xl"), lax.axis_index("c")
    y, xh = lax.axis_index("y"), lax.axis_index("xh")
    m = y * 2 + xh
    q = m * 2 + xl
    e = c * 2 + xl
    w = m * 4 + e
    b = c * NZ + z

    def at_z(zz):
        return {"z": zz}

    def at_zc(bb):
        return {"z": bb % NZ, "c": bb // NZ}

    def at_q(qq):
        return {"y": qq // 4, "xh": (qq // 2) % 2, "xl": qq % 2}

    def at_e(ee):
        return {"c": ee // 2, "xl": ee % 2}

    def at_w(ww):
        return {"y": ww // 8, "xh": (ww // 4) % 2, "c": (ww // 2) % 2, "xl": ww % 2}

    partner = {"c": 1 - c}
    barrier = pltpu.get_barrier_semaphore()

    def greet_z(t):
        zz = (z + far_first(t)) % NZ
        for cc in range(2):
            pl.semaphore_signal(barrier, inc=1, device_id={"z": zz, "c": cc}, device_id_type=MESH)

    def greet_w(t):
        pl.semaphore_signal(barrier, inc=1, device_id=at_w((w + t + 1) % 32), device_id_type=MESH)

    homes = (
        (jac_hbm, jac_ref),
        (tgt_hbm, tgt_ref),
        (dec_hbm, dec_ref),
        (xs_hbm, xs_ref),
        (w1_hbm, w1_ref),
        (hw_hbm, hw_ref),
        (b1_hbm, b1_ref),
        (hb_hbm, hb_ref),
    )
    loads = [pltpu.make_async_copy(a, v, taken.at[k]) for k, (a, v) in enumerate(homes)]
    for load in loads:
        load.start()
    each(NZ - 1, greet_z)
    each(31, greet_w)

    tfull[:, R + 16 :, :] = jnp.zeros((2, 2 * R - R - 16, H), BF)
    hot = (lax.broadcasted_iota(jnp.int32, (512, 64), 0) == idv_ref[...]).astype(F32).astype(BF)
    for load in loads[0:3]:
        load.wait()

    def pick(zz):
        for cc in range(2):
            for i in range(2):
                jsend[cc * NZ + zz, i] = jac_ref[ids_ref[zz * 4 + cc * 2 + i]]

    each(NZ, pick)
    dsend[:, 0:H] = dec_ref[...]
    dsend[:, H : H + 64] = dot(tgt_ref[...], hot).astype(BF)
    dsend[:, H + 64 :] = jnp.zeros((8, R - 64), BF)
    dblk[c, z] = dsend[...]
    jbuf[b] = jsend[b]
    for load in loads[3:]:
        load.wait()

    with jax.named_scope("barrier"):
        pl.semaphore_wait(barrier, 61)

    def tan_copy(peer, src):
        lanes = pl.ds(pl.multiple_of((src // 2) * R, R), R)
        dst = tfull.at[src % 2, pl.ds(0, R + 16), lanes]
        return remote(tsend, dst, sent.at[0], came.at[0], at_q(peer))

    def own_copy(d, k):
        return remote(
            dsend, dblk.at[c, z], sent.at[k], came.at[k], {"z": (z + d) % NZ}
        )

    def pass_copy(block, d):
        part = dblk.at[c, (z + block) % NZ]
        return remote(part, part, sent.at[2], came.at[2], {"z": (z + d) % NZ})

    def half_copy(side):
        return remote(dblk.at[side], dblk.at[side], sent.at[3], came.at[3], partner)

    def jac_copy(zz, cc):
        return remote(
            jsend.at[cc * NZ + zz], jbuf.at[b], sent.at[4], came.at[4], {"z": zz, "c": cc}
        )

    def start(n, me, copy):
        with jax.named_scope(copy.__name__ + "_start"):
            each(n - 1, lambda t: copy((me + t + 1) % n, me).start())

    def start_z(copy):
        with jax.named_scope(copy.__name__ + "_start"):
            each(NZ - 1, lambda t: copy((z + far_first(t)) % NZ, z).start())

    def recv(k, ref):
        with jax.named_scope(f"recv{k}"):
            remote(ref, ref, sent.at[k], came.at[k], partner).wait_recv()

    def left(k, ref):
        remote(ref, ref, sent.at[k], came.at[k], partner).wait_send()

    def start_jac(t):
        zz = (z + far_first(t)) % NZ
        for cc in range(2):
            jac_copy(zz, cc).start()

    for d in (5, 11):
        own_copy(d, 1).start()
    for d in (1, 15, 2, 14):
        own_copy(d, 16).start()
    each(5, start_jac)

    own = ids_ref[z * 4 + c * 2 + xl]
    x_hot = (lax.broadcasted_iota(jnp.int32, (16, 512), 1) == own).astype(F32).astype(BF)
    x_rows = dot(x_hot, xs_ref[...])
    w1 = w1_ref[...].astype(F32)
    b1 = b1_ref[...].astype(F32)
    b1 = jnp.concatenate([b1[k : k + 1] for k in range(8)], axis=1)
    first_pre = dot(x_rows.astype(BF), w1_ref[...]) + b1
    first_act = jnp.tanh(first_pre)[0:1]
    first_slope = 1.0 - first_act * first_act
    top16 = lax.broadcasted_iota(jnp.int32, (16, H), 0) == 0
    ft[0:R, :] = (first_slope * w1).astype(BF)
    ft[R : R + 16, :] = jnp.where(top16, jnp.broadcast_to(first_act, (16, H)), 0.0).astype(BF)
    lin = dot(ft[...], hw_ref[...])
    hidden_lin = lin[0:R]
    hidden_act = jnp.tanh(lin[R : R + 1] + hb_ref[...].astype(F32))
    hidden_slope = 1.0 - hidden_act * hidden_act
    top = lax.broadcasted_iota(jnp.int32, (16, R), 0) == 0
    tsend[0:R, :] = (hidden_slope * hidden_lin).astype(BF)
    tsend[R : R + 16, :] = jnp.where(top, jnp.broadcast_to(hidden_act, (16, R)), 0.0).astype(BF)
    start(16, q, tan_copy)
    mine = pl.ds(pl.multiple_of(m * R, R), R)
    tfull[xl, 0 : R + 16, mine] = tsend[...]

    recv(1, dblk.at[0, pl.ds(0, 2)])
    for d in (2, 14, 1, 15):
        for block in (5, 11):
            pass_copy(block, d).start()
    side = 1 - 2 * (z % 2)
    pass_copy(NZ - 5 * side, NZ + 3 * side).start()
    each(10, lambda t: start_jac(t + 5))
    jac_copy(z, 1 - c).start()
    recv(16, dblk.at[0, pl.ds(0, 4)])
    recv(2, dblk.at[0, pl.ds(0, 9)])
    half_copy(c).start()

    def unpack(side):
        rows = pl.ds(pl.multiple_of(side * R, R), R)
        dmat[rows, :] = dblk[side].astype(F32).reshape(R, WIDE).astype(BF)

    unpack(c)
    recv(0, rbuf.at[pl.ds(0, 15)])
    recv(4, jbuf.at[pl.ds(0, 31)])
    recv(3, dblk.at[0])
    unpack(1 - c)

    lane = lax.broadcasted_iota(jnp.int32, (2 * R, R), 1)
    tgt = dmat[:, H:].astype(F32)
    dec = dmat[:, 0:H]
    miss = []
    for i in range(2):
        want = jnp.sum(jnp.where(lane == z * 4 + c * 2 + i, tgt, 0.0), axis=1, keepdims=True)
        want = jnp.where(lane == 0, jnp.broadcast_to(want, (2 * R, R)), 0.0)
        stored = jbuf[:, i].astype(F32).reshape(2 * R, R)
        net = dot(dec, tfull[i], NT)
        miss_i = (net - jnp.concatenate([stored, want], axis=1)).astype(BF)
        miss.append(miss_i)
        pbuf[i] = dot(miss_i, dec, TN)[0 : R + 16].astype(BF)

    def back_copy(peer, src):
        lanes = pl.ds(pl.multiple_of((peer // 2) * R, R), R)
        return remote(
            pbuf.at[peer % 2, :, lanes], rbuf.at[src], sent.at[5], came.at[5], at_q(peer)
        )

    start(16, q, back_copy)

    gown[...] = dot(miss[0], tfull[0]) + dot(miss[1], tfull[1])
    theirs = gown[pl.ds(pl.multiple_of((1 - c) * R, R), R), :]
    gsend[...] = theirs.reshape(NZ, 8, H).astype(BF)
    remote(gsend, grecv, sent.at[6], came.at[6], partner).start()
    ours = gown[pl.ds(pl.multiple_of(c * R, R), R), :].reshape(NZ, 8, H)
    recv(6, grecv)
    hsend[...] = (ours + grecv[...].astype(F32)).astype(BF)

    def gz_copy(peer, src):
        return remote(
            hsend.at[peer], hrecv.at[src], sent.at[7], came.at[7], at_z(peer)
        )

    start_z(gz_copy)
    hrecv[z] = hsend[z]

    recv(5, rbuf.at[pl.ds(0, 15)])
    rbuf[q] = pbuf[xl, :, mine]
    back = jnp.sum(rbuf[...].astype(F32), axis=0)
    tan_back = back[0:R]
    act_back = back[R : R + 1]
    lin_round = (tan_back * hidden_slope).astype(BF)
    pre_back = act_back * hidden_slope - 2.0 * hidden_act * hidden_slope * jnp.sum(
        tan_back * hidden_lin, axis=0, keepdims=True
    )
    pre_round = jnp.where(top, jnp.broadcast_to(pre_back, (16, R)), 0.0).astype(BF)
    both = jnp.concatenate([lin_round, pre_round], axis=0)
    low = dot(both, hw_ref[...], NT)
    tan_lower = low[0:R]
    pre_lower = low[R : R + 1] * first_slope - 2.0 * first_act * first_slope * jnp.sum(
        tan_lower * w1, axis=0, keepdims=True
    )
    x_col = jnp.transpose(jnp.broadcast_to(x_rows[0:1], (R, R)))[:, 0:1]
    fw = x_col * pre_lower + tan_lower * first_slope
    place = lax.broadcasted_iota(jnp.int32, (8, H), 1) // R == m
    line = lax.broadcasted_iota(jnp.int32, (8, H), 0)
    pre_wide = jnp.concatenate([pre_back] * 8, axis=1)
    tail = jnp.where(line == 0, jnp.broadcast_to(pre_lower, (8, H)), 0.0)
    tail = tail + jnp.where((line == 1) & place, jnp.broadcast_to(pre_wide, (8, H)), 0.0)
    for k in range(4):
        fsend[k, 0:4] = fw[32 * k : 32 * k + 32].reshape(4, 8, H).astype(BF)
        fsend[k, 4] = tail.astype(BF)

    def f_copy(peer, src):
        lanes = pl.ds(pl.multiple_of((peer // 4) * R, R), R)
        return remote(
            fsend.at[peer % 4, :, :, lanes], frecv.at[src], sent.at[9], came.at[9], at_w(peer)
        )

    start(32, w, f_copy)
    frecv[w] = fsend[e, :, :, mine]

    qsend[...] = dot(ft[...], both, TN).astype(BF).reshape(4, 2 * R, R)

    def q_copy(peer, src):
        return remote(qsend.at[peer], qrecv.at[src], sent.at[8], came.at[8], at_e(peer))

    start(4, e, q_copy)
    qrecv[e] = qsend[e]

    recv(9, frecv.at[pl.ds(0, 31)])
    ysend[...] = jnp.sum(frecv[...].astype(F32), axis=0).astype(BF)
    for t in range(5):

        @pl.when(z != t)
        def _():
            remote(ysend.at[t], yrecv.at[z], sent.at[11], came.at[11], at_z(t)).start()

        @pl.when(z == t)
        def _():
            yrecv[z] = ysend[t]

    recv(8, qrecv.at[pl.ds(0, 3)])
    quarter = jnp.sum(qrecv[...].astype(F32), axis=0)
    zsend[...] = quarter.reshape(NZ, 2, 8, R).astype(BF)

    def zr_copy(peer, src):
        return remote(zsend.at[peer], zrecv.at[src], sent.at[10], came.at[10], at_z(peer))

    start_z(zr_copy)
    zrecv[z] = zsend[z]

    def y_copy(peer, src):
        return remote(yall.at[src], yall.at[src], sent.at[13], came.at[13], at_z(peer))

    @pl.when(z < 5)
    def _():
        recv(11, yrecv.at[pl.ds(0, 15)])
        yall[z] = jnp.sum(yrecv[...].astype(F32), axis=0).astype(BF)
        start_z(y_copy)

    recv(10, zrecv.at[pl.ds(0, 15)])
    zall[z] = jnp.sum(zrecv[...].astype(F32), axis=0).astype(BF)

    def zg_copy(peer, src):
        return remote(zall.at[src], zall.at[src], sent.at[12], came.at[12], at_z(peer))

    start_z(zg_copy)

    recv(7, hrecv.at[pl.ds(0, 15)])
    dg_ref[...] = jnp.sum(hrecv[...].astype(F32), axis=0)
    outs = (
        pltpu.make_async_copy(dg_ref, dg_hbm, put.at[0]),
        pltpu.make_async_copy(tile, tile_hbm, put.at[1]),
        pltpu.make_async_copy(hall, hall_hbm, put.at[2]),
        pltpu.make_async_copy(fall, fall_hbm, put.at[3]),
    )
    outs[0].start()

    @pl.when(z < 5)
    def _():
        recv(13, yall.at[pl.ds(0, 4)])

    @pl.when(z >= 5)
    def _():
        recv(13, yall.at[pl.ds(0, 5)])

    def fa_copy(peer, src):
        return remote(yall.at[pl.ds(0, 5)], fall.at[src], sent.at[15], came.at[15], at_w(peer))

    start(32, w, fa_copy)

    recv(12, zall.at[pl.ds(0, 15)])

    def h_copy(peer, src):
        return remote(zall, hall.at[src], sent.at[14], came.at[14], at_e(peer))

    start(4, e, h_copy)
    hall[e] = zall[...]
    fall[w] = yall[0:5]
    tile[...] = yall[4]
    outs[1].start()
    recv(14, hall.at[pl.ds(0, 3)])
    outs[2].start()
    recv(15, fall.at[pl.ds(0, 31)])
    outs[3].start()

    left(0, rbuf.at[pl.ds(0, 15)])
    left(1, dblk.at[0, pl.ds(0, 2)])
    left(16, dblk.at[0, pl.ds(0, 4)])
    left(2, dblk.at[0, pl.ds(0, 9)])
    left(3, dblk.at[0])
    left(4, jbuf.at[pl.ds(0, 31)])
    left(5, rbuf.at[pl.ds(0, 15)])
    left(6, grecv)
    left(7, hrecv.at[pl.ds(0, 15)])
    left(8, qrecv.at[pl.ds(0, 3)])
    left(9, frecv.at[pl.ds(0, 31)])
    left(10, zrecv.at[pl.ds(0, 15)])

    @pl.when(z < 5)
    def _():
        left(11, yall.at[pl.ds(0, 4)])
        left(13, yrecv.at[pl.ds(0, 15)])

    @pl.when(z >= 5)
    def _():
        left(11, yall.at[pl.ds(0, 5)])

    left(12, zrecv.at[pl.ds(0, 15)])
    left(14, hall.at[pl.ds(0, 3)])
    left(15, fall.at[pl.ds(0, 31)])
    for out in outs:
        out.wait()


def unfold(
    hall_hbm,
    fall_hbm,
    tile_hbm,
    dg_hbm,
    fw_hbm,
    fb_hbm,
    hg_hbm,
    hb_hbm,
    dgo_hbm,
    hall,
    fall,
    tile,
    dg,
    fw,
    fb,
    hg,
    hb,
    got,
    put,
):
    ins = (
        pltpu.make_async_copy(hall_hbm, hall, got.at[0]),
        pltpu.make_async_copy(fall_hbm, fall, got.at[1]),
        pltpu.make_async_copy(dg_hbm, dg, got.at[2]),
        pltpu.make_async_copy(tile_hbm, tile, got.at[3]),
    )
    outs = (
        pltpu.make_async_copy(hg, hg_hbm, put.at[0]),
        pltpu.make_async_copy(fw, fw_hbm, put.at[1]),
        pltpu.make_async_copy(dg, dgo_hbm, put.at[2]),
        pltpu.make_async_copy(hb, hb_hbm, put.at[3]),
        pltpu.make_async_copy(fb, fb_hbm, put.at[4]),
    )
    for copy in ins:
        copy.start()
    ins[0].wait()
    hg[...] = hall[...].astype(F32).reshape(H, R)
    outs[0].start()
    ins[1].wait()
    for mm in range(8):
        for ee in range(4):
            piece = fall[4 * mm + ee].astype(F32)
            fw[32 * ee : 32 * ee + 32, R * mm : R * mm + R] = piece[0:4].reshape(32, R)
            if ee == 0:
                fb[mm : mm + 1, :] = piece[4, 0:1]
    outs[1].start()
    outs[4].start()
    ins[2].wait()
    outs[2].start()
    ins[3].wait()
    hb[...] = tile[...].astype(F32)[1:2]
    outs[3].start()
    for copy in outs:
        copy.wait()


def on_device(
    inputs_store,
    window,
    targets_store,
    jac_store,
    first_weight,
    first_bias,
    hidden_weight,
    hidden_bias,
    decoder_weight,
):
    vmem = pl.BlockSpec(memory_space=pltpu.VMEM)
    smem = pl.BlockSpec(memory_space=pltpu.SMEM)
    hbm = pl.BlockSpec(memory_space=pltpu.HBM)
    dma = pltpu.SemaphoreType.DMA
    hall = jax.ShapeDtypeStruct((4, NZ, 2, 8, R), BF)
    fall = jax.ShapeDtypeStruct((32, 5, 8, R), BF)
    tile = jax.ShapeDtypeStruct((8, R), BF)
    dg = jax.ShapeDtypeStruct((8, H), F32)
    raw = (hall, fall, tile, dg)
    parts = pl.pallas_call(
        kernel,
        out_shape=raw,
        in_specs=[smem, vmem] + [hbm] * 8,
        out_specs=(hbm,) * 4,
        scratch_shapes=[
            pltpu.VMEM((512, R), BF),
            pltpu.VMEM((512, 8, R), BF),
            pltpu.VMEM((8, 512), BF),
            pltpu.VMEM((R, H), BF),
            pltpu.VMEM((8, R), BF),
            pltpu.VMEM((H, R), BF),
            pltpu.VMEM((1, R), BF),
            pltpu.VMEM((8, H), BF),
            pltpu.VMEM((R + 16, H), BF),
            pltpu.VMEM((R + 16, R), BF),
            pltpu.VMEM((2, 2 * R, H), BF),
            pltpu.VMEM((8, WIDE), BF),
            pltpu.VMEM((2, NZ, 8, WIDE), BF),
            pltpu.VMEM((2 * R, WIDE), BF),
            pltpu.VMEM((32, 2, 8, R), BF),
            pltpu.VMEM((32, 2, 8, R), BF),
            pltpu.VMEM((2, R + 16, H), BF),
            pltpu.VMEM((16, R + 16, R), BF),
            pltpu.VMEM((NZ, 8, H), BF),
            pltpu.VMEM((NZ, 8, H), BF),
            pltpu.VMEM((2 * R, H), F32),
            pltpu.VMEM((NZ, 8, H), BF),
            pltpu.VMEM((NZ, 8, H), BF),
            pltpu.VMEM((4, 2 * R, R), BF),
            pltpu.VMEM((4, 2 * R, R), BF),
            pltpu.VMEM((4, 5, 8, H), BF),
            pltpu.VMEM((32, 5, 8, R), BF),
            pltpu.VMEM((NZ, 2, 8, R), BF),
            pltpu.VMEM((NZ, 2, 8, R), BF),
            pltpu.VMEM((NZ, 2, 8, R), BF),
            pltpu.VMEM((5, 8, R), BF),
            pltpu.VMEM((NZ, 8, R), BF),
            pltpu.VMEM((NZ, 8, R), BF),
            pltpu.VMEM((4, NZ, 2, 8, R), BF),
            pltpu.VMEM((32, 5, 8, R), BF),
            pltpu.VMEM((8, R), BF),
            pltpu.VMEM((8, H), F32),
            dma((17,)),
            dma((17,)),
            dma((8,)),
            dma((4,)),
        ],
        compiler_params=pltpu.CompilerParams(
            collective_id=0, has_side_effects=True, vmem_limit_bytes=VMEM_MOST
        ),
    )(
        window,
        window.reshape(1, 64),
        inputs_store,
        jac_store,
        targets_store.T,
        first_weight,
        first_bias.reshape(8, R),
        hidden_weight,
        hidden_bias.reshape(1, R),
        decoder_weight,
    )
    final = (
        jax.ShapeDtypeStruct((R, H), F32),
        jax.ShapeDtypeStruct((8, R), F32),
        jax.ShapeDtypeStruct((H, R), F32),
        jax.ShapeDtypeStruct((1, R), F32),
        dg,
    )
    fw, fb, hg, hb, dgo = pl.pallas_call(
        unfold,
        out_shape=final,
        in_specs=[hbm] * 4,
        out_specs=(hbm,) * 5,
        scratch_shapes=[pltpu.VMEM(a.shape, a.dtype) for a in raw + final[0:4]]
        + [dma((4,)), dma((5,))],
        compiler_params=pltpu.CompilerParams(vmem_limit_bytes=VMEM_MOST),
    )(*parts)
    return fw, fb.reshape(H), hg, hb.reshape(R), dgo


def solution(mesh):
    torus = Mesh(mesh.devices.reshape(NZ, 2, 2, 4, 2), ALL)
    return jax.shard_map(
        on_device,
        mesh=torus,
        in_specs=(
            P(),
            P(),
            P(None, ALL),
            P(None, ALL, None),
            P(),
            P(),
            P(None, MP),
            P(MP),
            P(ALL, None),
        ),
        out_specs=(P(), P(), P(None, MP), P(MP), P(ALL, None)),
        check_vma=False,
    )
```

```python
import jax
import jax.numpy as jnp
from jax import lax
from jax.experimental import pallas as pl
from jax.experimental.pallas import tpu as pltpu
from jax.sharding import Mesh
from jax.sharding import PartitionSpec as P

MESH = pl.DeviceIdType.MESH
DP = ("z", "xl", "c")
MP = ("y", "xh")
ALL = DP + MP
BF = jnp.bfloat16
F32 = jnp.float32

R = 128
H = 1024
NZ = 16
WIDE = H + R
VMEM_MOST = 67043328
NT = (((1,), (1,)), ((), ()))
TN = (((0,), (0,)), ((), ()))


def dot(a, b, dims=(((1,), (0,)), ((), ()))):
    return lax.dot_general(a, b, dims, preferred_element_type=F32)


def remote(src, dst, send, recv, to):
    return pltpu.make_async_remote_copy(
        src_ref=src, dst_ref=dst, send_sem=send, recv_sem=recv, device_id=to, device_id_type=MESH
    )


def each(n, body):
    def step(t, carry):
        body(t)
        return carry

    lax.fori_loop(0, n, step, 0)


def wrap(v, n):
    return jnp.where(v >= n, v - n, v)


FAR_FIRST = (8, 7, 9, 6, 10, 5, 11, 4, 12, 3, 13, 2, 14, 1, 15)
PLANE = sorted(
    (
        (dy, dh, dl)
        for dy in range(4)
        for dh in range(2)
        for dl in range(2)
        if dy + dh + dl > 0
    ),
    key=lambda d: -(min(d[0], 4 - d[0]) + (2 if d[1:] == (1, 0) else max(d[1:]))),
)


def kernel(
    ids_ref,
    idv_ref,
    xs_hbm,
    jac_hbm,
    tgt_hbm,
    w1_hbm,
    b1_hbm,
    hw_hbm,
    hb_hbm,
    dec_hbm,
    hall_hbm,
    fall_hbm,
    tile_hbm,
    dg_hbm,
    xs_ref,
    jac_ref,
    tgt_ref,
    w1_ref,
    b1_ref,
    hw_ref,
    hb_ref,
    dec_ref,
    ft,
    tsend,
    tfull,
    dsend,
    dblk,
    dmat,
    jsend,
    jbuf,
    net,
    tbytes,
    pbuf,
    rbuf,
    gsend,
    grecv,
    gown,
    hsend,
    hrecv,
    qsend,
    qpart,
    qsum,
    qrecv,
    fsend,
    fpart,
    fsum,
    frecv,
    zsend,
    zrecv,
    zall,
    ysend,
    yrecv,
    yall,
    hall,
    fall,
    tile,
    dg_ref,
    sent,
    came,
    taken,
    put,
):
    z, xl, c = lax.axis_index("z"), lax.axis_index("xl"), lax.axis_index("c")
    y, xh = lax.axis_index("y"), lax.axis_index("xh")
    m = y * 2 + xh
    q = m * 2 + xl
    b = c * NZ + z

    def plane(d):
        dy, dh, dl = d
        yy = wrap(y + dy, 4)
        hh = 1 - xh if dh else xh
        ll = 1 - xl if dl else xl
        return (yy * 2 + hh) * 2 + ll, {"y": yy, "xh": hh, "xl": ll}

    partner = {"c": 1 - c}
    barrier = pltpu.get_barrier_semaphore()

    homes = (
        (jac_hbm, jac_ref),
        (tgt_hbm, tgt_ref),
        (dec_hbm, dec_ref),
        (xs_hbm, xs_ref),
        (w1_hbm, w1_ref),
        (hw_hbm, hw_ref),
        (b1_hbm, b1_ref),
        (hb_hbm, hb_ref),
    )
    loads = [pltpu.make_async_copy(a, v, taken.at[k]) for k, (a, v) in enumerate(homes)]
    for load in loads:
        load.start()
    def greet(to):
        pl.semaphore_signal(barrier, inc=1, device_id=to, device_id_type=MESH)

    for d in FAR_FIRST:
        for cc in range(2):
            greet({"z": wrap(z + d, NZ), "c": cc})
    for d in PLANE:
        greet(plane(d)[1])
    greet(partner)

    tfull[:, R + 16 :, :] = jnp.zeros((2, 2 * R - R - 16, H), BF)
    hot = (lax.broadcasted_iota(jnp.int32, (512, 64), 0) == idv_ref[...]).astype(F32).astype(BF)
    for load in loads[0:3]:
        load.wait()

    def pick(zz):
        for cc in range(2):
            for i in range(2):
                jsend[cc * NZ + zz, i] = jac_ref[ids_ref[zz * 4 + cc * 2 + i]]

    each(NZ, pick)
    dsend[:, 0:H] = dec_ref[...]
    dsend[:, H : H + 64] = dot(tgt_ref[...], hot).astype(BF)
    dsend[:, H + 64 :] = jnp.zeros((8, R - 64), BF)
    dblk[c, z] = dsend[...]
    jbuf[b] = jsend[b]
    for load in loads[3:]:
        load.wait()

    with jax.named_scope("barrier"):
        pl.semaphore_wait(barrier, 46)

    mine = pl.ds(pl.multiple_of(m * R, R), R)

    def tan_copy(to):
        return remote(
            tsend, tfull.at[xl, pl.ds(0, R + 16), mine], sent.at[0], came.at[0], to
        )

    def own_copy(d, k):
        return remote(
            dsend, dblk.at[c, z], sent.at[k], came.at[k], {"z": wrap(z + d, NZ)}
        )

    def pass_copy(block, d):
        part = dblk.at[c, wrap(z + block, NZ)]
        return remote(part, part, sent.at[2], came.at[2], {"z": wrap(z + d, NZ)})

    def half_copy(side):
        return remote(dblk.at[side], dblk.at[side], sent.at[3], came.at[3], partner)

    def jac_copy(zz, cc):
        return remote(
            jsend.at[cc * NZ + zz], jbuf.at[b], sent.at[4], came.at[4], {"z": zz, "c": cc}
        )

    def start_jac(ds):
        for d in ds:
            for cc in range(2):
                jac_copy(wrap(z + d, NZ), cc).start()

    def start_z(copy):
        for d in FAR_FIRST:
            copy(wrap(z + d, NZ)).start()

    xside = {"xl": 1 - xl}

    def recv(k, ref):
        with jax.named_scope(f"recv{k}"):
            remote(ref, ref, sent.at[k], came.at[k], partner).wait_recv()

    def left(k, ref):
        remote(ref, ref, sent.at[k], came.at[k], partner).wait_send()

    for d in (5, 11):
        own_copy(d, 1).start()
    for d in (1, 15, 2, 14):
        own_copy(d, 16).start()
    start_jac(FAR_FIRST[0:5])

    own = ids_ref[z * 4 + c * 2 + xl]
    x_hot = (lax.broadcasted_iota(jnp.int32, (16, 512), 1) == own).astype(F32).astype(BF)
    x_rows = dot(x_hot, xs_ref[...])
    w1 = w1_ref[...].astype(F32)
    b1 = b1_ref[...].astype(F32)
    b1 = jnp.concatenate([b1[k : k + 1] for k in range(8)], axis=1)
    first_pre = dot(x_rows.astype(BF), w1_ref[...]) + b1
    first_act = jnp.tanh(first_pre)[0:1]
    first_slope = 1.0 - first_act * first_act
    top16 = lax.broadcasted_iota(jnp.int32, (16, H), 0) == 0
    ft[0:R, :] = (first_slope * w1).astype(BF)
    ft[R : R + 16, :] = jnp.where(top16, jnp.broadcast_to(first_act, (16, H)), 0.0).astype(BF)
    lin = dot(ft[...], hw_ref[...])
    hidden_lin = lin[0:R]
    hidden_act = jnp.tanh(lin[R : R + 1] + hb_ref[...].astype(F32))
    hidden_slope = 1.0 - hidden_act * hidden_act
    top = lax.broadcasted_iota(jnp.int32, (16, R), 0) == 0
    tsend[0:R, :] = (hidden_slope * hidden_lin).astype(BF)
    tsend[R : R + 16, :] = jnp.where(top, jnp.broadcast_to(hidden_act, (16, R)), 0.0).astype(BF)
    for d in PLANE:
        tan_copy(plane(d)[1]).start()
    tfull[xl, 0 : R + 16, mine] = tsend[...]

    recv(1, dblk.at[0, pl.ds(0, 2)])
    for d in (2, 14, 1, 15):
        for block in (5, 11):
            pass_copy(block, d).start()
    odd = z % 2
    pass_copy(11 - 6 * odd, 3 + 10 * odd).start()
    start_jac(FAR_FIRST[5:])
    jac_copy(z, 1 - c).start()
    recv(16, dblk.at[0, pl.ds(0, 4)])
    recv(2, dblk.at[0, pl.ds(0, 9)])
    half_copy(c).start()

    def unpack(side):
        rows = pl.ds(pl.multiple_of(side * R, R), R)
        dmat[rows, :] = dblk[side].astype(F32).reshape(R, WIDE).astype(BF)

    unpack(c)
    recv(0, tbytes.at[pl.ds(0, 15)])
    recv(3, dblk.at[0])
    unpack(1 - c)

    lane = lax.broadcasted_iota(jnp.int32, (2 * R, R), 1)
    tgt = dmat[:, H:].astype(F32)
    dec = dmat[:, 0:H]
    for i in range(2):
        want = jnp.sum(jnp.where(lane == z * 4 + c * 2 + i, tgt, 0.0), axis=1, keepdims=True)
        want = jnp.where(lane == 0, jnp.broadcast_to(want, (2 * R, R)), 0.0)
        out = dot(dec, tfull[i], NT)
        net[i, :, 0:R] = out[:, 0:R]
        net[i, :, R:] = out[:, R:] - want
    recv(4, jbuf.at[pl.ds(0, 31)])
    miss = []
    for i in range(2):
        stored = jbuf[:, i].astype(F32).reshape(2 * R, R)
        miss_i = jnp.concatenate([net[i, :, 0:R] - stored, net[i, :, R:]], axis=1).astype(BF)
        miss.append(miss_i)
        back_i = dot(miss_i, dec, TN)[0 : R + 8]
        for k in range(8):
            part = back_i[:, R * k : R * k + R]
            pbuf[2 * k + i] = part.reshape(17, 8, R).astype(BF)
    for d in PLANE:
        peer, to = plane(d)
        remote(pbuf.at[peer], rbuf.at[q], sent.at[5], came.at[5], to).start()

    gown[...] = dot(miss[0], tfull[0]) + dot(miss[1], tfull[1])
    theirs = gown[pl.ds(pl.multiple_of((1 - c) * R, R), R), :]
    gsend[...] = theirs.reshape(NZ, 8, H).astype(BF)
    remote(gsend, grecv, sent.at[6], came.at[6], partner).start()
    ours = gown[pl.ds(pl.multiple_of(c * R, R), R), :].reshape(NZ, 8, H)
    recv(6, grecv)
    hsend[...] = (ours + grecv[...].astype(F32)).astype(BF)

    def gz_copy(peer):
        return remote(hsend.at[peer], hrecv.at[z], sent.at[7], came.at[7], {"z": peer})

    start_z(gz_copy)
    hrecv[z] = hsend[z]

    recv(5, rbuf.at[pl.ds(0, 15)])
    rbuf[q] = pbuf[q]
    back = jnp.sum(rbuf[...].astype(F32), axis=0).reshape(R + 8, R)
    tan_back = back[0:R]
    act_back = back[R : R + 1]
    lin_round = (tan_back * hidden_slope).astype(BF)
    pre_back = act_back * hidden_slope - 2.0 * hidden_act * hidden_slope * jnp.sum(
        tan_back * hidden_lin, axis=0, keepdims=True
    )
    pre_round = jnp.where(top, jnp.broadcast_to(pre_back, (16, R)), 0.0).astype(BF)
    both = jnp.concatenate([lin_round, pre_round], axis=0)
    low = dot(both, hw_ref[...], NT)
    tan_lower = low[0:R]
    pre_lower = low[R : R + 1] * first_slope - 2.0 * first_act * first_slope * jnp.sum(
        tan_lower * w1, axis=0, keepdims=True
    )
    x_col = jnp.transpose(jnp.broadcast_to(x_rows[0:1], (R, R)))[:, 0:1]
    fw = x_col * pre_lower + tan_lower * first_slope
    place = lax.broadcasted_iota(jnp.int32, (8, H), 1) // R == m
    line = lax.broadcasted_iota(jnp.int32, (8, H), 0)
    pre_wide = jnp.concatenate([pre_back] * 8, axis=1)
    tail = jnp.where(line == 0, jnp.broadcast_to(pre_lower, (8, H)), 0.0)
    tail = tail + jnp.where((line == 1) & place, jnp.broadcast_to(pre_wide, (8, H)), 0.0)
    for cc in range(2):
        for k in range(16):
            r0 = 64 * cc + 32 * (k % 2)
            l0 = R * (k // 2)
            fsend[cc, k, 0:4] = fw[r0 : r0 + 32, l0 : l0 + R].reshape(4, 8, R).astype(BF)
            fsend[cc, k, 4] = tail[:, l0 : l0 + R].astype(BF)
    remote(fsend.at[1 - c], fpart, sent.at[9], came.at[9], partner).start()
    qsend[...] = dot(ft[...], both, TN).astype(BF).reshape(2, 4 * R, R)
    remote(qsend.at[1 - c], qpart, sent.at[8], came.at[8], partner).start()
    recv(9, fpart)
    fsum[...] = (fsend[c].astype(F32) + fpart[...].astype(F32)).astype(BF)
    for d in PLANE:
        peer, to = plane(d)
        remote(fsum.at[peer], frecv.at[q], sent.at[17], came.at[17], to).start()
    frecv[q] = fsum[q]
    recv(8, qpart)
    halves = qsend[c].astype(F32) + qpart[...].astype(F32)
    qsum[...] = halves.astype(BF).reshape(2, 2 * R, R)
    remote(qsum.at[1 - xl], qrecv, sent.at[18], came.at[18], xside).start()

    recv(17, frecv.at[pl.ds(0, 15)])
    ysend[...] = jnp.sum(frecv[...].astype(F32), axis=0).astype(BF)
    for t in range(5):

        @pl.when(z != t)
        def _():
            remote(ysend.at[t], yrecv.at[z], sent.at[11], came.at[11], {"z": t}).start()

        @pl.when(z == t)
        def _():
            yrecv[z] = ysend[t]

    recv(18, qrecv)
    quarter = qsum[xl].astype(F32) + qrecv[...].astype(F32)
    zsend[...] = quarter.reshape(NZ, 2, 8, R).astype(BF)

    def zr_copy(peer):
        return remote(zsend.at[peer], zrecv.at[z], sent.at[10], came.at[10], {"z": peer})

    start_z(zr_copy)
    zrecv[z] = zsend[z]

    def y_copy(peer):
        return remote(yall.at[z], yall.at[z], sent.at[13], came.at[13], {"z": peer})

    @pl.when(z < 5)
    def _():
        recv(11, yrecv.at[pl.ds(0, 15)])
        yall[z] = jnp.sum(yrecv[...].astype(F32), axis=0).astype(BF)
        start_z(y_copy)

    recv(10, zrecv.at[pl.ds(0, 15)])
    zall[z] = jnp.sum(zrecv[...].astype(F32), axis=0).astype(BF)

    def zg_copy(peer):
        return remote(zall.at[z], zall.at[z], sent.at[12], came.at[12], {"z": peer})

    start_z(zg_copy)

    recv(7, hrecv.at[pl.ds(0, 15)])
    dg_ref[...] = jnp.sum(hrecv[...].astype(F32), axis=0)
    outs = (
        pltpu.make_async_copy(dg_ref, dg_hbm, put.at[0]),
        pltpu.make_async_copy(tile, tile_hbm, put.at[1]),
        pltpu.make_async_copy(hall, hall_hbm, put.at[2]),
        pltpu.make_async_copy(fall, fall_hbm, put.at[3]),
    )
    outs[0].start()

    @pl.when(z < 5)
    def _():
        recv(13, yall.at[pl.ds(0, 4)])

    @pl.when(z >= 5)
    def _():
        recv(13, yall.at[pl.ds(0, 5)])

    for d in PLANE:
        remote(
            yall.at[pl.ds(0, 5)], fall.at[c, q], sent.at[15], came.at[15], plane(d)[1]
        ).start()
    fall[c, q] = yall[0:5]
    tile[...] = yall[4]
    outs[1].start()
    recv(12, zall.at[pl.ds(0, 15)])
    remote(zall, hall.at[c, xl], sent.at[14], came.at[14], xside).start()
    hall[c, xl] = zall[...]
    recv(15, fall.at[0, pl.ds(0, 15)])
    remote(fall.at[c], fall.at[c], sent.at[19], came.at[19], partner).start()
    recv(14, zall)
    remote(hall.at[c], hall.at[c], sent.at[20], came.at[20], partner).start()
    recv(19, fall.at[0])
    outs[3].start()
    recv(20, hall.at[0])
    outs[2].start()

    left(0, tbytes.at[pl.ds(0, 15)])
    left(1, dblk.at[0, pl.ds(0, 2)])
    left(16, dblk.at[0, pl.ds(0, 4)])
    left(2, dblk.at[0, pl.ds(0, 9)])
    left(3, dblk.at[0])
    left(4, jbuf.at[pl.ds(0, 31)])
    left(5, rbuf.at[pl.ds(0, 15)])
    left(6, grecv)
    left(7, hrecv.at[pl.ds(0, 15)])
    left(8, qpart)
    left(9, fpart)
    left(17, frecv.at[pl.ds(0, 15)])
    left(18, qrecv)
    left(10, zrecv.at[pl.ds(0, 15)])

    @pl.when(z < 5)
    def _():
        left(11, yall.at[pl.ds(0, 4)])
        left(13, yrecv.at[pl.ds(0, 15)])

    @pl.when(z >= 5)
    def _():
        left(11, yall.at[pl.ds(0, 5)])

    left(12, zrecv.at[pl.ds(0, 15)])
    left(14, zall)
    left(15, fall.at[0, pl.ds(0, 15)])
    left(19, fall.at[0])
    left(20, hall.at[0])
    for out in outs:
        out.wait()


def unfold(
    hall_hbm,
    fall_hbm,
    tile_hbm,
    dg_hbm,
    fw_hbm,
    fb_hbm,
    hg_hbm,
    hb_hbm,
    dgo_hbm,
    hall,
    fall,
    tile,
    dg,
    fw,
    fb,
    hg,
    hb,
    got,
    put,
):
    ins = (
        pltpu.make_async_copy(hall_hbm, hall, got.at[0]),
        pltpu.make_async_copy(fall_hbm, fall, got.at[1]),
        pltpu.make_async_copy(dg_hbm, dg, got.at[2]),
        pltpu.make_async_copy(tile_hbm, tile, got.at[3]),
    )
    outs = (
        pltpu.make_async_copy(hg, hg_hbm, put.at[0]),
        pltpu.make_async_copy(fw, fw_hbm, put.at[1]),
        pltpu.make_async_copy(dg, dgo_hbm, put.at[2]),
        pltpu.make_async_copy(hb, hb_hbm, put.at[3]),
        pltpu.make_async_copy(fb, fb_hbm, put.at[4]),
    )
    for copy in ins:
        copy.start()
    ins[0].wait()
    hg[...] = hall[...].astype(F32).reshape(H, R)
    outs[0].start()
    ins[1].wait()
    for mm in range(8):
        for ee in range(4):
            piece = fall[ee // 2, 2 * mm + ee % 2].astype(F32)
            fw[32 * ee : 32 * ee + 32, R * mm : R * mm + R] = piece[0:4].reshape(32, R)
            if ee == 0:
                fb[mm : mm + 1, :] = piece[4, 0:1]
    outs[1].start()
    outs[4].start()
    ins[2].wait()
    outs[2].start()
    ins[3].wait()
    hb[...] = tile[...].astype(F32)[1:2]
    outs[3].start()
    for copy in outs:
        copy.wait()


def on_device(
    inputs_store,
    window,
    targets_store,
    jac_store,
    first_weight,
    first_bias,
    hidden_weight,
    hidden_bias,
    decoder_weight,
):
    vmem = pl.BlockSpec(memory_space=pltpu.VMEM)
    smem = pl.BlockSpec(memory_space=pltpu.SMEM)
    hbm = pl.BlockSpec(memory_space=pltpu.HBM)
    dma = pltpu.SemaphoreType.DMA
    hall = jax.ShapeDtypeStruct((2, 2, NZ, 2, 8, R), BF)
    fall = jax.ShapeDtypeStruct((2, 16, 5, 8, R), BF)
    tile = jax.ShapeDtypeStruct((8, R), BF)
    dg = jax.ShapeDtypeStruct((8, H), F32)
    raw = (hall, fall, tile, dg)
    parts = pl.pallas_call(
        kernel,
        out_shape=raw,
        in_specs=[smem, vmem] + [hbm] * 8,
        out_specs=(hbm,) * 4,
        scratch_shapes=[
            pltpu.VMEM((512, R), BF),
            pltpu.VMEM((512, 8, R), BF),
            pltpu.VMEM((8, 512), BF),
            pltpu.VMEM((R, H), BF),
            pltpu.VMEM((8, R), BF),
            pltpu.VMEM((H, R), BF),
            pltpu.VMEM((1, R), BF),
            pltpu.VMEM((8, H), BF),
            pltpu.VMEM((R + 16, H), BF),
            pltpu.VMEM((R + 16, R), BF),
            pltpu.VMEM((2, 2 * R, H), BF),
            pltpu.VMEM((8, WIDE), BF),
            pltpu.VMEM((2, NZ, 8, WIDE), BF),
            pltpu.VMEM((2 * R, WIDE), BF),
            pltpu.VMEM((32, 2, 8, R), BF),
            pltpu.VMEM((32, 2, 8, R), BF),
            pltpu.VMEM((2, 2 * R, 2 * R), F32),
            pltpu.VMEM((16, R + 16, R), BF),
            pltpu.VMEM((16, 17, 8, R), BF),
            pltpu.VMEM((16, 17, 8, R), BF),
            pltpu.VMEM((NZ, 8, H), BF),
            pltpu.VMEM((NZ, 8, H), BF),
            pltpu.VMEM((2 * R, H), F32),
            pltpu.VMEM((NZ, 8, H), BF),
            pltpu.VMEM((NZ, 8, H), BF),
            pltpu.VMEM((2, 4 * R, R), BF),
            pltpu.VMEM((4 * R, R), BF),
            pltpu.VMEM((2, 2 * R, R), BF),
            pltpu.VMEM((2 * R, R), BF),
            pltpu.VMEM((2, 16, 5, 8, R), BF),
            pltpu.VMEM((16, 5, 8, R), BF),
            pltpu.VMEM((16, 5, 8, R), BF),
            pltpu.VMEM((16, 5, 8, R), BF),
            pltpu.VMEM((NZ, 2, 8, R), BF),
            pltpu.VMEM((NZ, 2, 8, R), BF),
            pltpu.VMEM((NZ, 2, 8, R), BF),
            pltpu.VMEM((5, 8, R), BF),
            pltpu.VMEM((NZ, 8, R), BF),
            pltpu.VMEM((NZ, 8, R), BF),
            pltpu.VMEM((2, 2, NZ, 2, 8, R), BF),
            pltpu.VMEM((2, 16, 5, 8, R), BF),
            pltpu.VMEM((8, R), BF),
            pltpu.VMEM((8, H), F32),
            dma((21,)),
            dma((21,)),
            dma((8,)),
            dma((4,)),
        ],
        compiler_params=pltpu.CompilerParams(
            collective_id=0, has_side_effects=True, vmem_limit_bytes=VMEM_MOST
        ),
    )(
        window,
        window.reshape(1, 64),
        inputs_store,
        jac_store,
        targets_store.T,
        first_weight,
        first_bias.reshape(8, R),
        hidden_weight,
        hidden_bias.reshape(1, R),
        decoder_weight,
    )
    final = (
        jax.ShapeDtypeStruct((R, H), F32),
        jax.ShapeDtypeStruct((8, R), F32),
        jax.ShapeDtypeStruct((H, R), F32),
        jax.ShapeDtypeStruct((1, R), F32),
        dg,
    )
    fw, fb, hg, hb, dgo = pl.pallas_call(
        unfold,
        out_shape=final,
        in_specs=[hbm] * 4,
        out_specs=(hbm,) * 5,
        scratch_shapes=[pltpu.VMEM(a.shape, a.dtype) for a in raw + final[0:4]]
        + [dma((4,)), dma((5,))],
        compiler_params=pltpu.CompilerParams(vmem_limit_bytes=VMEM_MOST),
    )(*parts)
    return fw, fb.reshape(H), hg, hb.reshape(R), dgo


def solution(mesh):
    torus = Mesh(mesh.devices.reshape(NZ, 2, 2, 4, 2), ALL)
    return jax.shard_map(
        on_device,
        mesh=torus,
        in_specs=(
            P(),
            P(),
            P(None, ALL),
            P(None, ALL, None),
            P(),
            P(),
            P(None, MP),
            P(MP),
            P(ALL, None),
        ),
        out_specs=(P(), P(), P(None, MP), P(MP), P(ALL, None)),
        check_vma=False,
    )
```

```python
import jax
import jax.numpy as jnp
from jax import lax
from jax.experimental import pallas as pl
from jax.experimental.pallas import tpu as pltpu
from jax.sharding import Mesh
from jax.sharding import PartitionSpec as P

MESH = pl.DeviceIdType.MESH
DP = ("z", "xl", "c")
MP = ("y", "xh")
ALL = DP + MP
BF = jnp.bfloat16
F32 = jnp.float32

R = 128
H = 1024
NZ = 16
WIDE = H + R
VMEM_MOST = 67043328
NT = (((1,), (1,)), ((), ()))
TN = (((0,), (0,)), ((), ()))


def dot(a, b, dims=(((1,), (0,)), ((), ()))):
    return lax.dot_general(a, b, dims, preferred_element_type=F32)


def remote(src, dst, send, recv, to):
    return pltpu.make_async_remote_copy(
        src_ref=src, dst_ref=dst, send_sem=send, recv_sem=recv, device_id=to, device_id_type=MESH
    )


def each(n, body):
    def step(t, carry):
        body(t)
        return carry

    lax.fori_loop(0, n, step, 0)


def wrap(v, n):
    return jnp.where(v >= n, v - n, v)


FAR_FIRST = (8, 7, 9, 6, 10, 5, 11, 4, 12, 3, 13, 2, 14, 1, 15)
PLANE = sorted(
    (
        (dy, dh, dl)
        for dy in range(4)
        for dh in range(2)
        for dl in range(2)
        if dy + dh + dl > 0
    ),
    key=lambda d: -(min(d[0], 4 - d[0]) + (2 if d[1:] == (1, 0) else max(d[1:]))),
)


def kernel(
    ids_ref,
    idv_ref,
    xs_hbm,
    jac_hbm,
    tgt_hbm,
    w1_hbm,
    b1_hbm,
    hw_hbm,
    hb_hbm,
    dec_hbm,
    hall_hbm,
    fall_hbm,
    tile_hbm,
    dg_hbm,
    xs_ref,
    jac_ref,
    tgt_ref,
    w1_ref,
    b1_ref,
    hw_ref,
    hb_ref,
    dec_ref,
    ft,
    tsend,
    tfull,
    dsend,
    dblk,
    dmat,
    jsend,
    jbuf,
    net,
    tbytes,
    pbuf,
    rbuf,
    gsend,
    grecv,
    gown,
    hsend,
    hrecv,
    qsend,
    qpart,
    qsum,
    qrecv,
    fsend,
    fpart,
    fsum,
    frecv,
    zsend,
    zrecv,
    zall,
    ysend,
    yrecv,
    yall,
    hall,
    fall,
    tile,
    dg_ref,
    sent,
    came,
    taken,
    put,
):
    z, xl, c = lax.axis_index("z"), lax.axis_index("xl"), lax.axis_index("c")
    y, xh = lax.axis_index("y"), lax.axis_index("xh")
    m = y * 2 + xh
    q = m * 2 + xl
    b = c * NZ + z

    def plane(d):
        dy, dh, dl = d
        yy = wrap(y + dy, 4)
        hh = 1 - xh if dh else xh
        ll = 1 - xl if dl else xl
        return (yy * 2 + hh) * 2 + ll, {"y": yy, "xh": hh, "xl": ll}

    partner = {"c": 1 - c}
    barrier = pltpu.get_barrier_semaphore()

    homes = (
        (tgt_hbm, tgt_ref),
        (dec_hbm, dec_ref),
        (jac_hbm, jac_ref),
        (xs_hbm, xs_ref),
        (w1_hbm, w1_ref),
        (hw_hbm, hw_ref),
        (b1_hbm, b1_ref),
        (hb_hbm, hb_ref),
    )
    loads = [pltpu.make_async_copy(a, v, taken.at[k]) for k, (a, v) in enumerate(homes)]
    for load in loads:
        load.start()

    def greet(to):
        pl.semaphore_signal(barrier, inc=1, device_id=to, device_id_type=MESH)

    for d in FAR_FIRST:
        for cc in range(2):
            greet({"z": wrap(z + d, NZ), "c": cc})
    for d in PLANE:
        greet(plane(d)[1])
    greet(partner)

    hot = (lax.broadcasted_iota(jnp.int32, (512, 64), 0) == idv_ref[...]).astype(F32).astype(BF)
    for load in loads[0:2]:
        load.wait()
    dsend[:, 0:H] = dec_ref[...]
    dsend[:, H : H + 64] = dot(tgt_ref[...], hot).astype(BF)
    dsend[:, H + 64 :] = jnp.zeros((8, R - 64), BF)

    with jax.named_scope("barrier"):
        pl.semaphore_wait(barrier, 46)

    mine = pl.ds(pl.multiple_of(m * R, R), R)

    def tan_copy(to):
        return remote(
            tsend, tfull.at[xl, pl.ds(0, R + 16), mine], sent.at[0], came.at[0], to
        )

    def own_copy(d, k):
        return remote(
            dsend, dblk.at[c, z], sent.at[k], came.at[k], {"z": wrap(z + d, NZ)}
        )

    def pass_copy(block, d):
        part = dblk.at[c, wrap(z + block, NZ)]
        return remote(part, part, sent.at[2], came.at[2], {"z": wrap(z + d, NZ)})

    def half_copy(side):
        return remote(dblk.at[side], dblk.at[side], sent.at[3], came.at[3], partner)

    def jac_copy(zz, cc, i):
        return remote(
            jsend.at[i, cc * NZ + zz],
            jbuf.at[i, b],
            sent.at[4 if i == 0 else 21],
            came.at[4 if i == 0 else 21],
            {"z": zz, "c": cc},
        )

    def start_jac(i):
        for d in FAR_FIRST:
            for cc in range(2):
                jac_copy(wrap(z + d, NZ), cc, i).start()
        jac_copy(z, 1 - c, i).start()

    def start_z(copy):
        for d in FAR_FIRST:
            copy(wrap(z + d, NZ)).start()

    xside = {"xl": 1 - xl}

    def recv(k, ref):
        with jax.named_scope(f"recv{k}"):
            remote(ref, ref, sent.at[k], came.at[k], partner).wait_recv()

    def left(k, ref):
        remote(ref, ref, sent.at[k], came.at[k], partner).wait_send()

    for d in (5, 11):
        own_copy(d, 1).start()
    for d in (1, 15, 2, 14):
        own_copy(d, 16).start()
    dblk[c, z] = dsend[...]
    loads[2].wait()

    def pick(zz):
        for cc in range(2):
            for i in range(2):
                jsend[i, cc * NZ + zz] = jac_ref[ids_ref[zz * 4 + cc * 2 + i]]

    with jax.named_scope("pick"):
        each(NZ, pick)
    start_jac(0)
    for i in range(2):
        jbuf[i, b] = jsend[i, b]
    for load in loads[3:]:
        load.wait()

    own = ids_ref[z * 4 + c * 2 + xl]
    x_hot = (lax.broadcasted_iota(jnp.int32, (16, 512), 1) == own).astype(F32).astype(BF)
    x_rows = dot(x_hot, xs_ref[...])
    w1 = w1_ref[...].astype(F32)
    b1 = b1_ref[...].astype(F32)
    b1 = jnp.concatenate([b1[k : k + 1] for k in range(8)], axis=1)
    first_pre = dot(x_rows.astype(BF), w1_ref[...]) + b1
    first_act = jnp.tanh(first_pre)[0:1]
    first_slope = 1.0 - first_act * first_act
    top16 = lax.broadcasted_iota(jnp.int32, (16, H), 0) == 0
    ft[0:R, :] = (first_slope * w1).astype(BF)
    ft[R : R + 16, :] = jnp.where(top16, jnp.broadcast_to(first_act, (16, H)), 0.0).astype(BF)
    lin = dot(ft[...], hw_ref[...])
    hidden_lin = lin[0:R]
    hidden_act = jnp.tanh(lin[R : R + 1] + hb_ref[...].astype(F32))
    hidden_slope = 1.0 - hidden_act * hidden_act
    top = lax.broadcasted_iota(jnp.int32, (16, R), 0) == 0
    tsend[0:R, :] = (hidden_slope * hidden_lin).astype(BF)
    tsend[R : R + 16, :] = jnp.where(top, jnp.broadcast_to(hidden_act, (16, R)), 0.0).astype(BF)
    for d in PLANE:
        tan_copy(plane(d)[1]).start()
    tfull[:, R + 16 :, :] = jnp.zeros((2, 2 * R - R - 16, H), BF)
    tfull[xl, 0 : R + 16, mine] = tsend[...]

    recv(1, dblk.at[0, pl.ds(0, 2)])
    for d in (2, 14, 1, 15):
        for block in (5, 11):
            pass_copy(block, d).start()
    odd = z % 2
    pass_copy(11 - 6 * odd, 3 + 10 * odd).start()
    start_jac(1)
    recv(16, dblk.at[0, pl.ds(0, 4)])
    recv(2, dblk.at[0, pl.ds(0, 9)])
    half_copy(c).start()

    def unpack(side):
        rows = pl.ds(pl.multiple_of(side * R, R), R)
        dmat[rows, :] = dblk[side].astype(F32).reshape(R, WIDE).astype(BF)

    unpack(c)
    recv(0, tbytes.at[pl.ds(0, 15)])
    recv(3, dblk.at[0])
    unpack(1 - c)

    lane = lax.broadcasted_iota(jnp.int32, (2 * R, R), 1)
    tgt = dmat[:, H:].astype(F32)
    dec = dmat[:, 0:H]
    for i in range(2):
        want = jnp.sum(jnp.where(lane == z * 4 + c * 2 + i, tgt, 0.0), axis=1, keepdims=True)
        want = jnp.where(lane == 0, jnp.broadcast_to(want, (2 * R, R)), 0.0)
        out = dot(dec, tfull[i], NT)
        net[i, :, 0:R] = out[:, 0:R]
        net[i, :, R:] = out[:, R:] - want
    miss = []
    for i in range(2):
        recv(4 if i == 0 else 21, jbuf.at[0, pl.ds(0, 31)])
        stored = jbuf[i].astype(F32).reshape(2 * R, R)
        miss_i = jnp.concatenate([net[i, :, 0:R] - stored, net[i, :, R:]], axis=1).astype(BF)
        miss.append(miss_i)
        back_i = dot(miss_i, dec, TN)[0 : R + 8]
        for k in range(8):
            part = back_i[:, R * k : R * k + R]
            pbuf[i, k] = part.reshape(17, 8, R).astype(BF)
        for dy in (2, 1, 3, 0):
            for hh in range(2):
                yy = wrap(y + dy, 4)
                to = {"y": yy, "xh": hh, "xl": i}

                def send():
                    remote(
                        pbuf.at[i, yy * 2 + hh], rbuf.at[q], sent.at[5], came.at[5], to
                    ).start()

                if dy:
                    send()
                else:
                    pl.when((hh != xh) | (xl != i))(send)

    gown[...] = dot(miss[0], tfull[0]) + dot(miss[1], tfull[1])
    theirs = gown[pl.ds(pl.multiple_of((1 - c) * R, R), R), :]
    gsend[...] = theirs.reshape(NZ, 8, H).astype(BF)
    remote(gsend, grecv, sent.at[6], came.at[6], partner).start()
    ours = gown[pl.ds(pl.multiple_of(c * R, R), R), :].reshape(NZ, 8, H)
    recv(6, grecv)
    hsend[...] = (ours + grecv[...].astype(F32)).astype(BF)

    def gz_copy(peer):
        return remote(hsend.at[peer], hrecv.at[z], sent.at[7], came.at[7], {"z": peer})

    start_z(gz_copy)
    hrecv[z] = hsend[z]

    recv(5, rbuf.at[pl.ds(0, 15)])
    rbuf[q] = pbuf[xl, m]
    back = jnp.sum(rbuf[...].astype(F32), axis=0).reshape(R + 8, R)
    tan_back = back[0:R]
    act_back = back[R : R + 1]
    lin_round = (tan_back * hidden_slope).astype(BF)
    pre_back = act_back * hidden_slope - 2.0 * hidden_act * hidden_slope * jnp.sum(
        tan_back * hidden_lin, axis=0, keepdims=True
    )
    pre_round = jnp.where(top, jnp.broadcast_to(pre_back, (16, R)), 0.0).astype(BF)
    both = jnp.concatenate([lin_round, pre_round], axis=0)
    low = dot(both, hw_ref[...], NT)
    tan_lower = low[0:R]
    pre_lower = low[R : R + 1] * first_slope - 2.0 * first_act * first_slope * jnp.sum(
        tan_lower * w1, axis=0, keepdims=True
    )
    x_col = jnp.transpose(jnp.broadcast_to(x_rows[0:1], (R, R)))[:, 0:1]
    fw = x_col * pre_lower + tan_lower * first_slope
    place = lax.broadcasted_iota(jnp.int32, (8, H), 1) // R == m
    line = lax.broadcasted_iota(jnp.int32, (8, H), 0)
    pre_wide = jnp.concatenate([pre_back] * 8, axis=1)
    tail = jnp.where(line == 0, jnp.broadcast_to(pre_lower, (8, H)), 0.0)
    tail = tail + jnp.where((line == 1) & place, jnp.broadcast_to(pre_wide, (8, H)), 0.0)
    for cc in range(2):
        for k in range(16):
            r0 = 64 * cc + 32 * (k % 2)
            l0 = R * (k // 2)
            fsend[cc, k, 0:4] = fw[r0 : r0 + 32, l0 : l0 + R].reshape(4, 8, R).astype(BF)
            fsend[cc, k, 4] = tail[:, l0 : l0 + R].astype(BF)
    remote(fsend.at[1 - c], fpart, sent.at[9], came.at[9], partner).start()
    qsend[...] = dot(ft[...], both, TN).astype(BF).reshape(2, 4 * R, R)
    remote(qsend.at[1 - c], qpart, sent.at[8], came.at[8], partner).start()
    recv(9, fpart)
    fsum[...] = (fsend[c].astype(F32) + fpart[...].astype(F32)).astype(BF)
    for d in PLANE:
        peer, to = plane(d)
        remote(fsum.at[peer], frecv.at[q], sent.at[17], came.at[17], to).start()
    frecv[q] = fsum[q]
    recv(8, qpart)
    halves = qsend[c].astype(F32) + qpart[...].astype(F32)
    qsum[...] = halves.astype(BF).reshape(2, 2 * R, R)
    remote(qsum.at[1 - xl], qrecv, sent.at[18], came.at[18], xside).start()

    recv(17, frecv.at[pl.ds(0, 15)])
    ysend[...] = jnp.sum(frecv[...].astype(F32), axis=0).astype(BF)
    for t in range(5):

        @pl.when(z != t)
        def _():
            remote(ysend.at[t], yrecv.at[z], sent.at[11], came.at[11], {"z": t}).start()

        @pl.when(z == t)
        def _():
            yrecv[z] = ysend[t]

    recv(18, qrecv)
    quarter = qsum[xl].astype(F32) + qrecv[...].astype(F32)
    zsend[...] = quarter.reshape(NZ, 2, 8, R).astype(BF)

    def zr_copy(peer):
        return remote(zsend.at[peer], zrecv.at[z], sent.at[10], came.at[10], {"z": peer})

    start_z(zr_copy)
    zrecv[z] = zsend[z]

    def y_copy(peer):
        return remote(yall.at[z], yall.at[z], sent.at[13], came.at[13], {"z": peer})

    @pl.when(z < 5)
    def _():
        recv(11, yrecv.at[pl.ds(0, 15)])
        yall[z] = jnp.sum(yrecv[...].astype(F32), axis=0).astype(BF)
        start_z(y_copy)

    recv(10, zrecv.at[pl.ds(0, 15)])
    zall[z] = jnp.sum(zrecv[...].astype(F32), axis=0).astype(BF)

    def zg_copy(peer):
        return remote(zall.at[z], zall.at[z], sent.at[12], came.at[12], {"z": peer})

    start_z(zg_copy)

    recv(7, hrecv.at[pl.ds(0, 15)])
    dg_ref[...] = jnp.sum(hrecv[...].astype(F32), axis=0)
    outs = (
        pltpu.make_async_copy(dg_ref, dg_hbm, put.at[0]),
        pltpu.make_async_copy(tile, tile_hbm, put.at[1]),
        pltpu.make_async_copy(hall, hall_hbm, put.at[2]),
        pltpu.make_async_copy(fall, fall_hbm, put.at[3]),
    )
    outs[0].start()

    @pl.when(z < 5)
    def _():
        recv(13, yall.at[pl.ds(0, 4)])

    @pl.when(z >= 5)
    def _():
        recv(13, yall.at[pl.ds(0, 5)])

    for d in PLANE:
        remote(
            yall.at[pl.ds(0, 5)], fall.at[c, q], sent.at[15], came.at[15], plane(d)[1]
        ).start()
    fall[c, q] = yall[0:5]
    tile[...] = yall[4]
    outs[1].start()
    recv(12, zall.at[pl.ds(0, 15)])
    remote(zall, hall.at[c, xl], sent.at[14], came.at[14], xside).start()
    hall[c, xl] = zall[...]
    recv(15, fall.at[0, pl.ds(0, 15)])
    remote(fall.at[c], fall.at[c], sent.at[19], came.at[19], partner).start()
    recv(14, zall)
    remote(hall.at[c], hall.at[c], sent.at[20], came.at[20], partner).start()
    recv(19, fall.at[0])
    outs[3].start()
    recv(20, hall.at[0])
    outs[2].start()

    left(0, tbytes.at[pl.ds(0, 15)])
    left(1, dblk.at[0, pl.ds(0, 2)])
    left(16, dblk.at[0, pl.ds(0, 4)])
    left(2, dblk.at[0, pl.ds(0, 9)])
    left(3, dblk.at[0])
    left(4, jbuf.at[0, pl.ds(0, 31)])
    left(21, jbuf.at[0, pl.ds(0, 31)])
    left(5, rbuf.at[pl.ds(0, 15)])
    left(6, grecv)
    left(7, hrecv.at[pl.ds(0, 15)])
    left(8, qpart)
    left(9, fpart)
    left(17, frecv.at[pl.ds(0, 15)])
    left(18, qrecv)
    left(10, zrecv.at[pl.ds(0, 15)])

    @pl.when(z < 5)
    def _():
        left(11, yall.at[pl.ds(0, 4)])
        left(13, yrecv.at[pl.ds(0, 15)])

    @pl.when(z >= 5)
    def _():
        left(11, yall.at[pl.ds(0, 5)])

    left(12, zrecv.at[pl.ds(0, 15)])
    left(14, zall)
    left(15, fall.at[0, pl.ds(0, 15)])
    left(19, fall.at[0])
    left(20, hall.at[0])
    for out in outs:
        out.wait()


def unfold(
    hall_hbm,
    fall_hbm,
    tile_hbm,
    dg_hbm,
    fw_hbm,
    fb_hbm,
    hg_hbm,
    hb_hbm,
    dgo_hbm,
    hall,
    fall,
    tile,
    dg,
    fw,
    fb,
    hg,
    hb,
    got,
    put,
):
    ins = (
        pltpu.make_async_copy(hall_hbm, hall, got.at[0]),
        pltpu.make_async_copy(fall_hbm, fall, got.at[1]),
        pltpu.make_async_copy(dg_hbm, dg, got.at[2]),
        pltpu.make_async_copy(tile_hbm, tile, got.at[3]),
    )
    outs = (
        pltpu.make_async_copy(hg, hg_hbm, put.at[0]),
        pltpu.make_async_copy(fw, fw_hbm, put.at[1]),
        pltpu.make_async_copy(dg, dgo_hbm, put.at[2]),
        pltpu.make_async_copy(hb, hb_hbm, put.at[3]),
        pltpu.make_async_copy(fb, fb_hbm, put.at[4]),
    )
    for copy in ins:
        copy.start()
    ins[0].wait()
    hg[...] = hall[...].astype(F32).reshape(H, R)
    outs[0].start()
    ins[1].wait()
    for mm in range(8):
        for ee in range(4):
            piece = fall[ee // 2, 2 * mm + ee % 2].astype(F32)
            fw[32 * ee : 32 * ee + 32, R * mm : R * mm + R] = piece[0:4].reshape(32, R)
            if ee == 0:
                fb[mm : mm + 1, :] = piece[4, 0:1]
    outs[1].start()
    outs[4].start()
    ins[2].wait()
    outs[2].start()
    ins[3].wait()
    hb[...] = tile[...].astype(F32)[1:2]
    outs[3].start()
    for copy in outs:
        copy.wait()


def on_device(
    inputs_store,
    window,
    targets_store,
    jac_store,
    first_weight,
    first_bias,
    hidden_weight,
    hidden_bias,
    decoder_weight,
):
    vmem = pl.BlockSpec(memory_space=pltpu.VMEM)
    smem = pl.BlockSpec(memory_space=pltpu.SMEM)
    hbm = pl.BlockSpec(memory_space=pltpu.HBM)
    dma = pltpu.SemaphoreType.DMA
    hall = jax.ShapeDtypeStruct((2, 2, NZ, 2, 8, R), BF)
    fall = jax.ShapeDtypeStruct((2, 16, 5, 8, R), BF)
    tile = jax.ShapeDtypeStruct((8, R), BF)
    dg = jax.ShapeDtypeStruct((8, H), F32)
    raw = (hall, fall, tile, dg)
    parts = pl.pallas_call(
        kernel,
        out_shape=raw,
        in_specs=[smem, vmem] + [hbm] * 8,
        out_specs=(hbm,) * 4,
        scratch_shapes=[
            pltpu.VMEM((512, R), BF),
            pltpu.VMEM((512, 8, R), BF),
            pltpu.VMEM((8, 512), BF),
            pltpu.VMEM((R, H), BF),
            pltpu.VMEM((8, R), BF),
            pltpu.VMEM((H, R), BF),
            pltpu.VMEM((1, R), BF),
            pltpu.VMEM((8, H), BF),
            pltpu.VMEM((R + 16, H), BF),
            pltpu.VMEM((R + 16, R), BF),
            pltpu.VMEM((2, 2 * R, H), BF),
            pltpu.VMEM((8, WIDE), BF),
            pltpu.VMEM((2, NZ, 8, WIDE), BF),
            pltpu.VMEM((2 * R, WIDE), BF),
            pltpu.VMEM((2, 32, 8, R), BF),
            pltpu.VMEM((2, 32, 8, R), BF),
            pltpu.VMEM((2, 2 * R, 2 * R), F32),
            pltpu.VMEM((16, R + 16, R), BF),
            pltpu.VMEM((2, 8, 17, 8, R), BF),
            pltpu.VMEM((16, 17, 8, R), BF),
            pltpu.VMEM((NZ, 8, H), BF),
            pltpu.VMEM((NZ, 8, H), BF),
            pltpu.VMEM((2 * R, H), F32),
            pltpu.VMEM((NZ, 8, H), BF),
            pltpu.VMEM((NZ, 8, H), BF),
            pltpu.VMEM((2, 4 * R, R), BF),
            pltpu.VMEM((4 * R, R), BF),
            pltpu.VMEM((2, 2 * R, R), BF),
            pltpu.VMEM((2 * R, R), BF),
            pltpu.VMEM((2, 16, 5, 8, R), BF),
            pltpu.VMEM((16, 5, 8, R), BF),
            pltpu.VMEM((16, 5, 8, R), BF),
            pltpu.VMEM((16, 5, 8, R), BF),
            pltpu.VMEM((NZ, 2, 8, R), BF),
            pltpu.VMEM((NZ, 2, 8, R), BF),
            pltpu.VMEM((NZ, 2, 8, R), BF),
            pltpu.VMEM((5, 8, R), BF),
            pltpu.VMEM((NZ, 8, R), BF),
            pltpu.VMEM((NZ, 8, R), BF),
            pltpu.VMEM((2, 2, NZ, 2, 8, R), BF),
            pltpu.VMEM((2, 16, 5, 8, R), BF),
            pltpu.VMEM((8, R), BF),
            pltpu.VMEM((8, H), F32),
            dma((22,)),
            dma((22,)),
            dma((8,)),
            dma((4,)),
        ],
        compiler_params=pltpu.CompilerParams(
            collective_id=0, has_side_effects=True, vmem_limit_bytes=VMEM_MOST
        ),
    )(
        window,
        window.reshape(1, 64),
        inputs_store,
        jac_store,
        targets_store.T,
        first_weight,
        first_bias.reshape(8, R),
        hidden_weight,
        hidden_bias.reshape(1, R),
        decoder_weight,
    )
    final = (
        jax.ShapeDtypeStruct((R, H), F32),
        jax.ShapeDtypeStruct((8, R), F32),
        jax.ShapeDtypeStruct((H, R), F32),
        jax.ShapeDtypeStruct((1, R), F32),
        dg,
    )
    fw, fb, hg, hb, dgo = pl.pallas_call(
        unfold,
        out_shape=final,
        in_specs=[hbm] * 4,
        out_specs=(hbm,) * 5,
        scratch_shapes=[pltpu.VMEM(a.shape, a.dtype) for a in raw + final[0:4]]
        + [dma((4,)), dma((5,))],
        compiler_params=pltpu.CompilerParams(vmem_limit_bytes=VMEM_MOST),
    )(*parts)
    return fw, fb.reshape(H), hg, hb.reshape(R), dgo


def solution(mesh):
    torus = Mesh(mesh.devices.reshape(NZ, 2, 2, 4, 2), ALL)
    return jax.shard_map(
        on_device,
        mesh=torus,
        in_specs=(
            P(),
            P(),
            P(None, ALL),
            P(None, ALL, None),
            P(),
            P(),
            P(None, MP),
            P(MP),
            P(ALL, None),
        ),
        out_specs=(P(), P(), P(None, MP), P(MP), P(ALL, None)),
        check_vma=False,
    )
```

```python
import jax
import jax.numpy as jnp
from jax import lax
from jax.experimental import pallas as pl
from jax.experimental.pallas import tpu as pltpu
from jax.sharding import Mesh
from jax.sharding import PartitionSpec as P

MESH = pl.DeviceIdType.MESH
DP = ("z", "xl", "c")
MP = ("y", "xh")
ALL = DP + MP
BF = jnp.bfloat16
F32 = jnp.float32

R = 128
H = 1024
NZ = 16
WIDE = H + R
VMEM_MOST = 67043328
NT = (((1,), (1,)), ((), ()))
TN = (((0,), (0,)), ((), ()))


def dot(a, b, dims=(((1,), (0,)), ((), ()))):
    return lax.dot_general(a, b, dims, preferred_element_type=F32)


def remote(src, dst, send, recv, to):
    return pltpu.make_async_remote_copy(
        src_ref=src, dst_ref=dst, send_sem=send, recv_sem=recv, device_id=to, device_id_type=MESH
    )


def each(n, body):
    def step(t, carry):
        body(t)
        return carry

    lax.fori_loop(0, n, step, 0)


def wrap(v, n):
    return jnp.where(v >= n, v - n, v)


FAR_FIRST = (8, 7, 9, 6, 10, 5, 11, 4, 12, 3, 13, 2, 14, 1, 15)
PLANE = sorted(
    (
        (dy, dh, dl)
        for dy in range(4)
        for dh in range(2)
        for dl in range(2)
        if dy + dh + dl > 0
    ),
    key=lambda d: -(min(d[0], 4 - d[0]) + (2 if d[1:] == (1, 0) else max(d[1:]))),
)


def kernel(
    ids_ref,
    idv_ref,
    xs_hbm,
    jac_hbm,
    tgt_hbm,
    w1_hbm,
    b1_hbm,
    hw_hbm,
    hb_hbm,
    dec_hbm,
    hall_hbm,
    fall_hbm,
    tile_hbm,
    dg_hbm,
    xs_ref,
    jac_ref,
    tgt_ref,
    w1_ref,
    b1_ref,
    hw_ref,
    hb_ref,
    dec_ref,
    ft,
    tsend,
    tfull,
    dsend,
    dblk,
    dmat,
    jsend,
    jbuf,
    net,
    tbytes,
    pbuf,
    rbuf,
    gsend,
    grecv,
    gown,
    hsend,
    hrecv,
    qsend,
    qpart,
    qsum,
    qrecv,
    fsend,
    fpart,
    fsum,
    frecv,
    zsend,
    zrecv,
    zall,
    ysend,
    yrecv,
    yall,
    hall,
    fall,
    tile,
    dg_ref,
    sent,
    came,
    taken,
    put,
):
    z, xl, c = lax.axis_index("z"), lax.axis_index("xl"), lax.axis_index("c")
    y, xh = lax.axis_index("y"), lax.axis_index("xh")
    m = y * 2 + xh
    q = m * 2 + xl
    b = c * NZ + z

    def plane(d):
        dy, dh, dl = d
        yy = wrap(y + dy, 4)
        hh = 1 - xh if dh else xh
        ll = 1 - xl if dl else xl
        return (yy * 2 + hh) * 2 + ll, {"y": yy, "xh": hh, "xl": ll}

    partner = {"c": 1 - c}
    barrier = pltpu.get_barrier_semaphore()

    homes = (
        (tgt_hbm, tgt_ref),
        (dec_hbm, dec_ref),
        (jac_hbm, jac_ref),
        (xs_hbm, xs_ref),
        (w1_hbm, w1_ref),
        (hw_hbm, hw_ref),
        (b1_hbm, b1_ref),
        (hb_hbm, hb_ref),
    )
    loads = [pltpu.make_async_copy(a, v, taken.at[k]) for k, (a, v) in enumerate(homes)]
    for load in loads:
        load.start()

    def greet(to):
        pl.semaphore_signal(barrier, inc=1, device_id=to, device_id_type=MESH)

    for d in FAR_FIRST:
        for cc in range(2):
            greet({"z": wrap(z + d, NZ), "c": cc})
    for d in PLANE:
        greet(plane(d)[1])
    greet(partner)

    hot = (lax.broadcasted_iota(jnp.int32, (512, 64), 0) == idv_ref[...]).astype(F32).astype(BF)
    for load in loads[0:2]:
        load.wait()
    dsend[:, 0:H] = dec_ref[...]
    dsend[:, H : H + 64] = dot(tgt_ref[...], hot).astype(BF)
    dsend[:, H + 64 :] = jnp.zeros((8, R - 64), BF)

    with jax.named_scope("barrier"):
        pl.semaphore_wait(barrier, 46)

    mine = pl.ds(pl.multiple_of(m * R, R), R)

    def tan_copy(to):
        return remote(
            tsend, tfull.at[xl, pl.ds(0, R + 16), mine], sent.at[0], came.at[0], to
        )

    def own_copy(d, k):
        return remote(
            dsend, dblk.at[c, z], sent.at[k], came.at[k], {"z": wrap(z + d, NZ)}
        )

    def pass_copy(block, d):
        part = dblk.at[c, wrap(z + block, NZ)]
        return remote(part, part, sent.at[2], came.at[2], {"z": wrap(z + d, NZ)})

    def half_copy(side):
        return remote(dblk.at[side], dblk.at[side], sent.at[3], came.at[3], partner)

    def jac_copy(zz, cc):
        return remote(
            jsend.at[cc * NZ + zz], jbuf.at[b], sent.at[4], came.at[4], {"z": zz, "c": cc}
        )

    def start_jac(ds):
        for d in ds:
            for cc in range(2):
                jac_copy(wrap(z + d, NZ), cc).start()

    def start_z(copy):
        for d in FAR_FIRST:
            copy(wrap(z + d, NZ)).start()

    xside = {"xl": 1 - xl}

    def recv(k, ref):
        with jax.named_scope(f"recv{k}"):
            remote(ref, ref, sent.at[k], came.at[k], partner).wait_recv()

    def left(k, ref):
        remote(ref, ref, sent.at[k], came.at[k], partner).wait_send()

    for d in (5, 11):
        own_copy(d, 1).start()
    for d in (1, 15, 2, 14):
        own_copy(d, 16).start()
    dblk[c, z] = dsend[...]
    loads[2].wait()

    def pick(zz):
        for cc in range(2):
            for i in range(2):
                jsend[cc * NZ + zz, i] = jac_ref[ids_ref[zz * 4 + cc * 2 + i]]

    each(NZ, pick)
    start_jac(FAR_FIRST[0:5])
    jbuf[b] = jsend[b]
    for load in loads[3:]:
        load.wait()

    own = ids_ref[z * 4 + c * 2 + xl]
    x_hot = (lax.broadcasted_iota(jnp.int32, (16, 512), 1) == own).astype(F32).astype(BF)
    x_rows = dot(x_hot, xs_ref[...])
    w1 = w1_ref[...].astype(F32)
    b1 = b1_ref[...].astype(F32)
    b1 = jnp.concatenate([b1[k : k + 1] for k in range(8)], axis=1)
    first_pre = dot(x_rows.astype(BF), w1_ref[...]) + b1
    first_act = jnp.tanh(first_pre)[0:1]
    first_slope = 1.0 - first_act * first_act
    top16 = lax.broadcasted_iota(jnp.int32, (16, H), 0) == 0
    ft[0:R, :] = (first_slope * w1).astype(BF)
    ft[R : R + 16, :] = jnp.where(top16, jnp.broadcast_to(first_act, (16, H)), 0.0).astype(BF)
    lin = dot(ft[...], hw_ref[...])
    hidden_lin = lin[0:R]
    hidden_act = jnp.tanh(lin[R : R + 1] + hb_ref[...].astype(F32))
    hidden_slope = 1.0 - hidden_act * hidden_act
    top = lax.broadcasted_iota(jnp.int32, (16, R), 0) == 0
    tsend[0:R, :] = (hidden_slope * hidden_lin).astype(BF)
    tsend[R : R + 16, :] = jnp.where(top, jnp.broadcast_to(hidden_act, (16, R)), 0.0).astype(BF)
    for d in PLANE:
        tan_copy(plane(d)[1]).start()
    tfull[:, R + 16 :, :] = jnp.zeros((2, 2 * R - R - 16, H), BF)
    tfull[xl, 0 : R + 16, mine] = tsend[...]

    recv(1, dblk.at[0, pl.ds(0, 2)])
    for d in (2, 14, 1, 15):
        for block in (5, 11):
            pass_copy(block, d).start()
    odd = z % 2
    pass_copy(11 - 6 * odd, 3 + 10 * odd).start()
    start_jac(FAR_FIRST[5:])
    jac_copy(z, 1 - c).start()
    recv(16, dblk.at[0, pl.ds(0, 4)])
    recv(2, dblk.at[0, pl.ds(0, 9)])
    half_copy(c).start()

    def unpack(side):
        rows = pl.ds(pl.multiple_of(side * R, R), R)
        dmat[rows, :] = dblk[side].astype(F32).reshape(R, WIDE).astype(BF)

    unpack(c)
    recv(0, tbytes.at[pl.ds(0, 15)])
    recv(3, dblk.at[0])
    unpack(1 - c)

    lane = lax.broadcasted_iota(jnp.int32, (2 * R, R), 1)
    tgt = dmat[:, H:].astype(F32)
    dec = dmat[:, 0:H]
    for i in range(2):
        want = jnp.sum(jnp.where(lane == z * 4 + c * 2 + i, tgt, 0.0), axis=1, keepdims=True)
        want = jnp.where(lane == 0, jnp.broadcast_to(want, (2 * R, R)), 0.0)
        out = dot(dec, tfull[i], NT)
        net[i, :, 0:R] = out[:, 0:R]
        net[i, :, R:] = out[:, R:] - want
    recv(4, jbuf.at[pl.ds(0, 31)])
    miss = []
    for i in range(2):
        stored = jbuf[:, i].astype(F32).reshape(2 * R, R)
        miss_i = jnp.concatenate([net[i, :, 0:R] - stored, net[i, :, R:]], axis=1).astype(BF)
        miss.append(miss_i)
        back_i = dot(miss_i, dec, TN)[0 : R + 8]
        for k in range(8):
            part = back_i[:, R * k : R * k + R]
            pbuf[i, k] = part.reshape(17, 8, R).astype(BF)
        for dy in (2, 1, 3, 0):
            for hh in range(2):
                yy = wrap(y + dy, 4)
                to = {"y": yy, "xh": hh, "xl": i}

                def send():
                    remote(
                        pbuf.at[i, yy * 2 + hh], rbuf.at[q], sent.at[5], came.at[5], to
                    ).start()

                if dy:
                    send()
                else:
                    pl.when((hh != xh) | (xl != i))(send)

    gown[...] = dot(miss[0], tfull[0]) + dot(miss[1], tfull[1])
    theirs = gown[pl.ds(pl.multiple_of((1 - c) * R, R), R), :]
    gsend[...] = theirs.reshape(NZ, 8, H).astype(BF)
    remote(gsend, grecv, sent.at[6], came.at[6], partner).start()
    ours = gown[pl.ds(pl.multiple_of(c * R, R), R), :].reshape(NZ, 8, H)
    recv(6, grecv)
    hsend[...] = (ours + grecv[...].astype(F32)).astype(BF)

    def gz_copy(peer):
        return remote(hsend.at[peer], hrecv.at[z], sent.at[7], came.at[7], {"z": peer})

    start_z(gz_copy)
    hrecv[z] = hsend[z]

    recv(5, rbuf.at[pl.ds(0, 15)])
    rbuf[q] = pbuf[xl, m]
    back = jnp.sum(rbuf[...].astype(F32), axis=0).reshape(R + 8, R)
    tan_back = back[0:R]
    act_back = back[R : R + 1]
    lin_round = (tan_back * hidden_slope).astype(BF)
    pre_back = act_back * hidden_slope - 2.0 * hidden_act * hidden_slope * jnp.sum(
        tan_back * hidden_lin, axis=0, keepdims=True
    )
    pre_round = jnp.where(top, jnp.broadcast_to(pre_back, (16, R)), 0.0).astype(BF)
    both = jnp.concatenate([lin_round, pre_round], axis=0)
    qsend[...] = dot(ft[...], both, TN).astype(BF).reshape(2, 4 * R, R)
    remote(qsend.at[1 - c], qpart, sent.at[8], came.at[8], partner).start()

    low = dot(both, hw_ref[...], NT)
    tan_lower = low[0:R]
    pre_lower = low[R : R + 1] * first_slope - 2.0 * first_act * first_slope * jnp.sum(
        tan_lower * w1, axis=0, keepdims=True
    )
    x_col = jnp.transpose(jnp.broadcast_to(x_rows[0:1], (R, R)))[:, 0:1]
    fw = x_col * pre_lower + tan_lower * first_slope
    place = lax.broadcasted_iota(jnp.int32, (8, H), 1) // R == m
    line = lax.broadcasted_iota(jnp.int32, (8, H), 0)
    pre_wide = jnp.concatenate([pre_back] * 8, axis=1)
    tail = jnp.where(line == 0, jnp.broadcast_to(pre_lower, (8, H)), 0.0)
    tail = tail + jnp.where((line == 1) & place, jnp.broadcast_to(pre_wide, (8, H)), 0.0)
    for cc in range(2):
        for k in range(16):
            r0 = 64 * cc + 32 * (k % 2)
            l0 = R * (k // 2)
            fsend[cc, k, 0:4] = fw[r0 : r0 + 32, l0 : l0 + R].reshape(4, 8, R).astype(BF)
            fsend[cc, k, 4] = tail[:, l0 : l0 + R].astype(BF)
    remote(fsend.at[1 - c], fpart, sent.at[9], came.at[9], partner).start()
    recv(8, qpart)
    halves = qsend[c].astype(F32) + qpart[...].astype(F32)
    qsum[...] = halves.astype(BF).reshape(2, 2 * R, R)
    remote(qsum.at[1 - xl], qrecv, sent.at[18], came.at[18], xside).start()
    recv(9, fpart)
    fsum[...] = (fsend[c].astype(F32) + fpart[...].astype(F32)).astype(BF)
    for d in PLANE:
        peer, to = plane(d)
        remote(fsum.at[peer], frecv.at[q], sent.at[17], came.at[17], to).start()
    frecv[q] = fsum[q]
    recv(18, qrecv)
    quarter = qsum[xl].astype(F32) + qrecv[...].astype(F32)
    zsend[...] = quarter.reshape(NZ, 2, 8, R).astype(BF)

    def zr_copy(peer):
        return remote(zsend.at[peer], zrecv.at[z], sent.at[10], came.at[10], {"z": peer})

    start_z(zr_copy)
    zrecv[z] = zsend[z]

    recv(17, frecv.at[pl.ds(0, 15)])
    ysend[...] = jnp.sum(frecv[...].astype(F32), axis=0).astype(BF)

    def y_copy(d, k):
        to = {"z": wrap(z + d, NZ)}
        return remote(ysend, yrecv.at[z], sent.at[k], came.at[k], to)

    def y_pass(block, d):
        part = yrecv.at[wrap(z + block, NZ)]
        return remote(part, part, sent.at[21], came.at[21], {"z": wrap(z + d, NZ)})

    for d in (5, 11):
        y_copy(d, 11).start()
    for d in (1, 15, 2, 14):
        y_copy(d, 13).start()
    yrecv[z] = ysend[...]

    recv(10, zrecv.at[pl.ds(0, 15)])
    zall[z] = jnp.sum(zrecv[...].astype(F32), axis=0).astype(BF)

    def zg_copy(peer):
        return remote(zall.at[z], zall.at[z], sent.at[12], came.at[12], {"z": peer})

    start_z(zg_copy)

    recv(11, yrecv.at[pl.ds(0, 2)])
    for d in (2, 14, 1, 15):
        for block in (5, 11):
            y_pass(block, d).start()
    y_pass(11 - 6 * odd, 3 + 10 * odd).start()

    recv(7, hrecv.at[pl.ds(0, 15)])
    dg_ref[...] = jnp.sum(hrecv[...].astype(F32), axis=0)
    outs = (
        pltpu.make_async_copy(dg_ref, dg_hbm, put.at[0]),
        pltpu.make_async_copy(tile, tile_hbm, put.at[1]),
        pltpu.make_async_copy(hall, hall_hbm, put.at[2]),
        pltpu.make_async_copy(fall, fall_hbm, put.at[3]),
    )
    outs[0].start()

    recv(13, yrecv.at[pl.ds(0, 4)])
    recv(21, yrecv.at[pl.ds(0, 9)])
    yall[...] = jnp.sum(yrecv[...].astype(F32), axis=0).astype(BF)
    for d in PLANE:
        remote(yall, fall.at[c, q], sent.at[15], came.at[15], plane(d)[1]).start()
    fall[c, q] = yall[...]
    tile[...] = yall[4]
    outs[1].start()
    recv(12, zall.at[pl.ds(0, 15)])
    remote(zall, hall.at[c, xl], sent.at[14], came.at[14], xside).start()
    hall[c, xl] = zall[...]
    recv(15, fall.at[0, pl.ds(0, 15)])
    remote(fall.at[c], fall.at[c], sent.at[19], came.at[19], partner).start()
    recv(14, zall)
    remote(hall.at[c], hall.at[c], sent.at[20], came.at[20], partner).start()
    recv(19, fall.at[0])
    outs[3].start()
    recv(20, hall.at[0])
    outs[2].start()

    left(0, tbytes.at[pl.ds(0, 15)])
    left(1, dblk.at[0, pl.ds(0, 2)])
    left(16, dblk.at[0, pl.ds(0, 4)])
    left(2, dblk.at[0, pl.ds(0, 9)])
    left(3, dblk.at[0])
    left(4, jbuf.at[pl.ds(0, 31)])
    left(5, rbuf.at[pl.ds(0, 15)])
    left(6, grecv)
    left(7, hrecv.at[pl.ds(0, 15)])
    left(8, qpart)
    left(9, fpart)
    left(17, frecv.at[pl.ds(0, 15)])
    left(18, qrecv)
    left(10, zrecv.at[pl.ds(0, 15)])

    left(11, yrecv.at[pl.ds(0, 2)])
    left(13, yrecv.at[pl.ds(0, 4)])
    left(21, yrecv.at[pl.ds(0, 9)])
    left(12, zrecv.at[pl.ds(0, 15)])
    left(14, zall)
    left(15, fall.at[0, pl.ds(0, 15)])
    left(19, fall.at[0])
    left(20, hall.at[0])
    for out in outs:
        out.wait()


def unfold(
    hall_hbm,
    fall_hbm,
    tile_hbm,
    dg_hbm,
    fw_hbm,
    fb_hbm,
    hg_hbm,
    hb_hbm,
    dgo_hbm,
    hall,
    fall,
    tile,
    dg,
    fw,
    fb,
    hg,
    hb,
    got,
    put,
):
    ins = (
        pltpu.make_async_copy(hall_hbm, hall, got.at[0]),
        pltpu.make_async_copy(fall_hbm, fall, got.at[1]),
        pltpu.make_async_copy(dg_hbm, dg, got.at[2]),
        pltpu.make_async_copy(tile_hbm, tile, got.at[3]),
    )
    outs = (
        pltpu.make_async_copy(hg, hg_hbm, put.at[0]),
        pltpu.make_async_copy(fw, fw_hbm, put.at[1]),
        pltpu.make_async_copy(dg, dgo_hbm, put.at[2]),
        pltpu.make_async_copy(hb, hb_hbm, put.at[3]),
        pltpu.make_async_copy(fb, fb_hbm, put.at[4]),
    )
    for copy in ins:
        copy.start()
    ins[0].wait()
    hg[...] = hall[...].astype(F32).reshape(H, R)
    outs[0].start()
    ins[1].wait()
    for mm in range(8):
        for ee in range(4):
            piece = fall[ee // 2, 2 * mm + ee % 2].astype(F32)
            fw[32 * ee : 32 * ee + 32, R * mm : R * mm + R] = piece[0:4].reshape(32, R)
            if ee == 0:
                fb[mm : mm + 1, :] = piece[4, 0:1]
    outs[1].start()
    outs[4].start()
    ins[2].wait()
    outs[2].start()
    ins[3].wait()
    hb[...] = tile[...].astype(F32)[1:2]
    outs[3].start()
    for copy in outs:
        copy.wait()


def on_device(
    inputs_store,
    window,
    targets_store,
    jac_store,
    first_weight,
    first_bias,
    hidden_weight,
    hidden_bias,
    decoder_weight,
):
    vmem = pl.BlockSpec(memory_space=pltpu.VMEM)
    smem = pl.BlockSpec(memory_space=pltpu.SMEM)
    hbm = pl.BlockSpec(memory_space=pltpu.HBM)
    dma = pltpu.SemaphoreType.DMA
    hall = jax.ShapeDtypeStruct((2, 2, NZ, 2, 8, R), BF)
    fall = jax.ShapeDtypeStruct((2, 16, 5, 8, R), BF)
    tile = jax.ShapeDtypeStruct((8, R), BF)
    dg = jax.ShapeDtypeStruct((8, H), F32)
    raw = (hall, fall, tile, dg)
    parts = pl.pallas_call(
        kernel,
        out_shape=raw,
        in_specs=[smem, vmem] + [hbm] * 8,
        out_specs=(hbm,) * 4,
        scratch_shapes=[
            pltpu.VMEM((512, R), BF),
            pltpu.VMEM((512, 8, R), BF),
            pltpu.VMEM((8, 512), BF),
            pltpu.VMEM((R, H), BF),
            pltpu.VMEM((8, R), BF),
            pltpu.VMEM((H, R), BF),
            pltpu.VMEM((1, R), BF),
            pltpu.VMEM((8, H), BF),
            pltpu.VMEM((R + 16, H), BF),
            pltpu.VMEM((R + 16, R), BF),
            pltpu.VMEM((2, 2 * R, H), BF),
            pltpu.VMEM((8, WIDE), BF),
            pltpu.VMEM((2, NZ, 8, WIDE), BF),
            pltpu.VMEM((2 * R, WIDE), BF),
            pltpu.VMEM((32, 2, 8, R), BF),
            pltpu.VMEM((32, 2, 8, R), BF),
            pltpu.VMEM((2, 2 * R, 2 * R), F32),
            pltpu.VMEM((16, R + 16, R), BF),
            pltpu.VMEM((2, 8, 17, 8, R), BF),
            pltpu.VMEM((16, 17, 8, R), BF),
            pltpu.VMEM((NZ, 8, H), BF),
            pltpu.VMEM((NZ, 8, H), BF),
            pltpu.VMEM((2 * R, H), F32),
            pltpu.VMEM((NZ, 8, H), BF),
            pltpu.VMEM((NZ, 8, H), BF),
            pltpu.VMEM((2, 4 * R, R), BF),
            pltpu.VMEM((4 * R, R), BF),
            pltpu.VMEM((2, 2 * R, R), BF),
            pltpu.VMEM((2 * R, R), BF),
            pltpu.VMEM((2, 16, 5, 8, R), BF),
            pltpu.VMEM((16, 5, 8, R), BF),
            pltpu.VMEM((16, 5, 8, R), BF),
            pltpu.VMEM((16, 5, 8, R), BF),
            pltpu.VMEM((NZ, 2, 8, R), BF),
            pltpu.VMEM((NZ, 2, 8, R), BF),
            pltpu.VMEM((NZ, 2, 8, R), BF),
            pltpu.VMEM((5, 8, R), BF),
            pltpu.VMEM((NZ, 5, 8, R), BF),
            pltpu.VMEM((5, 8, R), BF),
            pltpu.VMEM((2, 2, NZ, 2, 8, R), BF),
            pltpu.VMEM((2, 16, 5, 8, R), BF),
            pltpu.VMEM((8, R), BF),
            pltpu.VMEM((8, H), F32),
            dma((22,)),
            dma((22,)),
            dma((8,)),
            dma((4,)),
        ],
        compiler_params=pltpu.CompilerParams(
            collective_id=0, has_side_effects=True, vmem_limit_bytes=VMEM_MOST
        ),
    )(
        window,
        window.reshape(1, 64),
        inputs_store,
        jac_store,
        targets_store.T,
        first_weight,
        first_bias.reshape(8, R),
        hidden_weight,
        hidden_bias.reshape(1, R),
        decoder_weight,
    )
    final = (
        jax.ShapeDtypeStruct((R, H), F32),
        jax.ShapeDtypeStruct((8, R), F32),
        jax.ShapeDtypeStruct((H, R), F32),
        jax.ShapeDtypeStruct((1, R), F32),
        dg,
    )
    fw, fb, hg, hb, dgo = pl.pallas_call(
        unfold,
        out_shape=final,
        in_specs=[hbm] * 4,
        out_specs=(hbm,) * 5,
        scratch_shapes=[pltpu.VMEM(a.shape, a.dtype) for a in raw + final[0:4]]
        + [dma((4,)), dma((5,))],
        compiler_params=pltpu.CompilerParams(vmem_limit_bytes=VMEM_MOST),
    )(*parts)
    return fw, fb.reshape(H), hg, hb.reshape(R), dgo


def solution(mesh):
    torus = Mesh(mesh.devices.reshape(NZ, 2, 2, 4, 2), ALL)
    return jax.shard_map(
        on_device,
        mesh=torus,
        in_specs=(
            P(),
            P(),
            P(None, ALL),
            P(None, ALL, None),
            P(),
            P(),
            P(None, MP),
            P(MP),
            P(ALL, None),
        ),
        out_specs=(P(), P(), P(None, MP), P(MP), P(ALL, None)),
        check_vma=False,
    )
```

```python
import jax
import jax.numpy as jnp
from jax import lax
from jax.experimental import pallas as pl
from jax.experimental.pallas import tpu as pltpu
from jax.sharding import Mesh
from jax.sharding import PartitionSpec as P

MESH = pl.DeviceIdType.MESH
DP = ("z", "xl", "c")
MP = ("y", "xh")
ALL = DP + MP
BF = jnp.bfloat16
F32 = jnp.float32

R = 128
H = 1024
NZ = 16
WIDE = H + R
VMEM_MOST = 67043328
NT = (((1,), (1,)), ((), ()))
TN = (((0,), (0,)), ((), ()))


def dot(a, b, dims=(((1,), (0,)), ((), ()))):
    return lax.dot_general(a, b, dims, preferred_element_type=F32)


def remote(src, dst, send, recv, to):
    return pltpu.make_async_remote_copy(
        src_ref=src, dst_ref=dst, send_sem=send, recv_sem=recv, device_id=to, device_id_type=MESH
    )


def each(n, body):
    def step(t, carry):
        body(t)
        return carry

    lax.fori_loop(0, n, step, 0)


def wrap(v, n):
    return jnp.where(v >= n, v - n, v)


FAR_FIRST = (8, 7, 9, 6, 10, 5, 11, 4, 12, 3, 13, 2, 14, 1, 15)
PLANE = sorted(
    (
        (dy, dh, dl)
        for dy in range(4)
        for dh in range(2)
        for dl in range(2)
        if dy + dh + dl > 0
    ),
    key=lambda d: -(min(d[0], 4 - d[0]) + (2 if d[1:] == (1, 0) else max(d[1:]))),
)


def kernel(
    ids_ref,
    idv_ref,
    xs_hbm,
    jac_hbm,
    tgt_hbm,
    w1_hbm,
    b1_hbm,
    hw_hbm,
    hb_hbm,
    dec_hbm,
    hall_hbm,
    fall_hbm,
    tile_hbm,
    dg_hbm,
    xs_ref,
    jac_ref,
    tgt_ref,
    w1_ref,
    b1_ref,
    hw_ref,
    hb_ref,
    dec_ref,
    ft,
    tsend,
    tfull,
    dsend,
    dblk,
    dmat,
    jsend,
    jbuf,
    net,
    tbytes,
    pbuf,
    rbuf,
    gsend,
    grecv,
    gown,
    hsend,
    hrecv,
    qsend,
    qpart,
    qsum,
    qrecv,
    fsend,
    fpart,
    fsum,
    frecv,
    zsend,
    zrecv,
    zall,
    ysend,
    yrecv,
    yall,
    hall,
    fall,
    tile,
    dg_ref,
    sent,
    came,
    taken,
    put,
):
    z, xl, c = lax.axis_index("z"), lax.axis_index("xl"), lax.axis_index("c")
    y, xh = lax.axis_index("y"), lax.axis_index("xh")
    m = y * 2 + xh
    q = m * 2 + xl
    b = c * NZ + z

    def plane(d):
        dy, dh, dl = d
        yy = wrap(y + dy, 4)
        hh = 1 - xh if dh else xh
        ll = 1 - xl if dl else xl
        return (yy * 2 + hh) * 2 + ll, {"y": yy, "xh": hh, "xl": ll}

    partner = {"c": 1 - c}
    barrier = pltpu.get_barrier_semaphore()

    homes = (
        (tgt_hbm, tgt_ref),
        (dec_hbm, dec_ref),
        (jac_hbm, jac_ref),
        (xs_hbm, xs_ref),
        (w1_hbm, w1_ref),
        (hw_hbm, hw_ref),
        (b1_hbm, b1_ref),
        (hb_hbm, hb_ref),
    )
    loads = [pltpu.make_async_copy(a, v, taken.at[k]) for k, (a, v) in enumerate(homes)]
    for load in loads:
        load.start()

    def greet(to):
        pl.semaphore_signal(barrier, inc=1, device_id=to, device_id_type=MESH)

    for d in FAR_FIRST:
        for cc in range(2):
            greet({"z": wrap(z + d, NZ), "c": cc})
    for d in PLANE:
        greet(plane(d)[1])
    greet(partner)

    hot = (lax.broadcasted_iota(jnp.int32, (512, 64), 0) == idv_ref[...]).astype(F32).astype(BF)
    for load in loads[0:2]:
        load.wait()
    dsend[:, 0:H] = dec_ref[...]
    dsend[:, H : H + 64] = dot(tgt_ref[...], hot).astype(BF)
    dsend[:, H + 64 :] = jnp.zeros((8, R - 64), BF)

    with jax.named_scope("barrier"):
        pl.semaphore_wait(barrier, 46)

    mine = pl.ds(pl.multiple_of(m * R, R), R)

    def tan_copy(to):
        return remote(
            tsend, tfull.at[xl, pl.ds(0, R + 16), mine], sent.at[0], came.at[0], to
        )

    def own_copy(d, k):
        return remote(
            dsend, dblk.at[c, z], sent.at[k], came.at[k], {"z": wrap(z + d, NZ)}
        )

    def pass_copy(block, d):
        part = dblk.at[c, wrap(z + block, NZ)]
        return remote(part, part, sent.at[2], came.at[2], {"z": wrap(z + d, NZ)})

    def half_copy(side):
        return remote(dblk.at[side], dblk.at[side], sent.at[3], came.at[3], partner)

    def jac_copy(zz, cc):
        return remote(
            jsend.at[cc * NZ + zz], jbuf.at[b], sent.at[4], came.at[4], {"z": zz, "c": cc}
        )

    def start_jac(ds):
        for d in ds:
            for cc in range(2):
                jac_copy(wrap(z + d, NZ), cc).start()

    def start_z(copy):
        for d in FAR_FIRST:
            copy(wrap(z + d, NZ)).start()

    xside = {"xl": 1 - xl}

    def recv(k, ref):
        with jax.named_scope(f"recv{k}"):
            remote(ref, ref, sent.at[k], came.at[k], partner).wait_recv()

    def left(k, ref):
        remote(ref, ref, sent.at[k], came.at[k], partner).wait_send()

    for d in (5, 11):
        own_copy(d, 1).start()
    for d in (1, 15):
        own_copy(d, 16).start()
    dblk[c, z] = dsend[...]
    loads[2].wait()

    def pick(zz):
        for cc in range(2):
            for i in range(2):
                jsend[cc * NZ + zz, i] = jac_ref[ids_ref[zz * 4 + cc * 2 + i]]

    each(NZ, pick)
    start_jac(FAR_FIRST[0:5])
    jbuf[b] = jsend[b]
    for load in loads[3:]:
        load.wait()

    own = ids_ref[z * 4 + c * 2 + xl]
    x_hot = (lax.broadcasted_iota(jnp.int32, (16, 512), 1) == own).astype(F32).astype(BF)
    x_rows = dot(x_hot, xs_ref[...])
    w1 = w1_ref[...].astype(F32)
    b1 = b1_ref[...].astype(F32)
    b1 = jnp.concatenate([b1[k : k + 1] for k in range(8)], axis=1)
    first_pre = dot(x_rows.astype(BF), w1_ref[...]) + b1
    first_act = jnp.tanh(first_pre)[0:1]
    first_slope = 1.0 - first_act * first_act
    top16 = lax.broadcasted_iota(jnp.int32, (16, H), 0) == 0
    ft[0:R, :] = (first_slope * w1).astype(BF)
    ft[R : R + 16, :] = jnp.where(top16, jnp.broadcast_to(first_act, (16, H)), 0.0).astype(BF)
    lin = dot(ft[...], hw_ref[...])
    hidden_lin = lin[0:R]
    hidden_act = jnp.tanh(lin[R : R + 1] + hb_ref[...].astype(F32))
    hidden_slope = 1.0 - hidden_act * hidden_act
    top = lax.broadcasted_iota(jnp.int32, (16, R), 0) == 0
    tsend[0:R, :] = (hidden_slope * hidden_lin).astype(BF)
    tsend[R : R + 16, :] = jnp.where(top, jnp.broadcast_to(hidden_act, (16, R)), 0.0).astype(BF)
    for d in PLANE:
        tan_copy(plane(d)[1]).start()
    tfull[:, R + 16 :, :] = jnp.zeros((2, 2 * R - R - 16, H), BF)
    tfull[xl, 0 : R + 16, mine] = tsend[...]

    recv(16, dblk.at[0, pl.ds(0, 2)])
    pass_copy(15, 1).start()
    pass_copy(1, 15).start()
    recv(1, dblk.at[0, pl.ds(0, 2)])
    for d in (2, 14, 1, 15):
        for block in (5, 11):
            pass_copy(block, d).start()
    odd = z % 2
    pass_copy(11 - 6 * odd, 3 + 10 * odd).start()
    start_jac(FAR_FIRST[5:])
    jac_copy(z, 1 - c).start()
    recv(2, dblk.at[0, pl.ds(0, 11)])
    half_copy(c).start()

    def unpack(side):
        rows = pl.ds(pl.multiple_of(side * R, R), R)
        dmat[rows, :] = dblk[side].astype(F32).reshape(R, WIDE).astype(BF)

    unpack(c)
    recv(0, tbytes.at[pl.ds(0, 15)])
    recv(3, dblk.at[0])
    unpack(1 - c)

    lane = lax.broadcasted_iota(jnp.int32, (2 * R, R), 1)
    tgt = dmat[:, H:].astype(F32)
    dec = dmat[:, 0:H]
    for i in range(2):
        want = jnp.sum(jnp.where(lane == z * 4 + c * 2 + i, tgt, 0.0), axis=1, keepdims=True)
        want = jnp.where(lane == 0, jnp.broadcast_to(want, (2 * R, R)), 0.0)
        out = dot(dec, tfull[i], NT)
        net[i, :, 0:R] = out[:, 0:R]
        net[i, :, R:] = out[:, R:] - want
    recv(4, jbuf.at[pl.ds(0, 31)])
    miss = []
    for i in range(2):
        stored = jbuf[:, i].astype(F32).reshape(2 * R, R)
        miss_i = jnp.concatenate([net[i, :, 0:R] - stored, net[i, :, R:]], axis=1).astype(BF)
        miss.append(miss_i)
        back_i = dot(miss_i, dec, TN)[0 : R + 8]
        for k in range(8):
            part = back_i[:, R * k : R * k + R]
            pbuf[i, k] = part.reshape(17, 8, R).astype(BF)
        for dy in (2, 1, 3, 0):
            for hh in range(2):
                yy = wrap(y + dy, 4)
                to = {"y": yy, "xh": hh, "xl": i}

                def send():
                    remote(
                        pbuf.at[i, yy * 2 + hh], rbuf.at[q], sent.at[5], came.at[5], to
                    ).start()

                if dy:
                    send()
                else:
                    pl.when((hh != xh) | (xl != i))(send)

    gown[...] = dot(miss[0], tfull[0]) + dot(miss[1], tfull[1])
    theirs = gown[pl.ds(pl.multiple_of((1 - c) * R, R), R), :]
    gsend[...] = theirs.reshape(NZ, 8, H).astype(BF)
    remote(gsend, grecv, sent.at[6], came.at[6], partner).start()
    ours = gown[pl.ds(pl.multiple_of(c * R, R), R), :].reshape(NZ, 8, H)
    recv(6, grecv)
    hsend[...] = (ours + grecv[...].astype(F32)).astype(BF)

    def gz_copy(peer):
        return remote(hsend.at[peer], hrecv.at[z], sent.at[7], came.at[7], {"z": peer})

    start_z(gz_copy)
    hrecv[z] = hsend[z]

    recv(5, rbuf.at[pl.ds(0, 15)])
    rbuf[q] = pbuf[xl, m]
    back = jnp.sum(rbuf[...].astype(F32), axis=0).reshape(R + 8, R)
    tan_back = back[0:R]
    act_back = back[R : R + 1]
    lin_round = (tan_back * hidden_slope).astype(BF)
    pre_back = act_back * hidden_slope - 2.0 * hidden_act * hidden_slope * jnp.sum(
        tan_back * hidden_lin, axis=0, keepdims=True
    )
    pre_round = jnp.where(top, jnp.broadcast_to(pre_back, (16, R)), 0.0).astype(BF)
    both = jnp.concatenate([lin_round, pre_round], axis=0)
    qsend[...] = dot(ft[...], both, TN).astype(BF).reshape(2, 4 * R, R)
    remote(qsend.at[1 - c], qpart, sent.at[8], came.at[8], partner).start()

    low = dot(both, hw_ref[...], NT)
    tan_lower = low[0:R]
    pre_lower = low[R : R + 1] * first_slope - 2.0 * first_act * first_slope * jnp.sum(
        tan_lower * w1, axis=0, keepdims=True
    )
    x_col = jnp.transpose(jnp.broadcast_to(x_rows[0:1], (R, R)))[:, 0:1]
    fw = x_col * pre_lower + tan_lower * first_slope
    place = lax.broadcasted_iota(jnp.int32, (8, H), 1) // R == m
    line = lax.broadcasted_iota(jnp.int32, (8, H), 0)
    pre_wide = jnp.concatenate([pre_back] * 8, axis=1)
    tail = jnp.where(line == 0, jnp.broadcast_to(pre_lower, (8, H)), 0.0)
    tail = tail + jnp.where((line == 1) & place, jnp.broadcast_to(pre_wide, (8, H)), 0.0)
    for cc in range(2):
        for k in range(16):
            r0 = 64 * cc + 32 * (k % 2)
            l0 = R * (k // 2)
            fsend[cc, k, 0:4] = fw[r0 : r0 + 32, l0 : l0 + R].reshape(4, 8, R).astype(BF)
            fsend[cc, k, 4] = tail[:, l0 : l0 + R].astype(BF)
    remote(fsend.at[1 - c], fpart, sent.at[9], came.at[9], partner).start()
    recv(8, qpart)
    halves = qsend[c].astype(F32) + qpart[...].astype(F32)
    qsum[...] = halves.astype(BF).reshape(2, 2 * R, R)
    remote(qsum.at[1 - xl], qrecv, sent.at[18], came.at[18], xside).start()
    recv(9, fpart)
    fsum[...] = (fsend[c].astype(F32) + fpart[...].astype(F32)).astype(BF)
    for d in PLANE:
        peer, to = plane(d)
        remote(fsum.at[peer], frecv.at[q], sent.at[17], came.at[17], to).start()
    frecv[q] = fsum[q]
    recv(18, qrecv)
    quarter = qsum[xl].astype(F32) + qrecv[...].astype(F32)
    zsend[...] = quarter.reshape(NZ, 2, 8, R).astype(BF)

    def zr_copy(peer):
        return remote(zsend.at[peer], zrecv.at[z], sent.at[10], came.at[10], {"z": peer})

    start_z(zr_copy)
    zrecv[z] = zsend[z]

    recv(17, frecv.at[pl.ds(0, 15)])
    ysend[...] = jnp.sum(frecv[...].astype(F32), axis=0).astype(BF)

    def y_copy(d, k):
        to = {"z": wrap(z + d, NZ)}
        return remote(ysend, yrecv.at[z], sent.at[k], came.at[k], to)

    def y_pass(block, d):
        part = yrecv.at[wrap(z + block, NZ)]
        return remote(part, part, sent.at[21], came.at[21], {"z": wrap(z + d, NZ)})

    for d in (5, 11):
        y_copy(d, 11).start()
    for d in (1, 15, 2, 14):
        y_copy(d, 13).start()
    yrecv[z] = ysend[...]

    recv(11, yrecv.at[pl.ds(0, 2)])
    for d in (2, 14, 1, 15):
        for block in (5, 11):
            y_pass(block, d).start()
    y_pass(11 - 6 * odd, 3 + 10 * odd).start()

    recv(10, zrecv.at[pl.ds(0, 15)])
    zall[z] = jnp.sum(zrecv[...].astype(F32), axis=0).astype(BF)

    def zg_copy(peer):
        return remote(zall.at[z], zall.at[z], sent.at[12], came.at[12], {"z": peer})

    start_z(zg_copy)

    recv(7, hrecv.at[pl.ds(0, 15)])
    dg_ref[...] = jnp.sum(hrecv[...].astype(F32), axis=0)
    outs = (
        pltpu.make_async_copy(dg_ref, dg_hbm, put.at[0]),
        pltpu.make_async_copy(tile, tile_hbm, put.at[1]),
        pltpu.make_async_copy(hall, hall_hbm.at[c], put.at[2]),
        pltpu.make_async_copy(fall, fall_hbm.at[c], put.at[3]),
    )
    outs[0].start()

    recv(13, yrecv.at[pl.ds(0, 4)])
    recv(21, yrecv.at[pl.ds(0, 9)])
    yall[...] = jnp.sum(yrecv[...].astype(F32), axis=0).astype(BF)
    for d in PLANE:
        remote(yall, fall.at[q], sent.at[15], came.at[15], plane(d)[1]).start()
    fall[q] = yall[...]
    tile[...] = yall[4]
    outs[1].start()
    recv(12, zall.at[pl.ds(0, 15)])
    remote(zall, hall.at[xl], sent.at[14], came.at[14], xside).start()
    hall[xl] = zall[...]
    recv(15, fall.at[pl.ds(0, 15)])
    remote(fall, fall_hbm.at[c], sent.at[19], came.at[19], partner).start()
    outs[3].start()
    recv(14, zall)
    remote(hall, hall_hbm.at[c], sent.at[20], came.at[20], partner).start()
    outs[2].start()
    recv(19, fall)
    recv(20, hall)

    left(0, tbytes.at[pl.ds(0, 15)])
    left(1, dblk.at[0, pl.ds(0, 2)])
    left(16, dblk.at[0, pl.ds(0, 2)])
    left(2, dblk.at[0, pl.ds(0, 11)])
    left(3, dblk.at[0])
    left(4, jbuf.at[pl.ds(0, 31)])
    left(5, rbuf.at[pl.ds(0, 15)])
    left(6, grecv)
    left(7, hrecv.at[pl.ds(0, 15)])
    left(8, qpart)
    left(9, fpart)
    left(17, frecv.at[pl.ds(0, 15)])
    left(18, qrecv)
    left(10, zrecv.at[pl.ds(0, 15)])

    left(11, yrecv.at[pl.ds(0, 2)])
    left(13, yrecv.at[pl.ds(0, 4)])
    left(21, yrecv.at[pl.ds(0, 9)])
    left(12, zrecv.at[pl.ds(0, 15)])
    left(14, zall)
    left(15, fall.at[pl.ds(0, 15)])
    left(19, fall)
    left(20, hall)
    for out in outs:
        out.wait()


def unfold(
    hall_hbm,
    fall_hbm,
    tile_hbm,
    dg_hbm,
    fw_hbm,
    fb_hbm,
    hg_hbm,
    hb_hbm,
    dgo_hbm,
    hall,
    fall,
    tile,
    dg,
    fw,
    fb,
    hg,
    hb,
    got,
    put,
):
    ins = (
        pltpu.make_async_copy(hall_hbm, hall, got.at[0]),
        pltpu.make_async_copy(fall_hbm, fall, got.at[1]),
        pltpu.make_async_copy(dg_hbm, dg, got.at[2]),
        pltpu.make_async_copy(tile_hbm, tile, got.at[3]),
    )
    outs = (
        pltpu.make_async_copy(hg, hg_hbm, put.at[0]),
        pltpu.make_async_copy(fw, fw_hbm, put.at[1]),
        pltpu.make_async_copy(dg, dgo_hbm, put.at[2]),
        pltpu.make_async_copy(hb, hb_hbm, put.at[3]),
        pltpu.make_async_copy(fb, fb_hbm, put.at[4]),
    )
    for copy in ins:
        copy.start()
    ins[0].wait()
    hg[...] = hall[...].astype(F32).reshape(H, R)
    outs[0].start()
    ins[1].wait()
    for mm in range(8):
        for ee in range(4):
            piece = fall[ee // 2, 2 * mm + ee % 2].astype(F32)
            fw[32 * ee : 32 * ee + 32, R * mm : R * mm + R] = piece[0:4].reshape(32, R)
            if ee == 0:
                fb[mm : mm + 1, :] = piece[4, 0:1]
    outs[1].start()
    outs[4].start()
    ins[2].wait()
    outs[2].start()
    ins[3].wait()
    hb[...] = tile[...].astype(F32)[1:2]
    outs[3].start()
    for copy in outs:
        copy.wait()


def on_device(
    inputs_store,
    window,
    targets_store,
    jac_store,
    first_weight,
    first_bias,
    hidden_weight,
    hidden_bias,
    decoder_weight,
):
    vmem = pl.BlockSpec(memory_space=pltpu.VMEM)
    smem = pl.BlockSpec(memory_space=pltpu.SMEM)
    hbm = pl.BlockSpec(memory_space=pltpu.HBM)
    dma = pltpu.SemaphoreType.DMA
    hall = jax.ShapeDtypeStruct((2, 2, NZ, 2, 8, R), BF)
    fall = jax.ShapeDtypeStruct((2, 16, 5, 8, R), BF)
    tile = jax.ShapeDtypeStruct((8, R), BF)
    dg = jax.ShapeDtypeStruct((8, H), F32)
    raw = (hall, fall, tile, dg)
    parts = pl.pallas_call(
        kernel,
        out_shape=raw,
        in_specs=[smem, vmem] + [hbm] * 8,
        out_specs=(hbm,) * 4,
        scratch_shapes=[
            pltpu.VMEM((512, R), BF),
            pltpu.VMEM((512, 8, R), BF),
            pltpu.VMEM((8, 512), BF),
            pltpu.VMEM((R, H), BF),
            pltpu.VMEM((8, R), BF),
            pltpu.VMEM((H, R), BF),
            pltpu.VMEM((1, R), BF),
            pltpu.VMEM((8, H), BF),
            pltpu.VMEM((R + 16, H), BF),
            pltpu.VMEM((R + 16, R), BF),
            pltpu.VMEM((2, 2 * R, H), BF),
            pltpu.VMEM((8, WIDE), BF),
            pltpu.VMEM((2, NZ, 8, WIDE), BF),
            pltpu.VMEM((2 * R, WIDE), BF),
            pltpu.VMEM((32, 2, 8, R), BF),
            pltpu.VMEM((32, 2, 8, R), BF),
            pltpu.VMEM((2, 2 * R, 2 * R), F32),
            pltpu.VMEM((16, R + 16, R), BF),
            pltpu.VMEM((2, 8, 17, 8, R), BF),
            pltpu.VMEM((16, 17, 8, R), BF),
            pltpu.VMEM((NZ, 8, H), BF),
            pltpu.VMEM((NZ, 8, H), BF),
            pltpu.VMEM((2 * R, H), F32),
            pltpu.VMEM((NZ, 8, H), BF),
            pltpu.VMEM((NZ, 8, H), BF),
            pltpu.VMEM((2, 4 * R, R), BF),
            pltpu.VMEM((4 * R, R), BF),
            pltpu.VMEM((2, 2 * R, R), BF),
            pltpu.VMEM((2 * R, R), BF),
            pltpu.VMEM((2, 16, 5, 8, R), BF),
            pltpu.VMEM((16, 5, 8, R), BF),
            pltpu.VMEM((16, 5, 8, R), BF),
            pltpu.VMEM((16, 5, 8, R), BF),
            pltpu.VMEM((NZ, 2, 8, R), BF),
            pltpu.VMEM((NZ, 2, 8, R), BF),
            pltpu.VMEM((NZ, 2, 8, R), BF),
            pltpu.VMEM((5, 8, R), BF),
            pltpu.VMEM((NZ, 5, 8, R), BF),
            pltpu.VMEM((5, 8, R), BF),
            pltpu.VMEM((2, NZ, 2, 8, R), BF),
            pltpu.VMEM((16, 5, 8, R), BF),
            pltpu.VMEM((8, R), BF),
            pltpu.VMEM((8, H), F32),
            dma((22,)),
            dma((22,)),
            dma((8,)),
            dma((4,)),
        ],
        compiler_params=pltpu.CompilerParams(
            collective_id=0, has_side_effects=True, vmem_limit_bytes=VMEM_MOST
        ),
    )(
        window,
        window.reshape(1, 64),
        inputs_store,
        jac_store,
        targets_store.T,
        first_weight,
        first_bias.reshape(8, R),
        hidden_weight,
        hidden_bias.reshape(1, R),
        decoder_weight,
    )
    final = (
        jax.ShapeDtypeStruct((R, H), F32),
        jax.ShapeDtypeStruct((8, R), F32),
        jax.ShapeDtypeStruct((H, R), F32),
        jax.ShapeDtypeStruct((1, R), F32),
        dg,
    )
    fw, fb, hg, hb, dgo = pl.pallas_call(
        unfold,
        out_shape=final,
        in_specs=[hbm] * 4,
        out_specs=(hbm,) * 5,
        scratch_shapes=[pltpu.VMEM(a.shape, a.dtype) for a in raw + final[0:4]]
        + [dma((4,)), dma((5,))],
        compiler_params=pltpu.CompilerParams(vmem_limit_bytes=VMEM_MOST),
    )(*parts)
    return fw, fb.reshape(H), hg, hb.reshape(R), dgo


def solution(mesh):
    torus = Mesh(mesh.devices.reshape(NZ, 2, 2, 4, 2), ALL)
    return jax.shard_map(
        on_device,
        mesh=torus,
        in_specs=(
            P(),
            P(),
            P(None, ALL),
            P(None, ALL, None),
            P(),
            P(),
            P(None, MP),
            P(MP),
            P(ALL, None),
        ),
        out_specs=(P(), P(), P(None, MP), P(MP), P(ALL, None)),
        check_vma=False,
    )
```

```python
import jax
import jax.numpy as jnp
from jax import lax
from jax.experimental import pallas as pl
from jax.experimental.pallas import tpu as pltpu
from jax.sharding import Mesh
from jax.sharding import PartitionSpec as P

MESH = pl.DeviceIdType.MESH
DP = ("z", "xl", "c")
MP = ("y", "xh")
ALL = DP + MP
BF = jnp.bfloat16
F32 = jnp.float32

R = 128
H = 1024
NZ = 16
WIDE = H + R
VMEM_MOST = 67043328
NT = (((1,), (1,)), ((), ()))
TN = (((0,), (0,)), ((), ()))


def dot(a, b, dims=(((1,), (0,)), ((), ()))):
    return lax.dot_general(a, b, dims, preferred_element_type=F32)


def remote(src, dst, send, recv, to):
    return pltpu.make_async_remote_copy(
        src_ref=src, dst_ref=dst, send_sem=send, recv_sem=recv, device_id=to, device_id_type=MESH
    )


def each(n, body):
    def step(t, carry):
        body(t)
        return carry

    lax.fori_loop(0, n, step, 0)


def wrap(v, n):
    return jnp.where(v >= n, v - n, v)


FAR_FIRST = (8, 7, 9, 6, 10, 5, 11, 4, 12, 3, 13, 2, 14, 1, 15)
LOW_FIRST = (0, 1, 2, 3, 4, 5, 6, 7, 15, 14, 13, 12, 8, 11, 9, 10)
PLANE = sorted(
    (
        (dy, dh, dl)
        for dy in range(4)
        for dh in range(2)
        for dl in range(2)
        if dy + dh + dl > 0
    ),
    key=lambda d: -(min(d[0], 4 - d[0]) + (2 if d[1:] == (1, 0) else max(d[1:]))),
)


def kernel(
    ids_ref,
    idv_ref,
    xs_hbm,
    jac_hbm,
    tgt_hbm,
    w1_hbm,
    b1_hbm,
    hw_hbm,
    hb_hbm,
    dec_hbm,
    hall_hbm,
    fall_hbm,
    tile_hbm,
    dg_hbm,
    xs_ref,
    jac_ref,
    tgt_ref,
    w1_ref,
    b1_ref,
    hw_ref,
    hb_ref,
    dec_ref,
    ft,
    tsend,
    tfull,
    dsend,
    dblk,
    dmat,
    jsend,
    jbuf,
    net,
    tbytes,
    pbuf,
    rbuf,
    gsend,
    grecv,
    gown,
    hsend,
    hrecv,
    qsend,
    qpart,
    qsum,
    qrecv,
    fsend,
    fpart,
    fsum,
    frecv,
    zsend,
    zrecv,
    zall,
    ysend,
    yrecv,
    yall,
    hall,
    fall,
    tile,
    dg_ref,
    sent,
    came,
    taken,
    put,
):
    z, xl, c = lax.axis_index("z"), lax.axis_index("xl"), lax.axis_index("c")
    y, xh = lax.axis_index("y"), lax.axis_index("xh")
    m = y * 2 + xh
    q = m * 2 + xl
    b = c * NZ + z

    def plane(d):
        dy, dh, dl = d
        yy = wrap(y + dy, 4)
        hh = 1 - xh if dh else xh
        ll = 1 - xl if dl else xl
        return (yy * 2 + hh) * 2 + ll, {"y": yy, "xh": hh, "xl": ll}

    partner = {"c": 1 - c}
    barrier = pltpu.get_barrier_semaphore()

    homes = (
        (tgt_hbm, tgt_ref),
        (dec_hbm, dec_ref),
        (jac_hbm, jac_ref),
        (xs_hbm, xs_ref),
        (w1_hbm, w1_ref),
        (hw_hbm, hw_ref),
        (b1_hbm, b1_ref),
        (hb_hbm, hb_ref),
    )
    loads = [pltpu.make_async_copy(a, v, taken.at[k]) for k, (a, v) in enumerate(homes)]
    for load in loads:
        load.start()

    def greet(to):
        pl.semaphore_signal(barrier, inc=1, device_id=to, device_id_type=MESH)

    for d in FAR_FIRST:
        for cc in range(2):
            greet({"z": wrap(z + d, NZ), "c": cc})
    for d in PLANE:
        greet(plane(d)[1])
    greet(partner)

    hot = (lax.broadcasted_iota(jnp.int32, (512, 64), 0) == idv_ref[...]).astype(F32).astype(BF)
    for load in loads[0:2]:
        load.wait()
    dsend[:, 0:H] = dec_ref[...]
    dsend[:, H : H + 64] = dot(tgt_ref[...], hot).astype(BF)
    dsend[:, H + 64 :] = jnp.zeros((8, R - 64), BF)

    with jax.named_scope("barrier"):
        pl.semaphore_wait(barrier, 46)

    mine = pl.ds(pl.multiple_of(m * R, R), R)

    def tan_copy(to):
        return remote(
            tsend, tfull.at[xl, pl.ds(0, R + 16), mine], sent.at[0], came.at[0], to
        )

    def own_copy(d, k):
        return remote(
            dsend, dblk.at[c, z], sent.at[k], came.at[k], {"z": wrap(z + d, NZ)}
        )

    def pass_copy(block, d):
        part = dblk.at[c, wrap(z + block, NZ)]
        return remote(part, part, sent.at[2], came.at[2], {"z": wrap(z + d, NZ)})

    def half_copy(side):
        return remote(dblk.at[side], dblk.at[side], sent.at[3], came.at[3], partner)

    def jac_copy(zz, cc):
        return remote(
            jsend.at[cc * NZ + zz], jbuf.at[b], sent.at[4], came.at[4], {"z": zz, "c": cc}
        )

    def start_jac(ds):
        for d in ds:
            for cc in range(2):
                jac_copy(wrap(z + d, NZ), cc).start()

    def start_z(copy):
        for d in FAR_FIRST:
            copy(wrap(z + d, NZ)).start()

    xside = {"xl": 1 - xl}

    def recv(k, ref):
        with jax.named_scope(f"recv{k}"):
            remote(ref, ref, sent.at[k], came.at[k], partner).wait_recv()

    def left(k, ref):
        remote(ref, ref, sent.at[k], came.at[k], partner).wait_send()

    for d in (5, 11):
        own_copy(d, 1).start()
    for d in (1, 15, 2, 14):
        own_copy(d, 16).start()
    dblk[c, z] = dsend[...]
    loads[2].wait()

    def pick(zz):
        for cc in range(2):
            for i in range(2):
                jsend[cc * NZ + zz, i] = jac_ref[ids_ref[zz * 4 + cc * 2 + i]]

    each(NZ, pick)
    start_jac(FAR_FIRST[0:5])
    jbuf[b] = jsend[b]
    for load in loads[3:]:
        load.wait()

    own = ids_ref[z * 4 + c * 2 + xl]
    x_hot = (lax.broadcasted_iota(jnp.int32, (16, 512), 1) == own).astype(F32).astype(BF)
    x_rows = dot(x_hot, xs_ref[...])
    w1 = w1_ref[...].astype(F32)
    b1 = b1_ref[...].astype(F32)
    b1 = jnp.concatenate([b1[k : k + 1] for k in range(8)], axis=1)
    first_pre = dot(x_rows.astype(BF), w1_ref[...]) + b1
    first_act = jnp.tanh(first_pre)[0:1]
    first_slope = 1.0 - first_act * first_act
    top16 = lax.broadcasted_iota(jnp.int32, (16, H), 0) == 0
    ft[0:R, :] = (first_slope * w1).astype(BF)
    ft[R : R + 16, :] = jnp.where(top16, jnp.broadcast_to(first_act, (16, H)), 0.0).astype(BF)
    lin = dot(ft[...], hw_ref[...])
    hidden_lin = lin[0:R]
    hidden_act = jnp.tanh(lin[R : R + 1] + hb_ref[...].astype(F32))
    hidden_slope = 1.0 - hidden_act * hidden_act
    top = lax.broadcasted_iota(jnp.int32, (16, R), 0) == 0
    tsend[0:R, :] = (hidden_slope * hidden_lin).astype(BF)
    tsend[R : R + 16, :] = jnp.where(top, jnp.broadcast_to(hidden_act, (16, R)), 0.0).astype(BF)
    for d in PLANE:
        tan_copy(plane(d)[1]).start()
    tfull[:, R + 16 :, :] = jnp.zeros((2, 2 * R - R - 16, H), BF)
    tfull[xl, 0 : R + 16, mine] = tsend[...]

    recv(1, dblk.at[0, pl.ds(0, 2)])
    for d in (2, 14, 1, 15):
        for block in (5, 11):
            pass_copy(block, d).start()
    odd = z % 2
    pass_copy(11 - 6 * odd, 3 + 10 * odd).start()
    start_jac(FAR_FIRST[5:])
    jac_copy(z, 1 - c).start()
    recv(16, dblk.at[0, pl.ds(0, 4)])
    recv(2, dblk.at[0, pl.ds(0, 9)])
    half_copy(c).start()

    def unpack(side):
        rows = pl.ds(pl.multiple_of(side * R, R), R)
        dmat[rows, :] = dblk[side].astype(F32).reshape(R, WIDE).astype(BF)

    unpack(c)
    recv(0, tbytes.at[pl.ds(0, 15)])
    recv(3, dblk.at[0])
    unpack(1 - c)

    lane = lax.broadcasted_iota(jnp.int32, (2 * R, R), 1)
    tgt = dmat[:, H:].astype(F32)
    dec = dmat[:, 0:H]
    for i in range(2):
        want = jnp.sum(jnp.where(lane == z * 4 + c * 2 + i, tgt, 0.0), axis=1, keepdims=True)
        want = jnp.where(lane == 0, jnp.broadcast_to(want, (2 * R, R)), 0.0)
        out = dot(dec, tfull[i], NT)
        net[i, :, 0:R] = out[:, 0:R]
        net[i, :, R:] = out[:, R:] - want
    recv(4, jbuf.at[pl.ds(0, 31)])
    miss = []
    for i in range(2):
        stored = jbuf[:, i].astype(F32).reshape(2 * R, R)
        miss_i = jnp.concatenate([net[i, :, 0:R] - stored, net[i, :, R:]], axis=1).astype(BF)
        miss.append(miss_i)
        back_i = dot(miss_i, dec, TN)[0 : R + 8]
        for k in range(8):
            part = back_i[:, R * k : R * k + R]
            pbuf[i, k] = part.reshape(17, 8, R).astype(BF)
        for dy in (2, 1, 3, 0):
            for hh in range(2):
                yy = wrap(y + dy, 4)
                to = {"y": yy, "xh": hh, "xl": i}

                def send():
                    remote(
                        pbuf.at[i, yy * 2 + hh], rbuf.at[q], sent.at[5], came.at[5], to
                    ).start()

                if dy:
                    send()
                else:
                    pl.when((hh != xh) | (xl != i))(send)

    gown[...] = dot(miss[0], tfull[0]) + dot(miss[1], tfull[1])
    theirs = gown[pl.ds(pl.multiple_of((1 - c) * R, R), R), :]
    gsend[...] = theirs.reshape(NZ, 8, H).astype(BF)
    remote(gsend, grecv, sent.at[6], came.at[6], partner).start()
    ours = gown[pl.ds(pl.multiple_of(c * R, R), R), :].reshape(NZ, 8, H)
    recv(6, grecv)
    hsend[...] = (ours + grecv[...].astype(F32)).astype(BF)

    def gz_copy(peer):
        return remote(hsend.at[peer], hrecv.at[z], sent.at[7], came.at[7], {"z": peer})

    start_z(gz_copy)
    hrecv[z] = hsend[z]

    recv(5, rbuf.at[pl.ds(0, 15)])
    rbuf[q] = pbuf[xl, m]
    back = jnp.sum(rbuf[...].astype(F32), axis=0).reshape(R + 8, R)
    tan_back = back[0:R]
    act_back = back[R : R + 1]
    lin_round = (tan_back * hidden_slope).astype(BF)
    pre_back = act_back * hidden_slope - 2.0 * hidden_act * hidden_slope * jnp.sum(
        tan_back * hidden_lin, axis=0, keepdims=True
    )
    pre_round = jnp.where(top, jnp.broadcast_to(pre_back, (16, R)), 0.0).astype(BF)
    both = jnp.concatenate([lin_round, pre_round], axis=0)
    qsend[...] = dot(ft[...], both, TN).astype(BF).reshape(2, 4 * R, R)
    remote(qsend.at[1 - c], qpart, sent.at[8], came.at[8], partner).start()

    low = dot(both, hw_ref[...], NT)
    tan_lower = low[0:R]
    pre_lower = low[R : R + 1] * first_slope - 2.0 * first_act * first_slope * jnp.sum(
        tan_lower * w1, axis=0, keepdims=True
    )
    x_col = jnp.transpose(jnp.broadcast_to(x_rows[0:1], (R, R)))[:, 0:1]
    fw = x_col * pre_lower + tan_lower * first_slope
    place = lax.broadcasted_iota(jnp.int32, (8, H), 1) // R == m
    line = lax.broadcasted_iota(jnp.int32, (8, H), 0)
    pre_wide = jnp.concatenate([pre_back] * 8, axis=1)
    tail = jnp.where(line == 0, jnp.broadcast_to(pre_lower, (8, H)), 0.0)
    tail = tail + jnp.where((line == 1) & place, jnp.broadcast_to(pre_wide, (8, H)), 0.0)
    for cc in range(2):
        for k in range(16):
            r0 = 64 * cc + 32 * (k % 2)
            l0 = R * (k // 2)
            fsend[cc, k, 0:4] = fw[r0 : r0 + 32, l0 : l0 + R].reshape(4, 8, R).astype(BF)
            fsend[cc, k, 4] = tail[:, l0 : l0 + R].astype(BF)
    remote(fsend.at[1 - c], fpart, sent.at[9], came.at[9], partner).start()
    recv(8, qpart)
    halves = qsend[c].astype(F32) + qpart[...].astype(F32)
    qsum[...] = halves.astype(BF).reshape(2, 2 * R, R)
    remote(qsum.at[1 - xl], qrecv, sent.at[18], came.at[18], xside).start()
    recv(9, fpart)
    fsum[...] = (fsend[c].astype(F32) + fpart[...].astype(F32)).astype(BF)
    for d in PLANE:
        peer, to = plane(d)
        remote(fsum.at[peer], frecv.at[q], sent.at[17], came.at[17], to).start()
    frecv[q] = fsum[q]
    recv(18, qrecv)
    quarter = qsum[xl].astype(F32) + qrecv[...].astype(F32)
    zsend[...] = quarter.reshape(NZ, 2, 8, R).astype(BF)

    def zr_copy(peer):
        return remote(zsend.at[peer], zrecv.at[z], sent.at[10], came.at[10], {"z": peer})

    start_z(zr_copy)
    zrecv[z] = zsend[z]

    recv(17, frecv.at[pl.ds(0, 15)])
    ysend[...] = jnp.sum(frecv[...].astype(F32), axis=0).astype(BF)
    for t in range(5):

        @pl.when(z != t)
        def _():
            remote(ysend.at[t], yrecv.at[z], sent.at[11], came.at[11], {"z": t}).start()

        @pl.when(z == t)
        def _():
            yrecv[z] = ysend[t]

    def low_first(copy):
        for zz in LOW_FIRST:
            pl.when(z != zz)(lambda: copy({"z": zz}).start())

    def y_copy(to):
        return remote(yall.at[z], yall.at[z], sent.at[13], came.at[13], to)

    def zg_copy(to):
        return remote(zall.at[z], zall.at[z], sent.at[12], came.at[12], to)

    @pl.when(z < 5)
    def _():
        recv(11, yrecv.at[pl.ds(0, 15)])
        yall[z] = jnp.sum(yrecv[...].astype(F32), axis=0).astype(BF)
        low_first(y_copy)

    recv(10, zrecv.at[pl.ds(0, 15)])
    zall[z] = jnp.sum(zrecv[...].astype(F32), axis=0).astype(BF)
    low_first(zg_copy)

    recv(7, hrecv.at[pl.ds(0, 15)])
    dg_ref[...] = jnp.sum(hrecv[...].astype(F32), axis=0)
    outs = (
        pltpu.make_async_copy(dg_ref, dg_hbm, put.at[0]),
        pltpu.make_async_copy(tile, tile_hbm, put.at[1]),
        pltpu.make_async_copy(hall, hall_hbm, put.at[2]),
        pltpu.make_async_copy(fall, fall_hbm, put.at[3]),
    )
    outs[0].start()

    @pl.when(z < 5)
    def _():
        recv(13, yall.at[pl.ds(0, 4)])

    @pl.when(z >= 5)
    def _():
        recv(13, yall.at[pl.ds(0, 5)])

    for d in PLANE:
        remote(
            yall.at[pl.ds(0, 5)], fall.at[c, q], sent.at[15], came.at[15], plane(d)[1]
        ).start()
    fall[c, q] = yall[0:5]
    tile[...] = yall[4]
    outs[1].start()
    recv(12, zall.at[pl.ds(0, 15)])
    remote(zall, hall.at[c, xl], sent.at[14], came.at[14], xside).start()
    hall[c, xl] = zall[...]
    recv(15, fall.at[0, pl.ds(0, 15)])
    remote(fall.at[c], fall.at[c], sent.at[19], came.at[19], partner).start()
    recv(14, zall)
    remote(hall.at[c], hall.at[c], sent.at[20], came.at[20], partner).start()
    recv(19, fall.at[0])
    outs[3].start()
    recv(20, hall.at[0])
    outs[2].start()

    left(0, tbytes.at[pl.ds(0, 15)])
    left(1, dblk.at[0, pl.ds(0, 2)])
    left(16, dblk.at[0, pl.ds(0, 4)])
    left(2, dblk.at[0, pl.ds(0, 9)])
    left(3, dblk.at[0])
    left(4, jbuf.at[pl.ds(0, 31)])
    left(5, rbuf.at[pl.ds(0, 15)])
    left(6, grecv)
    left(7, hrecv.at[pl.ds(0, 15)])
    left(8, qpart)
    left(9, fpart)
    left(17, frecv.at[pl.ds(0, 15)])
    left(18, qrecv)
    left(10, zrecv.at[pl.ds(0, 15)])

    @pl.when(z < 5)
    def _():
        left(11, yall.at[pl.ds(0, 4)])
        left(13, yrecv.at[pl.ds(0, 15)])

    @pl.when(z >= 5)
    def _():
        left(11, yall.at[pl.ds(0, 5)])

    left(12, zrecv.at[pl.ds(0, 15)])
    left(14, zall)
    left(15, fall.at[0, pl.ds(0, 15)])
    left(19, fall.at[0])
    left(20, hall.at[0])
    for out in outs:
        out.wait()


def unfold(
    hall_hbm,
    fall_hbm,
    tile_hbm,
    dg_hbm,
    fw_hbm,
    fb_hbm,
    hg_hbm,
    hb_hbm,
    dgo_hbm,
    hall,
    fall,
    tile,
    dg,
    fw,
    fb,
    hg,
    hb,
    got,
    put,
):
    ins = (
        pltpu.make_async_copy(hall_hbm, hall, got.at[0]),
        pltpu.make_async_copy(fall_hbm, fall, got.at[1]),
        pltpu.make_async_copy(dg_hbm, dg, got.at[2]),
        pltpu.make_async_copy(tile_hbm, tile, got.at[3]),
    )
    outs = (
        pltpu.make_async_copy(hg, hg_hbm, put.at[0]),
        pltpu.make_async_copy(fw, fw_hbm, put.at[1]),
        pltpu.make_async_copy(dg, dgo_hbm, put.at[2]),
        pltpu.make_async_copy(hb, hb_hbm, put.at[3]),
        pltpu.make_async_copy(fb, fb_hbm, put.at[4]),
    )
    for copy in ins:
        copy.start()
    ins[0].wait()
    hg[...] = hall[...].astype(F32).reshape(H, R)
    outs[0].start()
    ins[1].wait()
    for mm in range(8):
        for ee in range(4):
            piece = fall[ee // 2, 2 * mm + ee % 2].astype(F32)
            fw[32 * ee : 32 * ee + 32, R * mm : R * mm + R] = piece[0:4].reshape(32, R)
            if ee == 0:
                fb[mm : mm + 1, :] = piece[4, 0:1]
    outs[1].start()
    outs[4].start()
    ins[2].wait()
    outs[2].start()
    ins[3].wait()
    hb[...] = tile[...].astype(F32)[1:2]
    outs[3].start()
    for copy in outs:
        copy.wait()


def on_device(
    inputs_store,
    window,
    targets_store,
    jac_store,
    first_weight,
    first_bias,
    hidden_weight,
    hidden_bias,
    decoder_weight,
):
    vmem = pl.BlockSpec(memory_space=pltpu.VMEM)
    smem = pl.BlockSpec(memory_space=pltpu.SMEM)
    hbm = pl.BlockSpec(memory_space=pltpu.HBM)
    dma = pltpu.SemaphoreType.DMA
    hall = jax.ShapeDtypeStruct((2, 2, NZ, 2, 8, R), BF)
    fall = jax.ShapeDtypeStruct((2, 16, 5, 8, R), BF)
    tile = jax.ShapeDtypeStruct((8, R), BF)
    dg = jax.ShapeDtypeStruct((8, H), F32)
    raw = (hall, fall, tile, dg)
    parts = pl.pallas_call(
        kernel,
        out_shape=raw,
        in_specs=[smem, vmem] + [hbm] * 8,
        out_specs=(hbm,) * 4,
        scratch_shapes=[
            pltpu.VMEM((512, R), BF),
            pltpu.VMEM((512, 8, R), BF),
            pltpu.VMEM((8, 512), BF),
            pltpu.VMEM((R, H), BF),
            pltpu.VMEM((8, R), BF),
            pltpu.VMEM((H, R), BF),
            pltpu.VMEM((1, R), BF),
            pltpu.VMEM((8, H), BF),
            pltpu.VMEM((R + 16, H), BF),
            pltpu.VMEM((R + 16, R), BF),
            pltpu.VMEM((2, 2 * R, H), BF),
            pltpu.VMEM((8, WIDE), BF),
            pltpu.VMEM((2, NZ, 8, WIDE), BF),
            pltpu.VMEM((2 * R, WIDE), BF),
            pltpu.VMEM((32, 2, 8, R), BF),
            pltpu.VMEM((32, 2, 8, R), BF),
            pltpu.VMEM((2, 2 * R, 2 * R), F32),
            pltpu.VMEM((16, R + 16, R), BF),
            pltpu.VMEM((2, 8, 17, 8, R), BF),
            pltpu.VMEM((16, 17, 8, R), BF),
            pltpu.VMEM((NZ, 8, H), BF),
            pltpu.VMEM((NZ, 8, H), BF),
            pltpu.VMEM((2 * R, H), F32),
            pltpu.VMEM((NZ, 8, H), BF),
            pltpu.VMEM((NZ, 8, H), BF),
            pltpu.VMEM((2, 4 * R, R), BF),
            pltpu.VMEM((4 * R, R), BF),
            pltpu.VMEM((2, 2 * R, R), BF),
            pltpu.VMEM((2 * R, R), BF),
            pltpu.VMEM((2, 16, 5, 8, R), BF),
            pltpu.VMEM((16, 5, 8, R), BF),
            pltpu.VMEM((16, 5, 8, R), BF),
            pltpu.VMEM((16, 5, 8, R), BF),
            pltpu.VMEM((NZ, 2, 8, R), BF),
            pltpu.VMEM((NZ, 2, 8, R), BF),
            pltpu.VMEM((NZ, 2, 8, R), BF),
            pltpu.VMEM((5, 8, R), BF),
            pltpu.VMEM((NZ, 8, R), BF),
            pltpu.VMEM((NZ, 8, R), BF),
            pltpu.VMEM((2, 2, NZ, 2, 8, R), BF),
            pltpu.VMEM((2, 16, 5, 8, R), BF),
            pltpu.VMEM((8, R), BF),
            pltpu.VMEM((8, H), F32),
            dma((21,)),
            dma((21,)),
            dma((8,)),
            dma((4,)),
        ],
        compiler_params=pltpu.CompilerParams(
            collective_id=0, has_side_effects=True, vmem_limit_bytes=VMEM_MOST
        ),
    )(
        window,
        window.reshape(1, 64),
        inputs_store,
        jac_store,
        targets_store.T,
        first_weight,
        first_bias.reshape(8, R),
        hidden_weight,
        hidden_bias.reshape(1, R),
        decoder_weight,
    )
    final = (
        jax.ShapeDtypeStruct((R, H), F32),
        jax.ShapeDtypeStruct((8, R), F32),
        jax.ShapeDtypeStruct((H, R), F32),
        jax.ShapeDtypeStruct((1, R), F32),
        dg,
    )
    fw, fb, hg, hb, dgo = pl.pallas_call(
        unfold,
        out_shape=final,
        in_specs=[hbm] * 4,
        out_specs=(hbm,) * 5,
        scratch_shapes=[pltpu.VMEM(a.shape, a.dtype) for a in raw + final[0:4]]
        + [dma((4,)), dma((5,))],
        compiler_params=pltpu.CompilerParams(vmem_limit_bytes=VMEM_MOST),
    )(*parts)
    return fw, fb.reshape(H), hg, hb.reshape(R), dgo


def solution(mesh):
    torus = Mesh(mesh.devices.reshape(NZ, 2, 2, 4, 2), ALL)
    return jax.shard_map(
        on_device,
        mesh=torus,
        in_specs=(
            P(),
            P(),
            P(None, ALL),
            P(None, ALL, None),
            P(),
            P(),
            P(None, MP),
            P(MP),
            P(ALL, None),
        ),
        out_specs=(P(), P(), P(None, MP), P(MP), P(ALL, None)),
        check_vma=False,
    )
```

```python
import jax
import jax.numpy as jnp
from jax import lax
from jax.experimental import pallas as pl
from jax.experimental.pallas import tpu as pltpu
from jax.sharding import Mesh
from jax.sharding import PartitionSpec as P

MESH = pl.DeviceIdType.MESH
DP = ("z", "xl", "c")
MP = ("y", "xh")
ALL = DP + MP
BF = jnp.bfloat16
F32 = jnp.float32

R = 128
H = 1024
NZ = 16
WIDE = H + R
VMEM_MOST = 67043328
NT = (((1,), (1,)), ((), ()))
TN = (((0,), (0,)), ((), ()))


def dot(a, b, dims=(((1,), (0,)), ((), ()))):
    return lax.dot_general(a, b, dims, preferred_element_type=F32)


def remote(src, dst, send, recv, to):
    return pltpu.make_async_remote_copy(
        src_ref=src, dst_ref=dst, send_sem=send, recv_sem=recv, device_id=to, device_id_type=MESH
    )


def each(n, body):
    def step(t, carry):
        body(t)
        return carry

    lax.fori_loop(0, n, step, 0)


def wrap(v, n):
    return jnp.where(v >= n, v - n, v)


FAR_FIRST = (8, 7, 9, 6, 10, 5, 11, 4, 12, 3, 13, 2, 14, 1, 15)
LOW_FIRST = (0, 1, 2, 3, 4, 5, 6, 7, 15, 14, 13, 12, 8, 11, 9, 10)
PLANE = sorted(
    (
        (dy, dh, dl)
        for dy in range(4)
        for dh in range(2)
        for dl in range(2)
        if dy + dh + dl > 0
    ),
    key=lambda d: -(min(d[0], 4 - d[0]) + (2 if d[1:] == (1, 0) else max(d[1:]))),
)


def kernel(
    ids_ref,
    idv_ref,
    xs_hbm,
    jac_hbm,
    tgt_hbm,
    w1_hbm,
    b1_hbm,
    hw_hbm,
    hb_hbm,
    dec_hbm,
    hall_hbm,
    fall_hbm,
    tile_hbm,
    dg_hbm,
    xs_ref,
    jac_ref,
    tgt_ref,
    w1_ref,
    b1_ref,
    hw_ref,
    hb_ref,
    dec_ref,
    ft,
    tsend,
    tfull,
    dsend,
    dblk,
    dmat,
    jsend,
    jbuf,
    net,
    tbytes,
    pbuf,
    rbuf,
    gsend,
    grecv,
    gown,
    hsend,
    hrecv,
    qsend,
    qpart,
    qsum,
    qrecv,
    fsend,
    fpart,
    fsum,
    frecv,
    zsend,
    zrecv,
    zall,
    ysend,
    yrecv,
    yall,
    hall,
    fall,
    tile,
    dg_ref,
    sent,
    came,
    taken,
    put,
):
    z, xl, c = lax.axis_index("z"), lax.axis_index("xl"), lax.axis_index("c")
    y, xh = lax.axis_index("y"), lax.axis_index("xh")
    m = y * 2 + xh
    q = m * 2 + xl
    b = c * NZ + z

    def plane(d):
        dy, dh, dl = d
        yy = wrap(y + dy, 4)
        hh = 1 - xh if dh else xh
        ll = 1 - xl if dl else xl
        return (yy * 2 + hh) * 2 + ll, {"y": yy, "xh": hh, "xl": ll}

    partner = {"c": 1 - c}
    barrier = pltpu.get_barrier_semaphore()

    homes = (
        (tgt_hbm, tgt_ref),
        (dec_hbm, dec_ref),
        (jac_hbm, jac_ref),
        (xs_hbm, xs_ref),
        (w1_hbm, w1_ref),
        (hw_hbm, hw_ref),
        (b1_hbm, b1_ref),
        (hb_hbm, hb_ref),
    )
    loads = [pltpu.make_async_copy(a, v, taken.at[k]) for k, (a, v) in enumerate(homes)]
    for load in loads:
        load.start()

    def greet(to):
        pl.semaphore_signal(barrier, inc=1, device_id=to, device_id_type=MESH)

    for d in FAR_FIRST:
        for cc in range(2):
            greet({"z": wrap(z + d, NZ), "c": cc})
    for d in PLANE:
        greet(plane(d)[1])
    greet(partner)

    hot = (lax.broadcasted_iota(jnp.int32, (512, 64), 0) == idv_ref[...]).astype(F32).astype(BF)
    for load in loads[0:2]:
        load.wait()
    dsend[:, 0:H] = dec_ref[...]
    dsend[:, H : H + 64] = dot(tgt_ref[...], hot).astype(BF)
    dsend[:, H + 64 :] = jnp.zeros((8, R - 64), BF)

    with jax.named_scope("barrier"):
        pl.semaphore_wait(barrier, 46)

    mine = pl.ds(pl.multiple_of(m * R, R), R)

    def tan_copy(to):
        return remote(
            tsend, tfull.at[xl, pl.ds(0, R + 16), mine], sent.at[0], came.at[0], to
        )

    def own_copy(d, k):
        return remote(
            dsend, dblk.at[c, z], sent.at[k], came.at[k], {"z": wrap(z + d, NZ)}
        )

    def pass_copy(block, d):
        part = dblk.at[c, wrap(z + block, NZ)]
        return remote(part, part, sent.at[2], came.at[2], {"z": wrap(z + d, NZ)})

    def half_copy(side):
        return remote(dblk.at[side], dblk.at[side], sent.at[3], came.at[3], partner)

    def jac_copy(zz, cc):
        return remote(
            jsend.at[cc * NZ + zz], jbuf.at[b], sent.at[4], came.at[4], {"z": zz, "c": cc}
        )

    def start_jac(ds):
        for d in ds:
            for cc in range(2):
                jac_copy(wrap(z + d, NZ), cc).start()

    def start_z(copy):
        for d in FAR_FIRST:
            copy(wrap(z + d, NZ)).start()

    xside = {"xl": 1 - xl}

    def recv(k, ref):
        with jax.named_scope(f"recv{k}"):
            remote(ref, ref, sent.at[k], came.at[k], partner).wait_recv()

    def left(k, ref):
        remote(ref, ref, sent.at[k], came.at[k], partner).wait_send()

    for d in (5, 11):
        own_copy(d, 1).start()
    for d in (1, 15, 2, 14):
        own_copy(d, 16).start()
    dblk[c, z] = dsend[...]
    loads[2].wait()

    def pick(zz):
        for cc in range(2):
            for i in range(2):
                jsend[cc * NZ + zz, i] = jac_ref[ids_ref[zz * 4 + cc * 2 + i]]

    each(NZ, pick)
    start_jac(FAR_FIRST[0:5])
    jbuf[b] = jsend[b]
    for load in loads[3:]:
        load.wait()

    own = ids_ref[z * 4 + c * 2 + xl]
    x_hot = (lax.broadcasted_iota(jnp.int32, (16, 512), 1) == own).astype(F32).astype(BF)
    x_rows = dot(x_hot, xs_ref[...])
    w1 = w1_ref[...].astype(F32)
    b1 = b1_ref[...].astype(F32)
    b1 = jnp.concatenate([b1[k : k + 1] for k in range(8)], axis=1)
    first_pre = dot(x_rows.astype(BF), w1_ref[...]) + b1
    first_act = jnp.tanh(first_pre)[0:1]
    first_slope = 1.0 - first_act * first_act
    top16 = lax.broadcasted_iota(jnp.int32, (16, H), 0) == 0
    ft[0:R, :] = (first_slope * w1).astype(BF)
    ft[R : R + 16, :] = jnp.where(top16, jnp.broadcast_to(first_act, (16, H)), 0.0).astype(BF)
    lin = dot(ft[...], hw_ref[...])
    hidden_lin = lin[0:R]
    hidden_act = jnp.tanh(lin[R : R + 1] + hb_ref[...].astype(F32))
    hidden_slope = 1.0 - hidden_act * hidden_act
    top = lax.broadcasted_iota(jnp.int32, (16, R), 0) == 0
    tsend[0:R, :] = (hidden_slope * hidden_lin).astype(BF)
    tsend[R : R + 16, :] = jnp.where(top, jnp.broadcast_to(hidden_act, (16, R)), 0.0).astype(BF)
    for d in PLANE:
        tan_copy(plane(d)[1]).start()
    tfull[:, R + 16 :, :] = jnp.zeros((2, 2 * R - R - 16, H), BF)
    tfull[xl, 0 : R + 16, mine] = tsend[...]

    recv(1, dblk.at[0, pl.ds(0, 2)])
    for d in (2, 14, 1, 15):
        for block in (5, 11):
            pass_copy(block, d).start()
    odd = z % 2
    pass_copy(11 - 6 * odd, 3 + 10 * odd).start()
    start_jac(FAR_FIRST[5:])
    jac_copy(z, 1 - c).start()
    recv(16, dblk.at[0, pl.ds(0, 4)])
    recv(2, dblk.at[0, pl.ds(0, 9)])
    half_copy(c).start()

    def unpack(side):
        rows = pl.ds(pl.multiple_of(side * R, R), R)
        dmat[rows, :] = dblk[side].astype(F32).reshape(R, WIDE).astype(BF)

    unpack(c)
    recv(0, tbytes.at[pl.ds(0, 15)])
    recv(3, dblk.at[0])
    unpack(1 - c)

    lane = lax.broadcasted_iota(jnp.int32, (2 * R, R), 1)
    tgt = dmat[:, H:].astype(F32)
    dec = dmat[:, 0:H]
    for i in range(2):
        want = jnp.sum(jnp.where(lane == z * 4 + c * 2 + i, tgt, 0.0), axis=1, keepdims=True)
        want = jnp.where(lane == 0, jnp.broadcast_to(want, (2 * R, R)), 0.0)
        out = dot(dec, tfull[i], NT)
        net[i, :, 0:R] = out[:, 0:R]
        net[i, :, R:] = out[:, R:] - want
    recv(4, jbuf.at[pl.ds(0, 31)])
    miss = []
    for i in range(2):
        stored = jbuf[:, i].astype(F32).reshape(2 * R, R)
        miss_i = jnp.concatenate([net[i, :, 0:R] - stored, net[i, :, R:]], axis=1).astype(BF)
        miss.append(miss_i)
        back_i = dot(miss_i, dec, TN)[0 : R + 8]
        for k in range(8):
            part = back_i[:, R * k : R * k + R]
            pbuf[i, k] = part.reshape(17, 8, R).astype(BF)
        for dy in (2, 1, 3, 0):
            for hh in range(2):
                yy = wrap(y + dy, 4)
                to = {"y": yy, "xh": hh, "xl": i}

                def send():
                    remote(
                        pbuf.at[i, yy * 2 + hh], rbuf.at[q], sent.at[5], came.at[5], to
                    ).start()

                if dy:
                    send()
                else:
                    pl.when((hh != xh) | (xl != i))(send)

    gown[...] = dot(miss[0], tfull[0]) + dot(miss[1], tfull[1])
    theirs = gown[pl.ds(pl.multiple_of((1 - c) * R, R), R), :]
    gsend[...] = theirs.reshape(NZ, 8, H).astype(BF)
    remote(gsend, grecv, sent.at[6], came.at[6], partner).start()
    ours = gown[pl.ds(pl.multiple_of(c * R, R), R), :].reshape(NZ, 8, H)
    recv(6, grecv)
    hsend[...] = (ours + grecv[...].astype(F32)).astype(BF)

    def gz_copy(peer):
        return remote(hsend.at[peer], hrecv.at[z], sent.at[7], came.at[7], {"z": peer})

    start_z(gz_copy)
    hrecv[z] = hsend[z]

    recv(5, rbuf.at[pl.ds(0, 15)])
    rbuf[q] = pbuf[xl, m]
    back = jnp.sum(rbuf[...].astype(F32), axis=0).reshape(R + 8, R)
    tan_back = back[0:R]
    act_back = back[R : R + 1]
    lin_round = (tan_back * hidden_slope).astype(BF)
    pre_back = act_back * hidden_slope - 2.0 * hidden_act * hidden_slope * jnp.sum(
        tan_back * hidden_lin, axis=0, keepdims=True
    )
    pre_round = jnp.where(top, jnp.broadcast_to(pre_back, (16, R)), 0.0).astype(BF)
    both = jnp.concatenate([lin_round, pre_round], axis=0)
    low = dot(both, hw_ref[...], NT)
    tan_lower = low[0:R]
    pre_lower = low[R : R + 1] * first_slope - 2.0 * first_act * first_slope * jnp.sum(
        tan_lower * w1, axis=0, keepdims=True
    )
    x_col = jnp.transpose(jnp.broadcast_to(x_rows[0:1], (R, R)))[:, 0:1]
    fw = x_col * pre_lower + tan_lower * first_slope
    place = lax.broadcasted_iota(jnp.int32, (8, H), 1) // R == m
    line = lax.broadcasted_iota(jnp.int32, (8, H), 0)
    pre_wide = jnp.concatenate([pre_back] * 8, axis=1)
    tail = jnp.where(line == 0, jnp.broadcast_to(pre_lower, (8, H)), 0.0)
    tail = tail + jnp.where((line == 1) & place, jnp.broadcast_to(pre_wide, (8, H)), 0.0)
    for cc in range(2):
        for k in range(16):
            r0 = 64 * cc + 32 * (k % 2)
            l0 = R * (k // 2)
            fsend[cc, k, 0:4] = fw[r0 : r0 + 32, l0 : l0 + R].reshape(4, 8, R).astype(BF)
            fsend[cc, k, 4] = tail[:, l0 : l0 + R].astype(BF)
    remote(fsend.at[1 - c], fpart, sent.at[9], came.at[9], partner).start()
    qsend[...] = dot(ft[...], both, TN).astype(BF).reshape(2, 4 * R, R)
    remote(qsend.at[1 - c], qpart, sent.at[8], came.at[8], partner).start()
    recv(9, fpart)
    fsum[...] = (fsend[c].astype(F32) + fpart[...].astype(F32)).astype(BF)
    for d in PLANE:
        peer, to = plane(d)
        remote(fsum.at[peer], frecv.at[q], sent.at[17], came.at[17], to).start()
    frecv[q] = fsum[q]
    recv(8, qpart)
    halves = qsend[c].astype(F32) + qpart[...].astype(F32)
    qsum[...] = halves.astype(BF).reshape(2, 2 * R, R)
    remote(qsum.at[1 - xl], qrecv, sent.at[18], came.at[18], xside).start()

    recv(17, frecv.at[pl.ds(0, 15)])
    ysend[...] = jnp.sum(frecv[...].astype(F32), axis=0).astype(BF)
    for t in range(5):

        @pl.when(z != t)
        def _():
            remote(ysend.at[t], yrecv.at[z], sent.at[11], came.at[11], {"z": t}).start()

        @pl.when(z == t)
        def _():
            yrecv[z] = ysend[t]

    recv(18, qrecv)
    quarter = qsum[xl].astype(F32) + qrecv[...].astype(F32)
    zsend[...] = quarter.reshape(NZ, 2, 8, R).astype(BF)

    def zr_copy(peer):
        return remote(zsend.at[peer], zrecv.at[z], sent.at[10], came.at[10], {"z": peer})

    start_z(zr_copy)
    zrecv[z] = zsend[z]

    def low_first(copy):
        for zz in LOW_FIRST:
            pl.when(z != zz)(lambda: copy({"z": zz}).start())

    def y_copy(to):
        return remote(yall.at[z], yall.at[z], sent.at[13], came.at[13], to)

    def zg_copy(to):
        return remote(zall.at[z], zall.at[z], sent.at[12], came.at[12], to)

    @pl.when(z < 5)
    def _():
        recv(11, yrecv.at[pl.ds(0, 15)])
        yall[z] = jnp.sum(yrecv[...].astype(F32), axis=0).astype(BF)
        low_first(y_copy)

    recv(10, zrecv.at[pl.ds(0, 15)])
    zall[z] = jnp.sum(zrecv[...].astype(F32), axis=0).astype(BF)
    low_first(zg_copy)

    recv(7, hrecv.at[pl.ds(0, 15)])
    dg_ref[...] = jnp.sum(hrecv[...].astype(F32), axis=0)
    outs = (
        pltpu.make_async_copy(dg_ref, dg_hbm, put.at[0]),
        pltpu.make_async_copy(tile, tile_hbm, put.at[1]),
        pltpu.make_async_copy(hall, hall_hbm, put.at[2]),
        pltpu.make_async_copy(fall, fall_hbm, put.at[3]),
    )
    outs[0].start()

    @pl.when(z < 5)
    def _():
        recv(13, yall.at[pl.ds(0, 4)])

    @pl.when(z >= 5)
    def _():
        recv(13, yall.at[pl.ds(0, 5)])

    for d in PLANE:
        remote(
            yall.at[pl.ds(0, 5)], fall.at[c, q], sent.at[15], came.at[15], plane(d)[1]
        ).start()
    fall[c, q] = yall[0:5]
    tile[...] = yall[4]
    outs[1].start()
    recv(12, zall.at[pl.ds(0, 15)])
    remote(zall, hall.at[c, xl], sent.at[14], came.at[14], xside).start()
    hall[c, xl] = zall[...]
    recv(15, fall.at[0, pl.ds(0, 15)])
    remote(fall.at[c], fall.at[c], sent.at[19], came.at[19], partner).start()
    recv(14, zall)
    remote(hall.at[c], hall.at[c], sent.at[20], came.at[20], partner).start()
    recv(19, fall.at[0])
    outs[3].start()
    recv(20, hall.at[0])
    outs[2].start()

    left(0, tbytes.at[pl.ds(0, 15)])
    left(1, dblk.at[0, pl.ds(0, 2)])
    left(16, dblk.at[0, pl.ds(0, 4)])
    left(2, dblk.at[0, pl.ds(0, 9)])
    left(3, dblk.at[0])
    left(4, jbuf.at[pl.ds(0, 31)])
    left(5, rbuf.at[pl.ds(0, 15)])
    left(6, grecv)
    left(7, hrecv.at[pl.ds(0, 15)])
    left(8, qpart)
    left(9, fpart)
    left(17, frecv.at[pl.ds(0, 15)])
    left(18, qrecv)
    left(10, zrecv.at[pl.ds(0, 15)])

    @pl.when(z < 5)
    def _():
        left(11, yall.at[pl.ds(0, 4)])
        left(13, yrecv.at[pl.ds(0, 15)])

    @pl.when(z >= 5)
    def _():
        left(11, yall.at[pl.ds(0, 5)])

    left(12, zrecv.at[pl.ds(0, 15)])
    left(14, zall)
    left(15, fall.at[0, pl.ds(0, 15)])
    left(19, fall.at[0])
    left(20, hall.at[0])
    for out in outs:
        out.wait()


def unfold(
    hall_hbm,
    fall_hbm,
    tile_hbm,
    dg_hbm,
    fw_hbm,
    fb_hbm,
    hg_hbm,
    hb_hbm,
    dgo_hbm,
    hall,
    fall,
    tile,
    dg,
    fw,
    fb,
    hg,
    hb,
    got,
    put,
):
    ins = (
        pltpu.make_async_copy(hall_hbm, hall, got.at[0]),
        pltpu.make_async_copy(fall_hbm, fall, got.at[1]),
        pltpu.make_async_copy(dg_hbm, dg, got.at[2]),
        pltpu.make_async_copy(tile_hbm, tile, got.at[3]),
    )
    outs = (
        pltpu.make_async_copy(hg, hg_hbm, put.at[0]),
        pltpu.make_async_copy(fw, fw_hbm, put.at[1]),
        pltpu.make_async_copy(dg, dgo_hbm, put.at[2]),
        pltpu.make_async_copy(hb, hb_hbm, put.at[3]),
        pltpu.make_async_copy(fb, fb_hbm, put.at[4]),
    )
    for copy in ins:
        copy.start()
    ins[0].wait()
    hg[...] = hall[...].astype(F32).reshape(H, R)
    outs[0].start()
    ins[1].wait()
    for mm in range(8):
        for ee in range(4):
            piece = fall[ee // 2, 2 * mm + ee % 2].astype(F32)
            fw[32 * ee : 32 * ee + 32, R * mm : R * mm + R] = piece[0:4].reshape(32, R)
            if ee == 0:
                fb[mm : mm + 1, :] = piece[4, 0:1]
    outs[1].start()
    outs[4].start()
    ins[2].wait()
    outs[2].start()
    ins[3].wait()
    hb[...] = tile[...].astype(F32)[1:2]
    outs[3].start()
    for copy in outs:
        copy.wait()


def on_device(
    inputs_store,
    window,
    targets_store,
    jac_store,
    first_weight,
    first_bias,
    hidden_weight,
    hidden_bias,
    decoder_weight,
):
    vmem = pl.BlockSpec(memory_space=pltpu.VMEM)
    smem = pl.BlockSpec(memory_space=pltpu.SMEM)
    hbm = pl.BlockSpec(memory_space=pltpu.HBM)
    dma = pltpu.SemaphoreType.DMA
    hall = jax.ShapeDtypeStruct((2, 2, NZ, 2, 8, R), BF)
    fall = jax.ShapeDtypeStruct((2, 16, 5, 8, R), BF)
    tile = jax.ShapeDtypeStruct((8, R), BF)
    dg = jax.ShapeDtypeStruct((8, H), F32)
    raw = (hall, fall, tile, dg)
    parts = pl.pallas_call(
        kernel,
        out_shape=raw,
        in_specs=[smem, vmem] + [hbm] * 8,
        out_specs=(hbm,) * 4,
        scratch_shapes=[
            pltpu.VMEM((512, R), BF),
            pltpu.VMEM((512, 8, R), BF),
            pltpu.VMEM((8, 512), BF),
            pltpu.VMEM((R, H), BF),
            pltpu.VMEM((8, R), BF),
            pltpu.VMEM((H, R), BF),
            pltpu.VMEM((1, R), BF),
            pltpu.VMEM((8, H), BF),
            pltpu.VMEM((R + 16, H), BF),
            pltpu.VMEM((R + 16, R), BF),
            pltpu.VMEM((2, 2 * R, H), BF),
            pltpu.VMEM((8, WIDE), BF),
            pltpu.VMEM((2, NZ, 8, WIDE), BF),
            pltpu.VMEM((2 * R, WIDE), BF),
            pltpu.VMEM((32, 2, 8, R), BF),
            pltpu.VMEM((32, 2, 8, R), BF),
            pltpu.VMEM((2, 2 * R, 2 * R), F32),
            pltpu.VMEM((16, R + 16, R), BF),
            pltpu.VMEM((2, 8, 17, 8, R), BF),
            pltpu.VMEM((16, 17, 8, R), BF),
            pltpu.VMEM((NZ, 8, H), BF),
            pltpu.VMEM((NZ, 8, H), BF),
            pltpu.VMEM((2 * R, H), F32),
            pltpu.VMEM((NZ, 8, H), BF),
            pltpu.VMEM((NZ, 8, H), BF),
            pltpu.VMEM((2, 4 * R, R), BF),
            pltpu.VMEM((4 * R, R), BF),
            pltpu.VMEM((2, 2 * R, R), BF),
            pltpu.VMEM((2 * R, R), BF),
            pltpu.VMEM((2, 16, 5, 8, R), BF),
            pltpu.VMEM((16, 5, 8, R), BF),
            pltpu.VMEM((16, 5, 8, R), BF),
            pltpu.VMEM((16, 5, 8, R), BF),
            pltpu.VMEM((NZ, 2, 8, R), BF),
            pltpu.VMEM((NZ, 2, 8, R), BF),
            pltpu.VMEM((NZ, 2, 8, R), BF),
            pltpu.VMEM((5, 8, R), BF),
            pltpu.VMEM((NZ, 8, R), BF),
            pltpu.VMEM((NZ, 8, R), BF),
            pltpu.VMEM((2, 2, NZ, 2, 8, R), BF),
            pltpu.VMEM((2, 16, 5, 8, R), BF),
            pltpu.VMEM((8, R), BF),
            pltpu.VMEM((8, H), F32),
            dma((21,)),
            dma((21,)),
            dma((8,)),
            dma((4,)),
        ],
        compiler_params=pltpu.CompilerParams(
            collective_id=0, has_side_effects=True, vmem_limit_bytes=VMEM_MOST
        ),
    )(
        window,
        window.reshape(1, 64),
        inputs_store,
        jac_store,
        targets_store.T,
        first_weight,
        first_bias.reshape(8, R),
        hidden_weight,
        hidden_bias.reshape(1, R),
        decoder_weight,
    )
    final = (
        jax.ShapeDtypeStruct((R, H), F32),
        jax.ShapeDtypeStruct((8, R), F32),
        jax.ShapeDtypeStruct((H, R), F32),
        jax.ShapeDtypeStruct((1, R), F32),
        dg,
    )
    fw, fb, hg, hb, dgo = pl.pallas_call(
        unfold,
        out_shape=final,
        in_specs=[hbm] * 4,
        out_specs=(hbm,) * 5,
        scratch_shapes=[pltpu.VMEM(a.shape, a.dtype) for a in raw + final[0:4]]
        + [dma((4,)), dma((5,))],
        compiler_params=pltpu.CompilerParams(vmem_limit_bytes=VMEM_MOST),
    )(*parts)
    return fw, fb.reshape(H), hg, hb.reshape(R), dgo


def solution(mesh):
    torus = Mesh(mesh.devices.reshape(NZ, 2, 2, 4, 2), ALL)
    return jax.shard_map(
        on_device,
        mesh=torus,
        in_specs=(
            P(),
            P(),
            P(None, ALL),
            P(None, ALL, None),
            P(),
            P(),
            P(None, MP),
            P(MP),
            P(ALL, None),
        ),
        out_specs=(P(), P(), P(None, MP), P(MP), P(ALL, None)),
        check_vma=False,
    )
```

```python
import jax
import jax.numpy as jnp
from jax import lax
from jax.experimental import pallas as pl
from jax.experimental.pallas import tpu as pltpu
from jax.sharding import Mesh
from jax.sharding import PartitionSpec as P

MESH = pl.DeviceIdType.MESH
DP = ("z", "xl", "c")
MP = ("y", "xh")
ALL = DP + MP
BF = jnp.bfloat16
F32 = jnp.float32

R = 128
H = 1024
NZ = 16
WIDE = H + R
VMEM_MOST = 67043328
NT = (((1,), (1,)), ((), ()))
TN = (((0,), (0,)), ((), ()))


def dot(a, b, dims=(((1,), (0,)), ((), ()))):
    return lax.dot_general(a, b, dims, preferred_element_type=F32)


def remote(src, dst, send, recv, to):
    return pltpu.make_async_remote_copy(
        src_ref=src, dst_ref=dst, send_sem=send, recv_sem=recv, device_id=to, device_id_type=MESH
    )


def each(n, body):
    def step(t, carry):
        body(t)
        return carry

    lax.fori_loop(0, n, step, 0)


def wrap(v, n):
    return jnp.where(v >= n, v - n, v)


FAR_FIRST = (8, 7, 9, 6, 10, 5, 11, 4, 12, 3, 13, 2, 14, 1, 15)
LOW_FIRST = (0, 1, 2, 3, 4, 5, 6, 7, 15, 14, 13, 12, 8, 11, 9, 10)
PLANE = sorted(
    (
        (dy, dh, dl)
        for dy in range(4)
        for dh in range(2)
        for dl in range(2)
        if dy + dh + dl > 0
    ),
    key=lambda d: -(min(d[0], 4 - d[0]) + (2 if d[1:] == (1, 0) else max(d[1:]))),
)


def kernel(
    ids_ref,
    idv_ref,
    xs_hbm,
    jac_hbm,
    tgt_hbm,
    w1_hbm,
    b1_hbm,
    hw_hbm,
    hb_hbm,
    dec_hbm,
    hall_hbm,
    fall_hbm,
    tile_hbm,
    dg_hbm,
    xs_ref,
    jac_ref,
    tgt_ref,
    w1_ref,
    b1_ref,
    hw_ref,
    hb_ref,
    dec_ref,
    ft,
    tsend,
    tfull,
    dsend,
    dblk,
    dmat,
    jsend,
    jbuf,
    net,
    tbytes,
    pbuf,
    rbuf,
    gsend,
    grecv,
    gown,
    hsend,
    hrecv,
    qsend,
    qpart,
    qsum,
    qrecv,
    fsend,
    fpart,
    fsum,
    frecv,
    zsend,
    zrecv,
    zall,
    ysend,
    yrecv,
    yall,
    hall,
    fall,
    tile,
    dg_ref,
    sent,
    came,
    taken,
    put,
):
    z, xl, c = lax.axis_index("z"), lax.axis_index("xl"), lax.axis_index("c")
    y, xh = lax.axis_index("y"), lax.axis_index("xh")
    m = y * 2 + xh
    q = m * 2 + xl
    b = c * NZ + z

    def plane(d):
        dy, dh, dl = d
        yy = wrap(y + dy, 4)
        hh = 1 - xh if dh else xh
        ll = 1 - xl if dl else xl
        return (yy * 2 + hh) * 2 + ll, {"y": yy, "xh": hh, "xl": ll}

    partner = {"c": 1 - c}
    barrier = pltpu.get_barrier_semaphore()

    homes = (
        (tgt_hbm, tgt_ref),
        (dec_hbm, dec_ref),
        (jac_hbm, jac_ref),
        (xs_hbm, xs_ref),
        (w1_hbm, w1_ref),
        (hw_hbm, hw_ref),
        (b1_hbm, b1_ref),
        (hb_hbm, hb_ref),
    )
    loads = [pltpu.make_async_copy(a, v, taken.at[k]) for k, (a, v) in enumerate(homes)]
    for load in loads:
        load.start()

    def greet(to):
        pl.semaphore_signal(barrier, inc=1, device_id=to, device_id_type=MESH)

    for d in FAR_FIRST:
        for cc in range(2):
            greet({"z": wrap(z + d, NZ), "c": cc})
    for d in PLANE:
        greet(plane(d)[1])
    greet(partner)

    hot = (lax.broadcasted_iota(jnp.int32, (512, 64), 0) == idv_ref[...]).astype(F32).astype(BF)
    for load in loads[0:2]:
        load.wait()
    dsend[:, 0:H] = dec_ref[...]
    dsend[:, H : H + 64] = dot(tgt_ref[...], hot).astype(BF)
    dsend[:, H + 64 :] = jnp.zeros((8, R - 64), BF)

    with jax.named_scope("barrier"):
        pl.semaphore_wait(barrier, 46)

    mine = pl.ds(pl.multiple_of(m * R, R), R)

    def tan_copy(to):
        return remote(
            tsend, tfull.at[xl, pl.ds(0, R + 16), mine], sent.at[0], came.at[0], to
        )

    def own_copy(d, k):
        return remote(
            dsend, dblk.at[c, z], sent.at[k], came.at[k], {"z": wrap(z + d, NZ)}
        )

    def pass_copy(block, d):
        part = dblk.at[c, wrap(z + block, NZ)]
        return remote(part, part, sent.at[2], came.at[2], {"z": wrap(z + d, NZ)})

    def half_copy(side):
        return remote(dblk.at[side], dblk.at[side], sent.at[3], came.at[3], partner)

    def jac_copy(zz, cc):
        return remote(
            jsend.at[cc * NZ + zz], jbuf.at[b], sent.at[4], came.at[4], {"z": zz, "c": cc}
        )

    def start_jac(ds):
        for d in ds:
            for cc in range(2):
                jac_copy(wrap(z + d, NZ), cc).start()

    def start_z(copy):
        for d in FAR_FIRST:
            copy(wrap(z + d, NZ)).start()

    xside = {"xl": 1 - xl}

    def recv(k, ref):
        with jax.named_scope(f"recv{k}"):
            remote(ref, ref, sent.at[k], came.at[k], partner).wait_recv()

    def left(k, ref):
        remote(ref, ref, sent.at[k], came.at[k], partner).wait_send()

    for d in (5, 11):
        own_copy(d, 1).start()
    for d in (1, 15, 2, 14):
        own_copy(d, 16).start()
    dblk[c, z] = dsend[...]
    loads[2].wait()

    def pick(zz):
        for cc in range(2):
            for i in range(2):
                jsend[cc * NZ + zz, i] = jac_ref[ids_ref[zz * 4 + cc * 2 + i]]

    each(NZ, pick)
    start_jac(FAR_FIRST[0:5])
    jbuf[b] = jsend[b]
    for load in loads[3:]:
        load.wait()

    own = ids_ref[z * 4 + c * 2 + xl]
    x_hot = (lax.broadcasted_iota(jnp.int32, (16, 512), 1) == own).astype(F32).astype(BF)
    x_rows = dot(x_hot, xs_ref[...])
    w1 = w1_ref[...].astype(F32)
    b1 = b1_ref[...].astype(F32)
    b1 = jnp.concatenate([b1[k : k + 1] for k in range(8)], axis=1)
    first_pre = dot(x_rows.astype(BF), w1_ref[...]) + b1
    first_act = jnp.tanh(first_pre)[0:1]
    first_slope = 1.0 - first_act * first_act
    top16 = lax.broadcasted_iota(jnp.int32, (16, H), 0) == 0
    ft[0:R, :] = (first_slope * w1).astype(BF)
    ft[R : R + 16, :] = jnp.where(top16, jnp.broadcast_to(first_act, (16, H)), 0.0).astype(BF)
    lin = dot(ft[...], hw_ref[...])
    hidden_lin = lin[0:R]
    hidden_act = jnp.tanh(lin[R : R + 1] + hb_ref[...].astype(F32))
    hidden_slope = 1.0 - hidden_act * hidden_act
    top = lax.broadcasted_iota(jnp.int32, (16, R), 0) == 0
    tsend[0:R, :] = (hidden_slope * hidden_lin).astype(BF)
    tsend[R : R + 16, :] = jnp.where(top, jnp.broadcast_to(hidden_act, (16, R)), 0.0).astype(BF)
    for d in PLANE:
        tan_copy(plane(d)[1]).start()
    tfull[:, R + 16 :, :] = jnp.zeros((2, 2 * R - R - 16, H), BF)
    tfull[xl, 0 : R + 16, mine] = tsend[...]

    recv(1, dblk.at[0, pl.ds(0, 2)])
    for d in (2, 14, 1, 15):
        for block in (5, 11):
            pass_copy(block, d).start()
    odd = z % 2
    pass_copy(11 - 6 * odd, 3 + 10 * odd).start()
    start_jac(FAR_FIRST[5:])
    jac_copy(z, 1 - c).start()
    recv(16, dblk.at[0, pl.ds(0, 4)])
    recv(2, dblk.at[0, pl.ds(0, 9)])
    half_copy(c).start()

    def unpack(side):
        rows = pl.ds(pl.multiple_of(side * R, R), R)
        dmat[rows, :] = dblk[side].astype(F32).reshape(R, WIDE).astype(BF)

    unpack(c)
    recv(0, tbytes.at[pl.ds(0, 15)])
    recv(3, dblk.at[0])
    unpack(1 - c)

    lane = lax.broadcasted_iota(jnp.int32, (2 * R, R), 1)
    tgt = dmat[:, H:].astype(F32)
    dec = dmat[:, 0:H]
    for i in range(2):
        want = jnp.sum(jnp.where(lane == z * 4 + c * 2 + i, tgt, 0.0), axis=1, keepdims=True)
        want = jnp.where(lane == 0, jnp.broadcast_to(want, (2 * R, R)), 0.0)
        out = dot(dec, tfull[i], NT)
        net[i, :, 0:R] = out[:, 0:R]
        net[i, :, R:] = out[:, R:] - want
    recv(4, jbuf.at[pl.ds(0, 31)])
    miss = []
    for i in range(2):
        stored = jbuf[:, i].astype(F32).reshape(2 * R, R)
        miss_i = jnp.concatenate([net[i, :, 0:R] - stored, net[i, :, R:]], axis=1).astype(BF)
        miss.append(miss_i)
        back_i = dot(miss_i, dec, TN)[0 : R + 8]
        for k in range(8):
            part = back_i[:, R * k : R * k + R]
            pbuf[i, k] = part.reshape(17, 8, R).astype(BF)
        for dy in (2, 1, 3, 0):
            for hh in range(2):
                yy = wrap(y + dy, 4)
                to = {"y": yy, "xh": hh, "xl": i}

                def send():
                    remote(
                        pbuf.at[i, yy * 2 + hh], rbuf.at[q], sent.at[5], came.at[5], to
                    ).start()

                if dy:
                    send()
                else:
                    pl.when((hh != xh) | (xl != i))(send)

    gown[...] = dot(miss[0], tfull[0]) + dot(miss[1], tfull[1])
    theirs = gown[pl.ds(pl.multiple_of((1 - c) * R, R), R), :]
    gsend[...] = theirs.reshape(NZ, 8, H).astype(BF)
    remote(gsend, grecv, sent.at[6], came.at[6], partner).start()
    ours = gown[pl.ds(pl.multiple_of(c * R, R), R), :].reshape(NZ, 8, H)
    recv(6, grecv)
    hsend[...] = (ours + grecv[...].astype(F32)).astype(BF)

    def gz_copy(peer):
        return remote(hsend.at[peer], hrecv.at[z], sent.at[7], came.at[7], {"z": peer})

    start_z(gz_copy)
    hrecv[z] = hsend[z]

    recv(5, rbuf.at[pl.ds(0, 15)])
    rbuf[q] = pbuf[xl, m]
    back = jnp.sum(rbuf[...].astype(F32), axis=0).reshape(R + 8, R)
    tan_back = back[0:R]
    act_back = back[R : R + 1]
    lin_round = (tan_back * hidden_slope).astype(BF)
    pre_back = act_back * hidden_slope - 2.0 * hidden_act * hidden_slope * jnp.sum(
        tan_back * hidden_lin, axis=0, keepdims=True
    )
    pre_round = jnp.where(top, jnp.broadcast_to(pre_back, (16, R)), 0.0).astype(BF)
    both = jnp.concatenate([lin_round, pre_round], axis=0)
    low = dot(both, hw_ref[...], NT)
    tan_lower = low[0:R]
    pre_lower = low[R : R + 1] * first_slope - 2.0 * first_act * first_slope * jnp.sum(
        tan_lower * w1, axis=0, keepdims=True
    )
    x_col = jnp.transpose(jnp.broadcast_to(x_rows[0:1], (R, R)))[:, 0:1]
    fw = x_col * pre_lower + tan_lower * first_slope
    place = lax.broadcasted_iota(jnp.int32, (8, H), 1) // R == m
    line = lax.broadcasted_iota(jnp.int32, (8, H), 0)
    pre_wide = jnp.concatenate([pre_back] * 8, axis=1)
    tail = jnp.where(line == 0, jnp.broadcast_to(pre_lower, (8, H)), 0.0)
    tail = tail + jnp.where((line == 1) & place, jnp.broadcast_to(pre_wide, (8, H)), 0.0)
    for cc in range(2):
        for k in range(16):
            r0 = 64 * cc + 32 * (k % 2)
            l0 = R * (k // 2)
            fsend[cc, k, 0:4] = fw[r0 : r0 + 32, l0 : l0 + R].reshape(4, 8, R).astype(BF)
            fsend[cc, k, 4] = tail[:, l0 : l0 + R].astype(BF)
    remote(fsend.at[1 - c], fpart, sent.at[9], came.at[9], partner).start()
    qsend[...] = dot(ft[...], both, TN).astype(BF).reshape(2, 4 * R, R)
    remote(qsend.at[1 - c], qpart, sent.at[8], came.at[8], partner).start()
    recv(9, fpart)
    fsum[...] = (fsend[c].astype(F32) + fpart[...].astype(F32)).astype(BF)
    for d in PLANE:
        peer, to = plane(d)
        remote(fsum.at[peer], frecv.at[q], sent.at[17], came.at[17], to).start()
    frecv[q] = fsum[q]
    recv(8, qpart)
    halves = qsend[c].astype(F32) + qpart[...].astype(F32)
    qsum[...] = halves.astype(BF).reshape(2, 2 * R, R)
    remote(qsum.at[1 - xl], qrecv, sent.at[18], came.at[18], xside).start()

    recv(17, frecv.at[pl.ds(0, 15)])
    ysend[...] = jnp.sum(frecv[...].astype(F32), axis=0).astype(BF)
    for t in range(5):

        @pl.when(z != t)
        def _():
            remote(ysend.at[t], yrecv.at[z], sent.at[11], came.at[11], {"z": t}).start()

        @pl.when(z == t)
        def _():
            yrecv[z] = ysend[t]

    recv(18, qrecv)
    quarter = qsum[xl].astype(F32) + qrecv[...].astype(F32)
    zsend[...] = quarter.reshape(NZ, 2, 8, R).astype(BF)

    def zr_copy(peer):
        return remote(zsend.at[peer], zrecv.at[z], sent.at[10], came.at[10], {"z": peer})

    start_z(zr_copy)
    zrecv[z] = zsend[z]

    def low_first(copy):
        for zz in LOW_FIRST:
            pl.when(z != zz)(lambda: copy({"z": zz}).start())

    def y_copy(to):
        return remote(yall.at[z], yall.at[z], sent.at[13], came.at[13], to)

    def zg_copy(to):
        return remote(zall.at[z], zall.at[z], sent.at[12], came.at[12], to)

    @pl.when(z < 5)
    def _():
        recv(11, yrecv.at[pl.ds(0, 15)])
        yall[z] = jnp.sum(yrecv[...].astype(F32), axis=0).astype(BF)
        low_first(y_copy)

    recv(10, zrecv.at[pl.ds(0, 15)])
    zall[z] = jnp.sum(zrecv[...].astype(F32), axis=0).astype(BF)
    low_first(zg_copy)

    recv(7, hrecv.at[pl.ds(0, 15)])
    dg_ref[...] = jnp.sum(hrecv[...].astype(F32), axis=0)
    outs = (
        pltpu.make_async_copy(dg_ref, dg_hbm, put.at[0]),
        pltpu.make_async_copy(tile, tile_hbm, put.at[1]),
        pltpu.make_async_copy(hall, hall_hbm.at[c], put.at[2]),
        pltpu.make_async_copy(fall, fall_hbm.at[c], put.at[3]),
    )
    outs[0].start()
    left(0, tbytes.at[pl.ds(0, 15)])
    left(1, dblk.at[0, pl.ds(0, 2)])
    left(16, dblk.at[0, pl.ds(0, 4)])
    left(2, dblk.at[0, pl.ds(0, 9)])
    left(3, dblk.at[0])
    left(4, jbuf.at[pl.ds(0, 31)])
    left(5, rbuf.at[pl.ds(0, 15)])
    left(6, grecv)
    left(7, hrecv.at[pl.ds(0, 15)])
    left(8, qpart)
    left(9, fpart)
    left(17, frecv.at[pl.ds(0, 15)])
    left(18, qrecv)
    left(10, zrecv.at[pl.ds(0, 15)])

    @pl.when(z < 5)
    def _():
        recv(13, yall.at[pl.ds(0, 4)])

    @pl.when(z >= 5)
    def _():
        recv(13, yall.at[pl.ds(0, 5)])

    for d in PLANE:
        remote(
            yall.at[pl.ds(0, 5)], fall.at[q], sent.at[15], came.at[15], plane(d)[1]
        ).start()
    fall[q] = yall[0:5]
    tile[...] = yall[4]
    outs[1].start()
    recv(12, zall.at[pl.ds(0, 15)])
    remote(zall, hall.at[xl], sent.at[14], came.at[14], xside).start()
    hall[xl] = zall[...]
    recv(15, fall.at[pl.ds(0, 15)])
    remote(fall, fall_hbm.at[c], sent.at[19], came.at[19], partner).start()
    outs[3].start()
    recv(14, zall)
    remote(hall, hall_hbm.at[c], sent.at[20], came.at[20], partner).start()
    outs[2].start()
    recv(19, fall)
    recv(20, hall)

    @pl.when(z < 5)
    def _():
        left(11, yall.at[pl.ds(0, 4)])
        left(13, yrecv.at[pl.ds(0, 15)])

    @pl.when(z >= 5)
    def _():
        left(11, yall.at[pl.ds(0, 5)])

    left(12, zrecv.at[pl.ds(0, 15)])
    left(14, zall)
    left(15, fall.at[pl.ds(0, 15)])
    left(19, fall)
    left(20, hall)
    for out in outs:
        out.wait()


def unfold(
    hall_hbm,
    fall_hbm,
    tile_hbm,
    dg_hbm,
    fw_hbm,
    fb_hbm,
    hg_hbm,
    hb_hbm,
    dgo_hbm,
    hall,
    fall,
    tile,
    dg,
    fw,
    fb,
    hg,
    hb,
    got,
    put,
):
    ins = (
        pltpu.make_async_copy(hall_hbm, hall, got.at[0]),
        pltpu.make_async_copy(fall_hbm, fall, got.at[1]),
        pltpu.make_async_copy(dg_hbm, dg, got.at[2]),
        pltpu.make_async_copy(tile_hbm, tile, got.at[3]),
    )
    outs = (
        pltpu.make_async_copy(hg, hg_hbm, put.at[0]),
        pltpu.make_async_copy(fw, fw_hbm, put.at[1]),
        pltpu.make_async_copy(dg, dgo_hbm, put.at[2]),
        pltpu.make_async_copy(hb, hb_hbm, put.at[3]),
        pltpu.make_async_copy(fb, fb_hbm, put.at[4]),
    )
    for copy in ins:
        copy.start()
    ins[0].wait()
    hg[...] = hall[...].astype(F32).reshape(H, R)
    outs[0].start()
    ins[1].wait()
    for mm in range(8):
        for ee in range(4):
            piece = fall[ee // 2, 2 * mm + ee % 2].astype(F32)
            fw[32 * ee : 32 * ee + 32, R * mm : R * mm + R] = piece[0:4].reshape(32, R)
            if ee == 0:
                fb[mm : mm + 1, :] = piece[4, 0:1]
    outs[1].start()
    outs[4].start()
    ins[2].wait()
    outs[2].start()
    ins[3].wait()
    hb[...] = tile[...].astype(F32)[1:2]
    outs[3].start()
    for copy in outs:
        copy.wait()


def on_device(
    inputs_store,
    window,
    targets_store,
    jac_store,
    first_weight,
    first_bias,
    hidden_weight,
    hidden_bias,
    decoder_weight,
):
    vmem = pl.BlockSpec(memory_space=pltpu.VMEM)
    smem = pl.BlockSpec(memory_space=pltpu.SMEM)
    hbm = pl.BlockSpec(memory_space=pltpu.HBM)
    dma = pltpu.SemaphoreType.DMA
    hall = jax.ShapeDtypeStruct((2, 2, NZ, 2, 8, R), BF)
    fall = jax.ShapeDtypeStruct((2, 16, 5, 8, R), BF)
    tile = jax.ShapeDtypeStruct((8, R), BF)
    dg = jax.ShapeDtypeStruct((8, H), F32)
    raw = (hall, fall, tile, dg)
    parts = pl.pallas_call(
        kernel,
        out_shape=raw,
        in_specs=[smem, vmem] + [hbm] * 8,
        out_specs=(hbm,) * 4,
        scratch_shapes=[
            pltpu.VMEM((512, R), BF),
            pltpu.VMEM((512, 8, R), BF),
            pltpu.VMEM((8, 512), BF),
            pltpu.VMEM((R, H), BF),
            pltpu.VMEM((8, R), BF),
            pltpu.VMEM((H, R), BF),
            pltpu.VMEM((1, R), BF),
            pltpu.VMEM((8, H), BF),
            pltpu.VMEM((R + 16, H), BF),
            pltpu.VMEM((R + 16, R), BF),
            pltpu.VMEM((2, 2 * R, H), BF),
            pltpu.VMEM((8, WIDE), BF),
            pltpu.VMEM((2, NZ, 8, WIDE), BF),
            pltpu.VMEM((2 * R, WIDE), BF),
            pltpu.VMEM((32, 2, 8, R), BF),
            pltpu.VMEM((32, 2, 8, R), BF),
            pltpu.VMEM((2, 2 * R, 2 * R), F32),
            pltpu.VMEM((16, R + 16, R), BF),
            pltpu.VMEM((2, 8, 17, 8, R), BF),
            pltpu.VMEM((16, 17, 8, R), BF),
            pltpu.VMEM((NZ, 8, H), BF),
            pltpu.VMEM((NZ, 8, H), BF),
            pltpu.VMEM((2 * R, H), F32),
            pltpu.VMEM((NZ, 8, H), BF),
            pltpu.VMEM((NZ, 8, H), BF),
            pltpu.VMEM((2, 4 * R, R), BF),
            pltpu.VMEM((4 * R, R), BF),
            pltpu.VMEM((2, 2 * R, R), BF),
            pltpu.VMEM((2 * R, R), BF),
            pltpu.VMEM((2, 16, 5, 8, R), BF),
            pltpu.VMEM((16, 5, 8, R), BF),
            pltpu.VMEM((16, 5, 8, R), BF),
            pltpu.VMEM((16, 5, 8, R), BF),
            pltpu.VMEM((NZ, 2, 8, R), BF),
            pltpu.VMEM((NZ, 2, 8, R), BF),
            pltpu.VMEM((NZ, 2, 8, R), BF),
            pltpu.VMEM((5, 8, R), BF),
            pltpu.VMEM((NZ, 8, R), BF),
            pltpu.VMEM((NZ, 8, R), BF),
            pltpu.VMEM((2, NZ, 2, 8, R), BF),
            pltpu.VMEM((16, 5, 8, R), BF),
            pltpu.VMEM((8, R), BF),
            pltpu.VMEM((8, H), F32),
            dma((21,)),
            dma((21,)),
            dma((8,)),
            dma((4,)),
        ],
        compiler_params=pltpu.CompilerParams(
            collective_id=0, has_side_effects=True, vmem_limit_bytes=VMEM_MOST
        ),
    )(
        window,
        window.reshape(1, 64),
        inputs_store,
        jac_store,
        targets_store.T,
        first_weight,
        first_bias.reshape(8, R),
        hidden_weight,
        hidden_bias.reshape(1, R),
        decoder_weight,
    )
    final = (
        jax.ShapeDtypeStruct((R, H), F32),
        jax.ShapeDtypeStruct((8, R), F32),
        jax.ShapeDtypeStruct((H, R), F32),
        jax.ShapeDtypeStruct((1, R), F32),
        dg,
    )
    fw, fb, hg, hb, dgo = pl.pallas_call(
        unfold,
        out_shape=final,
        in_specs=[hbm] * 4,
        out_specs=(hbm,) * 5,
        scratch_shapes=[pltpu.VMEM(a.shape, a.dtype) for a in raw + final[0:4]]
        + [dma((4,)), dma((5,))],
        compiler_params=pltpu.CompilerParams(vmem_limit_bytes=VMEM_MOST),
    )(*parts)
    return fw, fb.reshape(H), hg, hb.reshape(R), dgo


def solution(mesh):
    torus = Mesh(mesh.devices.reshape(NZ, 2, 2, 4, 2), ALL)
    return jax.shard_map(
        on_device,
        mesh=torus,
        in_specs=(
            P(),
            P(),
            P(None, ALL),
            P(None, ALL, None),
            P(),
            P(),
            P(None, MP),
            P(MP),
            P(ALL, None),
        ),
        out_specs=(P(), P(), P(None, MP), P(MP), P(ALL, None)),
        check_vma=False,
    )
```

```python
import jax
import jax.numpy as jnp
from jax import lax
from jax.experimental import pallas as pl
from jax.experimental.pallas import tpu as pltpu
from jax.sharding import Mesh
from jax.sharding import PartitionSpec as P

MESH = pl.DeviceIdType.MESH
DP = ("z", "xl", "c")
MP = ("y", "xh")
ALL = DP + MP
BF = jnp.bfloat16
F32 = jnp.float32

R = 128
H = 1024
NZ = 16
WIDE = H + R
VMEM_MOST = 67043328
NT = (((1,), (1,)), ((), ()))
TN = (((0,), (0,)), ((), ()))


def dot(a, b, dims=(((1,), (0,)), ((), ()))):
    return lax.dot_general(a, b, dims, preferred_element_type=F32)


def remote(src, dst, send, recv, to):
    return pltpu.make_async_remote_copy(
        src_ref=src, dst_ref=dst, send_sem=send, recv_sem=recv, device_id=to, device_id_type=MESH
    )


def each(n, body):
    def step(t, carry):
        body(t)
        return carry

    lax.fori_loop(0, n, step, 0)


def wrap(v, n):
    return jnp.where(v >= n, v - n, v)


FAR_FIRST = (8, 7, 9, 6, 10, 5, 11, 4, 12, 3, 13, 2, 14, 1, 15)
LOW_FIRST = (0, 1, 2, 3, 4, 5, 6, 7, 15, 14, 13, 12, 8, 11, 9, 10)
PLANE = sorted(
    (
        (dy, dh, dl)
        for dy in range(4)
        for dh in range(2)
        for dl in range(2)
        if dy + dh + dl > 0
    ),
    key=lambda d: -(min(d[0], 4 - d[0]) + (2 if d[1:] == (1, 0) else max(d[1:]))),
)


def kernel(
    ids_ref,
    idv_ref,
    xs_hbm,
    jac_hbm,
    tgt_hbm,
    w1_hbm,
    b1_hbm,
    hw_hbm,
    hb_hbm,
    dec_hbm,
    hall_hbm,
    fall_hbm,
    tile_hbm,
    dg_hbm,
    xs_ref,
    jac_ref,
    tgt_ref,
    w1_ref,
    b1_ref,
    hw_ref,
    hb_ref,
    dec_ref,
    ft,
    tsend,
    tfull,
    dsend,
    dblk,
    dmat,
    jsend,
    jbuf,
    net,
    tbytes,
    pbuf,
    rbuf,
    gsend,
    grecv,
    gown,
    hsend,
    hrecv,
    qsend,
    qpart,
    qsum,
    qrecv,
    fsend,
    fpart,
    fsum,
    frecv,
    zsend,
    zrecv,
    zall,
    ysend,
    yrecv,
    yall,
    hall,
    fall,
    tile,
    dg_ref,
    sent,
    came,
    taken,
    put,
):
    z, xl, c = lax.axis_index("z"), lax.axis_index("xl"), lax.axis_index("c")
    y, xh = lax.axis_index("y"), lax.axis_index("xh")
    m = y * 2 + xh
    q = m * 2 + xl
    b = c * NZ + z

    def plane(d):
        dy, dh, dl = d
        yy = wrap(y + dy, 4)
        hh = 1 - xh if dh else xh
        ll = 1 - xl if dl else xl
        return (yy * 2 + hh) * 2 + ll, {"y": yy, "xh": hh, "xl": ll}

    partner = {"c": 1 - c}
    barrier = pltpu.get_barrier_semaphore()

    homes = (
        (tgt_hbm, tgt_ref),
        (dec_hbm, dec_ref),
        (jac_hbm, jac_ref),
        (xs_hbm, xs_ref),
        (w1_hbm, w1_ref),
        (hw_hbm, hw_ref),
        (b1_hbm, b1_ref),
        (hb_hbm, hb_ref),
    )
    loads = [pltpu.make_async_copy(a, v, taken.at[k]) for k, (a, v) in enumerate(homes)]
    for load in loads:
        load.start()

    def greet(to):
        pl.semaphore_signal(barrier, inc=1, device_id=to, device_id_type=MESH)

    for d in FAR_FIRST:
        for cc in range(2):
            greet({"z": wrap(z + d, NZ), "c": cc})
    for d in PLANE:
        greet(plane(d)[1])
    greet(partner)

    hot = (lax.broadcasted_iota(jnp.int32, (512, 64), 0) == idv_ref[...]).astype(F32).astype(BF)
    for load in loads[0:2]:
        load.wait()
    dsend[:, 0:H] = dec_ref[...]
    dsend[:, H : H + 64] = dot(tgt_ref[...], hot).astype(BF)
    dsend[:, H + 64 :] = jnp.zeros((8, R - 64), BF)

    with jax.named_scope("barrier"):
        pl.semaphore_wait(barrier, 46)

    mine = pl.ds(pl.multiple_of(m * R, R), R)

    def tan_copy(to):
        return remote(
            tsend, tfull.at[xl, pl.ds(0, R + 16), mine], sent.at[0], came.at[0], to
        )

    def own_copy(d, k):
        return remote(
            dsend, dblk.at[c, z], sent.at[k], came.at[k], {"z": wrap(z + d, NZ)}
        )

    def pass_copy(block, d):
        part = dblk.at[c, wrap(z + block, NZ)]
        return remote(part, part, sent.at[2], came.at[2], {"z": wrap(z + d, NZ)})

    def half_copy(side):
        return remote(dblk.at[side], dblk.at[side], sent.at[3], came.at[3], partner)

    def jac_copy(zz, cc):
        return remote(
            jsend.at[cc * NZ + zz], jbuf.at[b], sent.at[4], came.at[4], {"z": zz, "c": cc}
        )

    def start_jac(ds):
        for d in ds:
            for cc in range(2):
                jac_copy(wrap(z + d, NZ), cc).start()

    def start_z(copy):
        for d in FAR_FIRST:
            copy(wrap(z + d, NZ)).start()

    xside = {"xl": 1 - xl}

    def recv(k, ref):
        with jax.named_scope(f"recv{k}"):
            remote(ref, ref, sent.at[k], came.at[k], partner).wait_recv()

    def left(k, ref):
        remote(ref, ref, sent.at[k], came.at[k], partner).wait_send()

    for d in (5, 11):
        own_copy(d, 1).start()
    for d in (1, 15, 2, 14):
        own_copy(d, 16).start()
    dblk[c, z] = dsend[...]
    loads[2].wait()

    def pick(zz):
        for cc in range(2):
            for i in range(2):
                jsend[cc * NZ + zz, i] = jac_ref[ids_ref[zz * 4 + cc * 2 + i]]

    each(NZ, pick)
    start_jac(FAR_FIRST[0:5])
    jbuf[b] = jsend[b]
    for load in loads[3:]:
        load.wait()

    own = ids_ref[z * 4 + c * 2 + xl]
    x_hot = (lax.broadcasted_iota(jnp.int32, (16, 512), 1) == own).astype(F32).astype(BF)
    x_rows = dot(x_hot, xs_ref[...])
    w1 = w1_ref[...].astype(F32)
    b1 = b1_ref[...].astype(F32)
    b1 = jnp.concatenate([b1[k : k + 1] for k in range(8)], axis=1)
    first_pre = dot(x_rows.astype(BF), w1_ref[...]) + b1
    first_act = jnp.tanh(first_pre)[0:1]
    first_slope = 1.0 - first_act * first_act
    top16 = lax.broadcasted_iota(jnp.int32, (16, H), 0) == 0
    ft[0:R, :] = (first_slope * w1).astype(BF)
    ft[R : R + 16, :] = jnp.where(top16, jnp.broadcast_to(first_act, (16, H)), 0.0).astype(BF)
    lin = dot(ft[...], hw_ref[...])
    hidden_lin = lin[0:R]
    hidden_act = jnp.tanh(lin[R : R + 1] + hb_ref[...].astype(F32))
    hidden_slope = 1.0 - hidden_act * hidden_act
    top = lax.broadcasted_iota(jnp.int32, (16, R), 0) == 0
    tsend[0:R, :] = (hidden_slope * hidden_lin).astype(BF)
    tsend[R : R + 16, :] = jnp.where(top, jnp.broadcast_to(hidden_act, (16, R)), 0.0).astype(BF)
    for d in PLANE:
        tan_copy(plane(d)[1]).start()
    tfull[:, R + 16 :, :] = jnp.zeros((2, 2 * R - R - 16, H), BF)
    tfull[xl, 0 : R + 16, mine] = tsend[...]

    recv(1, dblk.at[0, pl.ds(0, 2)])
    for d in (2, 14, 1, 15):
        for block in (5, 11):
            pass_copy(block, d).start()
    odd = z % 2
    pass_copy(11 - 6 * odd, 3 + 10 * odd).start()
    start_jac(FAR_FIRST[5:])
    jac_copy(z, 1 - c).start()
    recv(16, dblk.at[0, pl.ds(0, 4)])
    recv(2, dblk.at[0, pl.ds(0, 9)])
    half_copy(c).start()

    def unpack(side):
        rows = pl.ds(pl.multiple_of(side * R, R), R)
        dmat[rows, :] = dblk[side].astype(F32).reshape(R, WIDE).astype(BF)

    unpack(c)
    recv(0, tbytes.at[pl.ds(0, 15)])
    recv(3, dblk.at[0])
    unpack(1 - c)

    lane = lax.broadcasted_iota(jnp.int32, (2 * R, R), 1)
    tgt = dmat[:, H:].astype(F32)
    dec = dmat[:, 0:H]
    for i in range(2):
        want = jnp.sum(jnp.where(lane == z * 4 + c * 2 + i, tgt, 0.0), axis=1, keepdims=True)
        want = jnp.where(lane == 0, jnp.broadcast_to(want, (2 * R, R)), 0.0)
        out = dot(dec, tfull[i], NT)
        net[i, :, 0:R] = out[:, 0:R]
        net[i, :, R:] = out[:, R:] - want
    recv(4, jbuf.at[pl.ds(0, 31)])
    miss = []
    for i in range(2):
        stored = jbuf[:, i].astype(F32).reshape(2 * R, R)
        miss_i = jnp.concatenate([net[i, :, 0:R] - stored, net[i, :, R:]], axis=1).astype(BF)
        miss.append(miss_i)
        back_i = dot(miss_i, dec, TN)[0 : R + 8]
        for k in range(8):
            part = back_i[:, R * k : R * k + R]
            pbuf[i, k] = part.reshape(17, 8, R).astype(BF)
        for dy in (2, 1, 3, 0):
            for hh in range(2):
                yy = wrap(y + dy, 4)
                to = {"y": yy, "xh": hh, "xl": i}

                def send():
                    remote(
                        pbuf.at[i, yy * 2 + hh], rbuf.at[q], sent.at[5], came.at[5], to
                    ).start()

                if dy:
                    send()
                else:
                    pl.when((hh != xh) | (xl != i))(send)

    gown[...] = dot(miss[0], tfull[0]) + dot(miss[1], tfull[1])
    theirs = gown[pl.ds(pl.multiple_of((1 - c) * R, R), R), :]
    gsend[...] = theirs.reshape(NZ, 8, H).astype(BF)
    remote(gsend, grecv, sent.at[6], came.at[6], partner).start()
    ours = gown[pl.ds(pl.multiple_of(c * R, R), R), :].reshape(NZ, 8, H)
    recv(6, grecv)
    hsend[...] = (ours + grecv[...].astype(F32)).astype(BF)

    def gz_copy(peer):
        return remote(hsend.at[peer], hrecv.at[z], sent.at[7], came.at[7], {"z": peer})

    start_z(gz_copy)
    hrecv[z] = hsend[z]

    recv(5, rbuf.at[pl.ds(0, 15)])
    rbuf[q] = pbuf[xl, m]
    back = jnp.sum(rbuf[...].astype(F32), axis=0).reshape(R + 8, R)
    tan_back = back[0:R]
    act_back = back[R : R + 1]
    lin_round = (tan_back * hidden_slope).astype(BF)
    pre_back = act_back * hidden_slope - 2.0 * hidden_act * hidden_slope * jnp.sum(
        tan_back * hidden_lin, axis=0, keepdims=True
    )
    pre_round = jnp.where(top, jnp.broadcast_to(pre_back, (16, R)), 0.0).astype(BF)
    both = jnp.concatenate([lin_round, pre_round], axis=0)
    low = dot(both, hw_ref[...], NT)
    tan_lower = low[0:R]
    pre_lower = low[R : R + 1] * first_slope - 2.0 * first_act * first_slope * jnp.sum(
        tan_lower * w1, axis=0, keepdims=True
    )
    x_col = jnp.transpose(jnp.broadcast_to(x_rows[0:1], (R, R)))[:, 0:1]
    fw = x_col * pre_lower + tan_lower * first_slope
    place = lax.broadcasted_iota(jnp.int32, (8, H), 1) // R == m
    line = lax.broadcasted_iota(jnp.int32, (8, H), 0)
    pre_wide = jnp.concatenate([pre_back] * 8, axis=1)
    tail = jnp.where(line == 0, jnp.broadcast_to(pre_lower, (8, H)), 0.0)
    tail = tail + jnp.where((line == 1) & place, jnp.broadcast_to(pre_wide, (8, H)), 0.0)
    for cc in range(2):
        for k in range(16):
            r0 = 64 * cc + 32 * (k % 2)
            l0 = R * (k // 2)
            fsend[cc, k, 0:4] = fw[r0 : r0 + 32, l0 : l0 + R].reshape(4, 8, R).astype(BF)
            fsend[cc, k, 4] = tail[:, l0 : l0 + R].astype(BF)
    remote(fsend.at[1 - c], fpart, sent.at[9], came.at[9], partner).start()
    qsend[...] = dot(ft[...], both, TN).astype(BF).reshape(2, 4 * R, R)
    remote(qsend.at[1 - c], qpart, sent.at[8], came.at[8], partner).start()
    recv(9, fpart)
    fsum[...] = (fsend[c].astype(F32) + fpart[...].astype(F32)).astype(BF)
    for d in PLANE:
        peer, to = plane(d)
        remote(fsum.at[peer], frecv.at[q], sent.at[17], came.at[17], to).start()
    frecv[q] = fsum[q]
    recv(8, qpart)
    halves = qsend[c].astype(F32) + qpart[...].astype(F32)
    qsum[...] = halves.astype(BF).reshape(2, 2 * R, R)
    remote(qsum.at[1 - xl], qrecv, sent.at[18], came.at[18], xside).start()

    recv(17, frecv.at[pl.ds(0, 15)])
    ysend[...] = jnp.sum(frecv[...].astype(F32), axis=0).astype(BF)
    for t in range(5):

        @pl.when(z != t)
        def _():
            remote(ysend.at[t], yrecv.at[z], sent.at[11], came.at[11], {"z": t}).start()

        @pl.when(z == t)
        def _():
            yrecv[z] = ysend[t]

    recv(18, qrecv)
    quarter = qsum[xl].astype(F32) + qrecv[...].astype(F32)
    zsend[...] = quarter.reshape(NZ, 2, 8, R).astype(BF)

    def zr_copy(peer):
        return remote(zsend.at[peer], zrecv.at[z], sent.at[10], came.at[10], {"z": peer})

    start_z(zr_copy)
    zrecv[z] = zsend[z]

    def low_first(copy):
        for zz in LOW_FIRST:
            pl.when(z != zz)(lambda: copy({"z": zz}).start())

    def y_copy(to):
        return remote(yall.at[z], yall.at[z], sent.at[13], came.at[13], to)

    def zg_copy(to):
        return remote(zall.at[z], zall.at[z], sent.at[12], came.at[12], to)

    @pl.when(z < 5)
    def _():
        recv(11, yrecv.at[pl.ds(0, 15)])
        yall[z] = jnp.sum(yrecv[...].astype(F32), axis=0).astype(BF)
        low_first(y_copy)

    recv(10, zrecv.at[pl.ds(0, 15)])
    zall[z] = jnp.sum(zrecv[...].astype(F32), axis=0).astype(BF)
    low_first(zg_copy)

    recv(7, hrecv.at[pl.ds(0, 15)])
    dg_ref[...] = jnp.sum(hrecv[...].astype(F32), axis=0)
    outs = (
        pltpu.make_async_copy(dg_ref, dg_hbm, put.at[0]),
        pltpu.make_async_copy(tile, tile_hbm, put.at[1]),
        pltpu.make_async_copy(hall, hall_hbm.at[c], put.at[2]),
        pltpu.make_async_copy(fall, fall_hbm.at[c], put.at[3]),
    )
    outs[0].start()
    left(0, tbytes.at[pl.ds(0, 15)])
    left(1, dblk.at[0, pl.ds(0, 2)])
    left(16, dblk.at[0, pl.ds(0, 4)])
    left(2, dblk.at[0, pl.ds(0, 9)])
    left(3, dblk.at[0])
    left(4, jbuf.at[pl.ds(0, 31)])
    left(5, rbuf.at[pl.ds(0, 15)])
    left(6, grecv)
    left(7, hrecv.at[pl.ds(0, 15)])
    left(8, qpart)
    left(9, fpart)
    left(17, frecv.at[pl.ds(0, 15)])
    left(18, qrecv)
    left(10, zrecv.at[pl.ds(0, 15)])

    @pl.when(z < 5)
    def _():
        recv(13, yall.at[pl.ds(0, 4)])

    @pl.when(z >= 5)
    def _():
        recv(13, yall.at[pl.ds(0, 5)])

    for d in PLANE:
        remote(
            yall.at[pl.ds(0, 5)], fall.at[q], sent.at[15], came.at[15], plane(d)[1]
        ).start()
    fall[q] = yall[0:5]
    tile[...] = yall[4]
    outs[1].start()
    recv(12, zall.at[pl.ds(0, 15)])
    remote(zall, hall.at[xl], sent.at[14], came.at[14], xside).start()
    hall[xl] = zall[...]
    recv(15, fall.at[pl.ds(0, 15)])
    remote(fall, fall_hbm.at[c], sent.at[19], came.at[19], partner).start()
    outs[3].start()
    recv(14, zall)
    remote(hall, hall_hbm.at[c], sent.at[20], came.at[20], partner).start()
    outs[2].start()
    recv(19, fall)
    recv(20, hall)

    @pl.when(z < 5)
    def _():
        left(11, yall.at[pl.ds(0, 4)])
        left(13, yrecv.at[pl.ds(0, 15)])

    @pl.when(z >= 5)
    def _():
        left(11, yall.at[pl.ds(0, 5)])

    left(12, zrecv.at[pl.ds(0, 15)])
    left(14, zall)
    left(15, fall.at[pl.ds(0, 15)])
    left(19, fall)
    left(20, hall)
    for out in outs:
        out.wait()


def unfold(
    hall_hbm,
    fall_hbm,
    tile_hbm,
    dg_hbm,
    fw_hbm,
    fb_hbm,
    hg_hbm,
    hb_hbm,
    dgo_hbm,
    hall,
    fall,
    tile,
    dg,
    fw,
    fb,
    hg,
    hb,
    got,
    put,
):
    ins = (
        pltpu.make_async_copy(hall_hbm, hall, got.at[0]),
        pltpu.make_async_copy(fall_hbm, fall, got.at[1]),
        pltpu.make_async_copy(dg_hbm, dg, got.at[2]),
        pltpu.make_async_copy(tile_hbm, tile, got.at[3]),
    )
    outs = (
        pltpu.make_async_copy(hg, hg_hbm, put.at[0]),
        pltpu.make_async_copy(fw, fw_hbm, put.at[1]),
        pltpu.make_async_copy(dg, dgo_hbm, put.at[2]),
        pltpu.make_async_copy(hb, hb_hbm, put.at[3]),
        pltpu.make_async_copy(fb, fb_hbm, put.at[4]),
    )
    for k in (1, 0, 3, 2):
        ins[k].start()
    ins[1].wait()
    for mm in range(8):
        for ee in range(4):
            piece = fall[ee // 2, 2 * mm + ee % 2].astype(F32)
            fw[32 * ee : 32 * ee + 32, R * mm : R * mm + R] = piece[0:4].reshape(32, R)
            if ee == 0:
                fb[mm : mm + 1, :] = piece[4, 0:1]
    outs[1].start()
    outs[4].start()
    ins[3].wait()
    hb[...] = tile[...].astype(F32)[1:2]
    outs[3].start()
    ins[2].wait()
    outs[2].start()
    ins[0].wait()
    hg[...] = hall[...].astype(F32).reshape(H, R)
    outs[0].start()
    for copy in outs:
        copy.wait()


def on_device(
    inputs_store,
    window,
    targets_store,
    jac_store,
    first_weight,
    first_bias,
    hidden_weight,
    hidden_bias,
    decoder_weight,
):
    vmem = pl.BlockSpec(memory_space=pltpu.VMEM)
    smem = pl.BlockSpec(memory_space=pltpu.SMEM)
    hbm = pl.BlockSpec(memory_space=pltpu.HBM)
    dma = pltpu.SemaphoreType.DMA
    hall = jax.ShapeDtypeStruct((2, 2, NZ, 2, 8, R), BF)
    fall = jax.ShapeDtypeStruct((2, 16, 5, 8, R), BF)
    tile = jax.ShapeDtypeStruct((8, R), BF)
    dg = jax.ShapeDtypeStruct((8, H), F32)
    raw = (hall, fall, tile, dg)
    parts = pl.pallas_call(
        kernel,
        out_shape=raw,
        in_specs=[smem, vmem] + [hbm] * 8,
        out_specs=(hbm,) * 4,
        scratch_shapes=[
            pltpu.VMEM((512, R), BF),
            pltpu.VMEM((512, 8, R), BF),
            pltpu.VMEM((8, 512), BF),
            pltpu.VMEM((R, H), BF),
            pltpu.VMEM((8, R), BF),
            pltpu.VMEM((H, R), BF),
            pltpu.VMEM((1, R), BF),
            pltpu.VMEM((8, H), BF),
            pltpu.VMEM((R + 16, H), BF),
            pltpu.VMEM((R + 16, R), BF),
            pltpu.VMEM((2, 2 * R, H), BF),
            pltpu.VMEM((8, WIDE), BF),
            pltpu.VMEM((2, NZ, 8, WIDE), BF),
            pltpu.VMEM((2 * R, WIDE), BF),
            pltpu.VMEM((32, 2, 8, R), BF),
            pltpu.VMEM((32, 2, 8, R), BF),
            pltpu.VMEM((2, 2 * R, 2 * R), F32),
            pltpu.VMEM((16, R + 16, R), BF),
            pltpu.VMEM((2, 8, 17, 8, R), BF),
            pltpu.VMEM((16, 17, 8, R), BF),
            pltpu.VMEM((NZ, 8, H), BF),
            pltpu.VMEM((NZ, 8, H), BF),
            pltpu.VMEM((2 * R, H), F32),
            pltpu.VMEM((NZ, 8, H), BF),
            pltpu.VMEM((NZ, 8, H), BF),
            pltpu.VMEM((2, 4 * R, R), BF),
            pltpu.VMEM((4 * R, R), BF),
            pltpu.VMEM((2, 2 * R, R), BF),
            pltpu.VMEM((2 * R, R), BF),
            pltpu.VMEM((2, 16, 5, 8, R), BF),
            pltpu.VMEM((16, 5, 8, R), BF),
            pltpu.VMEM((16, 5, 8, R), BF),
            pltpu.VMEM((16, 5, 8, R), BF),
            pltpu.VMEM((NZ, 2, 8, R), BF),
            pltpu.VMEM((NZ, 2, 8, R), BF),
            pltpu.VMEM((NZ, 2, 8, R), BF),
            pltpu.VMEM((5, 8, R), BF),
            pltpu.VMEM((NZ, 8, R), BF),
            pltpu.VMEM((NZ, 8, R), BF),
            pltpu.VMEM((2, NZ, 2, 8, R), BF),
            pltpu.VMEM((16, 5, 8, R), BF),
            pltpu.VMEM((8, R), BF),
            pltpu.VMEM((8, H), F32),
            dma((21,)),
            dma((21,)),
            dma((8,)),
            dma((4,)),
        ],
        compiler_params=pltpu.CompilerParams(
            collective_id=0, has_side_effects=True, vmem_limit_bytes=VMEM_MOST
        ),
    )(
        window,
        window.reshape(1, 64),
        inputs_store,
        jac_store,
        targets_store.T,
        first_weight,
        first_bias.reshape(8, R),
        hidden_weight,
        hidden_bias.reshape(1, R),
        decoder_weight,
    )
    final = (
        jax.ShapeDtypeStruct((R, H), F32),
        jax.ShapeDtypeStruct((8, R), F32),
        jax.ShapeDtypeStruct((H, R), F32),
        jax.ShapeDtypeStruct((1, R), F32),
        dg,
    )
    fw, fb, hg, hb, dgo = pl.pallas_call(
        unfold,
        out_shape=final,
        in_specs=[hbm] * 4,
        out_specs=(hbm,) * 5,
        scratch_shapes=[pltpu.VMEM(a.shape, a.dtype) for a in raw + final[0:4]]
        + [dma((4,)), dma((5,))],
        compiler_params=pltpu.CompilerParams(vmem_limit_bytes=VMEM_MOST),
    )(*parts)
    return fw, fb.reshape(H), hg, hb.reshape(R), dgo


def solution(mesh):
    torus = Mesh(mesh.devices.reshape(NZ, 2, 2, 4, 2), ALL)
    return jax.shard_map(
        on_device,
        mesh=torus,
        in_specs=(
            P(),
            P(),
            P(None, ALL),
            P(None, ALL, None),
            P(),
            P(),
            P(None, MP),
            P(MP),
            P(ALL, None),
        ),
        out_specs=(P(), P(), P(None, MP), P(MP), P(ALL, None)),
        check_vma=False,
    )
```
